16 devices in a mesh: dp: 4 (over z, y), sp: 4 (over x, core).
Axes of the slice: x: 2, y: 2, z: 2, core: 2. Of those that a mesh axis runs over, the one named last changes fastest.
Arguments:
- hidden: bfloat16 [64, 1024, 768], P('dp', 'sp'), parts along dimension 0
- pos_ids: int32 [64, 1024], P('dp', 'sp'), parts along dimension 0
- block_ids: int32 [64, 1024], P('dp', 'sp'), parts along dimension 0
- ctx_len: int32 [64], P('dp'), parts along dimension 0
- ln_gamma: bfloat16 [768], replicated
- ln_beta: bfloat16 [768], replicated
- w_qkv: bfloat16 [768, 12, 3, 64], replicated
- b_qkv: bfloat16 [12, 3, 64], replicated
- w_dense: bfloat16 [768, 768], replicated
- b_dense: bfloat16 [768], replicated
Outputs:
- output 1: bfloat16 [64, 1024, 768], P('dp', 'sp'), parts along dimension 0
- output 2: bfloat16 [64, 1024, 12, 64], P('dp', None, 'sp'), parts along dimension 0
- output 3: bfloat16 [64, 1024, 12, 64], P('dp', None, 'sp'), parts along dimension 0
There are 4 independent parts. The reference program is written for one: setup_inputs(seed, part) draws one part's arguments, and reference() takes and returns one part's arrays. A program takes and returns all parts, laid end to end along the dimension named above; an argument that names none is the same for every part.
All inputs are finite; a program needn't handle non-finite values.
Results may differ from the reference program's by a relative error of at most 0.00594918.
Values are sent between devices in bfloat16 or wider.
A program may use at most 1 GiB of HBM per device.

```python
import math
import jax
import jax.numpy as jnp
from jax import lax

BATCH = 16
SEQ = 1024
HEADS = 12
HEAD = 64
HIDDEN = HEADS * HEAD
ALPHA = math.sqrt(56.0)
ROPE_BASE = 10000.0
LN_EPS = 1e-5
SCORE_SCALE = 1.0 / math.sqrt(HEAD)
QUERY_BLOCK = min(SEQ, 128)
GAIN = 1.0 / ALPHA
QKV_SCALE = ALPHA / math.sqrt(HIDDEN)
DENSE_SCALE = 0.5 * math.sqrt(SEQ / HIDDEN)
BIAS_SCALE = 1.0 / math.sqrt(SEQ)


def draw_positions(ctx_key, mask_key):
    ctx_len = jax.random.randint(ctx_key, (BATCH,), SEQ // 4, 3 * SEQ // 4 + 1, dtype=jnp.int32)
    mask_pos = jax.random.randint(mask_key, (BATCH,), 0, ctx_len, dtype=jnp.int32)
    token_pos = jnp.arange(SEQ, dtype=jnp.int32)[None, :]
    in_context = token_pos < ctx_len[:, None]
    pos_ids = jnp.where(in_context, token_pos, mask_pos[:, None]).astype(jnp.int32)
    block_ids = jnp.where(in_context, 0, token_pos - ctx_len[:, None] + 1).astype(jnp.int32)
    return pos_ids, block_ids, ctx_len


def setup_inputs(seed: int = 0, part: int = 0) -> dict:
    base_key = jax.random.key(seed)
    shared_key, part_key = jax.random.split(base_key)
    part_key = jax.random.fold_in(part_key, part)
    key_x, key_ctx, key_mask = jax.random.split(part_key, 3)
    key_g, key_b, key_w, key_wb, key_d, key_db = jax.random.split(shared_key, 6)
    pos_ids, block_ids, ctx_len = draw_positions(key_ctx, key_mask)
    hidden = jax.random.normal(key_x, (BATCH, SEQ, HIDDEN), jnp.float32)
    ln_gamma = (1.0 + 0.2 * jax.random.normal(key_g, (HIDDEN,), jnp.float32)) * GAIN
    ln_beta = jax.random.normal(key_b, (HIDDEN,), jnp.float32) * (GAIN * BIAS_SCALE)
    w_qkv = jax.random.normal(key_w, (HIDDEN, HEADS, 3, HEAD), jnp.float32) * QKV_SCALE
    b_qkv = jax.random.normal(key_wb, (HEADS, 3, HEAD), jnp.float32) * BIAS_SCALE
    w_dense = jax.random.normal(key_d, (HIDDEN, HIDDEN), jnp.float32) * DENSE_SCALE
    b_dense = jax.random.normal(key_db, (HIDDEN,), jnp.float32) * 0.5
    return {'hidden': hidden.astype(jnp.bfloat16), 'pos_ids': pos_ids, 'block_ids': block_ids, 'ctx_len': ctx_len, 'ln_gamma': ln_gamma.astype(jnp.bfloat16), 'ln_beta': ln_beta.astype(jnp.bfloat16), 'w_qkv': w_qkv.astype(jnp.bfloat16), 'b_qkv': b_qkv.astype(jnp.bfloat16), 'w_dense': w_dense.astype(jnp.bfloat16), 'b_dense': b_dense.astype(jnp.bfloat16)}


def layer_norm(hidden, ln_gamma, ln_beta):
    wide_in = hidden.astype(jnp.float32)
    row_mean = jnp.mean(wide_in, axis=-1, keepdims=True)
    centered = wide_in - row_mean
    row_var = jnp.mean(jnp.square(centered), axis=-1, keepdims=True)
    return (centered * lax.rsqrt(row_var + LN_EPS) * ln_gamma.astype(jnp.float32) + ln_beta.astype(jnp.float32)).astype(jnp.bfloat16)


def rotate(heads_in, pos_ids, block_ids):
    half_dim = heads_in.shape[-1] // 2
    quarter_dim = half_dim // 2
    inv_freq = ROPE_BASE ** (-jnp.arange(0, half_dim, 2).astype(jnp.float32) / half_dim)
    angles = jnp.stack([pos_ids, block_ids], axis=-1).astype(jnp.float32)[..., None] * inv_freq
    cos_a = jnp.cos(angles)[:, :, None]
    sin_a = jnp.sin(angles)[:, :, None]
    split_dims = heads_in.astype(jnp.float32).reshape(heads_in.shape[:-1] + (2, 2, quarter_dim))
    low_part = split_dims[..., 0, :]
    high_part = split_dims[..., 1, :]
    new_low = low_part * cos_a - high_part * sin_a
    new_high = high_part * cos_a + low_part * sin_a
    return jnp.stack([new_low, new_high], axis=-2).reshape(heads_in.shape).astype(jnp.bfloat16)


def reference(hidden, pos_ids, block_ids, ctx_len, ln_gamma, ln_beta, w_qkv, b_qkv, w_dense, b_dense):
    normed = layer_norm(hidden, ln_gamma, ln_beta)
    qkv_flat = jnp.dot(normed.reshape(BATCH * SEQ, HIDDEN), w_qkv.reshape(HIDDEN, 3 * HIDDEN), preferred_element_type=jnp.float32)
    qkv_proj = (qkv_flat.reshape(BATCH, SEQ, HEADS, 3, HEAD) + b_qkv.astype(jnp.float32)).astype(jnp.bfloat16)
    query_rot = rotate(qkv_proj[:, :, :, 0], pos_ids, block_ids)
    key_rot = rotate(qkv_proj[:, :, :, 1], pos_ids, block_ids)
    value_heads = qkv_proj[:, :, :, 2]
    key_pos = jnp.arange(SEQ)
    ctx_visible = key_pos[None, None, :] < ctx_len[:, None, None]

    def one_head(head_args):
        q_head, k_head, v_head = head_args
        k_wide = k_head.astype(jnp.float32)
        v_wide = v_head.astype(jnp.float32)

        def one_block(block_idx):
            block_start = block_idx * QUERY_BLOCK
            q_block = lax.dynamic_slice_in_dim(q_head, block_start, QUERY_BLOCK, axis=1).astype(jnp.float32)
            scores = jnp.einsum('bqe,bke->bqk', q_block, k_wide) * SCORE_SCALE
            q_pos = block_start + jnp.arange(QUERY_BLOCK)
            visible = ctx_visible | (key_pos[None, None, :] <= q_pos[None, :, None])
            attn_probs = jax.nn.softmax(jnp.where(visible, scores, -jnp.inf), axis=-1).astype(jnp.bfloat16)
            return jnp.einsum('bqk,bke->bqe', attn_probs.astype(jnp.float32), v_wide).astype(jnp.bfloat16)

        blocks = lax.map(one_block, jnp.arange(SEQ // QUERY_BLOCK))
        return jnp.moveaxis(blocks, 0, 1).reshape(BATCH, SEQ, HEAD)

    head_major = (jnp.moveaxis(query_rot, 2, 0), jnp.moveaxis(key_rot, 2, 0), jnp.moveaxis(value_heads, 2, 0))
    context = lax.map(one_head, head_major)
    context = jnp.moveaxis(context, 0, 2).reshape(BATCH * SEQ, HIDDEN)
    dense_out = jnp.dot(context, w_dense, preferred_element_type=jnp.float32) + b_dense.astype(jnp.float32)
    block_out = (normed.reshape(BATCH * SEQ, HIDDEN).astype(jnp.float32) * ALPHA + dense_out).astype(jnp.bfloat16)
    return block_out.reshape(BATCH, SEQ, HIDDEN), key_rot, value_heads
```

```python
import functools
import math

import jax
import jax.numpy as jnp
import numpy as np
from jax import lax
from jax.experimental import pallas as pl
from jax.experimental.pallas import tpu as pltpu
from jax.sharding import PartitionSpec as P

ALPHA = math.sqrt(56.0)
ROPE_BASE = 10000.0
LN_EPS = 1e-5
MESH = pl.DeviceIdType.MESH
F32 = jnp.float32
BF16 = jnp.bfloat16

ROWS = 16
PART = 256
SEQ = 1024
HID = 768
HEAD = 64
CHIP = 512
LOCAL = 6
WIDE = LOCAL * HEAD
EXP_SCALE = math.log2(math.e) / math.sqrt(HEAD)
CHUNK = 64


def rope_tables():
    freq = ROPE_BASE ** (-np.arange(0, 32, 2).astype(np.float64) / 32.0)
    angle = freq.astype(np.float32)[:, None] * np.arange(SEQ, dtype=np.float32)[None, :]
    return np.cos(angle.astype(np.float64)).astype(np.float32), np.sin(angle.astype(np.float64)).astype(np.float32)


def nt_dot(a, b):
    return lax.dot_general(a, b, (((1,), (1,)), ((), ())), preferred_element_type=F32)


def kernel(hid_hbm, pos_ref, ctx_ref, gamma_ref, beta_ref, bd_ref, w_hbm, bias_hbm, wd_hbm, tcos_ref, tsin_ref,
           out_ref, ko_ref, vo_ref,
           a_all, posr, w_sc, b_sc, wd_sc, y_sc, kt, vt, kk, qbd, ctab, stab, s_0, s_1, s_2, s_3, p_0, p_1, p_2, p_3, top_sc, inv_sc, ctx_buf, ctx_recv,
           hid_sem, w_sem, xs_sem, xr_sem, ds_sem, dr_sem, rs_sem, rr_sem, cs_sem, cr_sem, ps_sem, pr_sem):
    step = pl.program_id(0)
    s_refs, p_refs = (s_0, s_1, s_2, s_3), (p_0, p_1, p_2, p_3)
    me = lax.axis_index('sp')
    core = lax.rem(me, 2)
    chip = me // 2
    other = 1 - chip
    peer_x = other * 2 + core
    peer_d = chip * 2 + 1 - core
    peer_xd = other * 2 + 1 - core

    def send_x(r):
        return pltpu.make_async_remote_copy(a_all.at[r, me], a_all.at[r, me], xs_sem.at[r], xr_sem.at[r], device_id={'sp': peer_x}, device_id_type=MESH)

    def send_d(r):
        return pltpu.make_async_remote_copy(a_all.at[r, me], a_all.at[r, me], ds_sem.at[r], dr_sem.at[r], device_id={'sp': peer_d}, device_id_type=MESH)

    def recv_x(r):
        return pltpu.make_async_remote_copy(a_all.at[r, peer_x], a_all.at[r, peer_x], xs_sem.at[r], xr_sem.at[r], device_id={'sp': peer_x}, device_id_type=MESH)

    def recv_d(r):
        return pltpu.make_async_remote_copy(a_all.at[r, peer_d], a_all.at[r, peer_d], ds_sem.at[r], dr_sem.at[r], device_id={'sp': peer_d}, device_id_type=MESH)

    def relay(r):
        return pltpu.make_async_remote_copy(a_all.at[r, peer_x], a_all.at[r, peer_x], rs_sem.at[r], rr_sem.at[r], device_id={'sp': peer_d}, device_id_type=MESH)

    def recv_relay(r):
        return pltpu.make_async_remote_copy(a_all.at[r, peer_xd], a_all.at[r, peer_xd], rs_sem.at[r], rr_sem.at[r], device_id={'sp': peer_d}, device_id_type=MESH)

    def swap_ctx(r):
        return pltpu.make_async_remote_copy(ctx_buf.at[r, 1 - core], ctx_recv.at[r], cs_sem.at[r], cr_sem.at[r], device_id={'sp': peer_d}, device_id_type=MESH)

    def swap_pos(n, peer):
        return pltpu.make_async_remote_copy(pos_ref.at[:, pl.ds(128, 128)], posr.at[me], ps_sem.at[n], pr_sem.at[n], device_id={'sp': peer}, device_id_type=MESH)

    def recv_pos(n, peer):
        return pltpu.make_async_remote_copy(pos_ref.at[:, pl.ds(128, 128)], posr.at[peer], ps_sem.at[n], pr_sem.at[n], device_id={'sp': peer}, device_id_type=MESH)

    def load_hidden(r):
        return pltpu.make_async_copy(hid_hbm.at[r], a_all.at[r, me], hid_sem.at[r])

    def weight_copies():
        copies = []
        for group, owner in enumerate((me, peer_x)):
            for slot, kind in ((0, 1), (6, 2), (12, 0)):
                for h in range(3):
                    copies.append((w_hbm.at[owner * 3 + h, kind], w_sc.at[slot + 3 * group + h]))
                    copies.append((bias_hbm.at[owner * 3 + h, kind], b_sc.at[slot + 3 * group + h]))
        for slot, owner in enumerate((me, peer_x, peer_d, peer_xd)):
            copies.append((wd_hbm.at[pl.ds(pl.multiple_of(owner * 192, 64), 192)], wd_sc.at[pl.ds(slot * 192, 192)]))
        return [pltpu.make_async_copy(src, dst, w_sem.at[i]) for i, (src, dst) in enumerate(copies)]

    def norm_row(r):
        gamma = gamma_ref[...].astype(F32)
        beta = beta_ref[...].astype(F32)
        for t in range(0, PART, 32):
            wide = a_all[r, me, pl.ds(t, 32), :].astype(F32)
            mean = jnp.sum(wide, axis=-1, keepdims=True) * (1.0 / HID)
            cent = wide - mean
            var = jnp.sum(cent * cent, axis=-1, keepdims=True) * (1.0 / HID)
            a_all[r, me, pl.ds(t, 32), :] = (cent * lax.rsqrt(var + LN_EPS) * gamma + beta).astype(BF16)

    @pl.when(step == 0)
    def _():
        def fetch(r, c):
            load_hidden(r).start()
            return c

        lax.fori_loop(0, ROWS, fetch, 0)
        for c in weight_copies():
            c.start()
        barrier = pltpu.get_barrier_semaphore()
        for peer in (peer_x, peer_d, peer_xd):
            pl.semaphore_signal(barrier, inc=1, device_id={'sp': peer}, device_id_type=MESH)
        pl.semaphore_wait(barrier, 3)
        for n, peer in enumerate((peer_x, peer_d, peer_xd)):
            swap_pos(n, peer).start()
        posr[me] = pos_ref[:, 128:256]
        qbd[...] = jnp.zeros_like(qbd)

        def norm_and_send(r, c):
            load_hidden(r).wait()
            norm_row(r)

            @pl.when(r > 0)
            def _():
                send_x(r - 1).start()
                send_d(r - 1).start()

            return c

        lax.fori_loop(0, ROWS, norm_and_send, 0)
        for c in weight_copies():
            c.wait()
        for n, peer in enumerate((peer_x, peer_d, peer_xd)):
            recv_pos(n, peer).wait()
        send_x(ROWS - 1).start()
        send_d(ROWS - 1).start()

    def build_tables(r):
        tcos = tcos_ref[...]
        tsin = tsin_ref[...]
        lane = lax.broadcasted_iota(jnp.int32, (16, SEQ), 1)
        ctx = ctx_ref[r]
        last = posr[3, pl.ds(r, 1), :]
        last_lane = lax.broadcasted_iota(jnp.int32, (1, 128), 1)
        m_pos = jnp.sum(jnp.where(last_lane == 127, last, 0), axis=1, keepdims=True)

        def pick(table, hit):
            return jnp.sum(jnp.where(hit, table, 0.0), axis=1, keepdims=True)

        at_m = lane == m_pos
        at_c = lane == ctx - 1
        in_ctx = lane < ctx
        cos_c, sin_c = pick(tcos, at_c), pick(tsin, at_c)
        ctab[0:16] = jnp.where(in_ctx, tcos, pick(tcos, at_m))
        stab[0:16] = jnp.where(in_ctx, tsin, pick(tsin, at_m))
        ctab[16:32] = jnp.where(in_ctx, 1.0, tcos * cos_c + tsin * sin_c)
        stab[16:32] = jnp.where(in_ctx, 0.0, tsin * cos_c - tcos * sin_c)

    def project(r, which, with_q):
        rows = 3 * WIDE if with_q else 2 * WIDE
        tokens = a_all[r, pl.ds(2 * which, 2)].reshape(CHIP, HID)
        y_sc[0:rows] = nt_dot(w_sc[0:rows // HEAD].reshape(rows, HID), tokens)
        for lt in range(CHIP // 128):
            cols = pl.ds(pl.multiple_of(which * CHIP + lt * 128, 128), 128)
            ycols = slice(lt * 128, lt * 128 + 128)
            for h in range(LOCAL):
                for half in range(2):
                    cos = ctab[16 * half:16 * half + 16, cols]
                    sin = stab[16 * half:16 * half + 16, cols]

                    def rotated(base):
                        u0 = base + h * HEAD + half * 32
                        b0 = half * 32
                        bias = b_sc.at[base // HEAD + h]
                        u = (y_sc[u0:u0 + 16, ycols] + bias[b0:b0 + 16]).astype(BF16).astype(F32)
                        w = (y_sc[u0 + 16:u0 + 32, ycols] + bias[b0 + 16:b0 + 32]).astype(BF16).astype(F32)
                        return (u * cos - w * sin).astype(BF16), (w * cos + u * sin).astype(BF16)

                    k0 = h * HEAD + half * 32
                    ku, kw = rotated(0)
                    kt[k0:k0 + 16, cols] = ku
                    kt[k0 + 16:k0 + 32, cols] = kw
                    if with_q:
                        qu, qw = rotated(2 * WIDE)
                        q0 = (h % 2) * HEAD + half * 32
                        qc = slice((h % 2) * CHIP + lt * 128, (h % 2) * CHIP + lt * 128 + 128)
                        qbd[h // 2, q0:q0 + 16, qc] = qu
                        qbd[h // 2, q0 + 16:q0 + 32, qc] = qw
                v0 = WIDE + h * HEAD
                vt[h * HEAD:(h + 1) * HEAD, cols] = (y_sc[v0:v0 + HEAD, ycols] + b_sc[6 + h]).astype(BF16)

    def attend(r, this_chip):
        spec = ((768, 256), (768, 256)) if this_chip == 0 else ((768, 512), (1024, 768))

        def score(pair, j):
            for qb in range(2):
                key_len, mask_from = spec[qb]
                q0 = j * CHIP + qb * PART
                scores = jnp.dot(kk[pair, 0:key_len, :], qbd[pair, :, q0:q0 + PART], preferred_element_type=F32)
                q_pos = this_chip * CHIP + qb * PART + lax.broadcasted_iota(jnp.int32, (1, PART), 1)
                limit = jnp.maximum(q_pos, ctx_ref[r] - 1)
                top = None
                for k0 in range(0, key_len, CHUNK):
                    part = scores[k0:k0 + CHUNK]
                    if k0 >= mask_from:
                        k_pos = k0 + lax.broadcasted_iota(jnp.int32, (CHUNK, PART), 0)
                        part = jnp.where(k_pos <= limit, part, -jnp.inf)
                    s_refs[2 * j + qb][k0:k0 + CHUNK] = part
                    peak = jnp.max(part.reshape(CHUNK // 8, 8, PART), axis=0)
                    top = peak if top is None else jnp.maximum(top, peak)
                top_sc[2 * j + qb] = jnp.broadcast_to(jnp.max(top, axis=0, keepdims=True) * EXP_SCALE, (8, PART))

        def weigh(j):
            for qb in range(2):
                key_len = spec[qb][0]
                top = top_sc[2 * j + qb, 0:1]
                total = jnp.zeros((8, PART), F32)
                for k0 in range(0, key_len, CHUNK):
                    prob = jnp.exp2(s_refs[2 * j + qb][k0:k0 + CHUNK] * EXP_SCALE - top)
                    total = total + jnp.sum(prob.reshape(CHUNK // 8, 8, PART), axis=0)
                    p_refs[2 * j + qb][k0:k0 + CHUNK] = prob.astype(BF16)
                inv_sc[2 * j + qb] = jnp.broadcast_to(1.0 / jnp.sum(total, axis=0, keepdims=True), (8, PART))

        def mix(pair, j):
            v_rows = pl.ds(pl.multiple_of((2 * pair + j) * HEAD, HEAD), HEAD)
            for qb in range(2):
                key_len = spec[qb][0]
                mixed = jnp.dot(vt[v_rows, 0:key_len], p_refs[2 * j + qb][0:key_len], preferred_element_type=F32)
                ctx_buf[r, qb, v_rows, :] = (mixed * inv_sc[2 * j + qb, 0:1]).astype(BF16)

        score(0, 0)
        score(0, 1)
        weigh(0)

        def one_pair(pair, c):
            score(pair + 1, 0)
            weigh(1)
            mix(pair, 0)
            score(pair + 1, 1)
            weigh(0)
            mix(pair, 1)
            return c

        lax.fori_loop(0, LOCAL // 2 - 1, one_pair, 0)
        weigh(1)
        mix(LOCAL // 2 - 1, 0)
        mix(LOCAL // 2 - 1, 1)

    def dense(r):
        mixed = jnp.concatenate([ctx_buf[r, core], ctx_recv[r]], axis=0)
        dense_out = lax.dot_general(mixed, wd_sc[...], (((0,), (0,)), ((), ())), preferred_element_type=F32)
        normed = a_all[r, me].astype(F32)
        out_ref[0] = (normed * ALPHA + dense_out + bd_ref[...].astype(F32)).astype(BF16)

    @pl.when(step < ROWS)
    def _():
        build_tables(step)
        recv_d(step).wait_recv()
        project(step, chip, True)

    @pl.when(step > 0)
    def _():
        swap_ctx(step - 1).start()

    @pl.when(step < ROWS)
    def _():
        recv_x(step).wait_recv()
        relay(step).start()

    @pl.when(step > 0)
    def _():
        swap_ctx(step - 1).wait_recv()
        dense(step - 1)

    @pl.when(step < ROWS)
    def _():
        recv_relay(step).wait_recv()
        project(step, other, False)
        ko_ref[0] = kt[0:192].reshape(3, HEAD, SEQ)
        vo_ref[0] = vt[0:192].reshape(3, HEAD, SEQ)
        for pair in range(LOCAL // 2):
            kk[pair] = kt[pair * 128:(pair + 1) * 128, :].T

    @pl.when(jnp.logical_and(step < ROWS, chip == 0))
    def _():
        attend(step, 0)

    @pl.when(jnp.logical_and(step < ROWS, chip == 1))
    def _():
        attend(step, 1)

    @pl.when(step == ROWS)
    def _():
        def drain(r, c):
            send_x(r).wait_send()
            send_d(r).wait_send()
            relay(r).wait_send()
            swap_ctx(r).wait_send()
            return c

        lax.fori_loop(0, ROWS, drain, 0)


def solution(mesh):
    seq_spec = P('dp', 'sp', None)
    row_spec = P('dp', 'sp')
    head_spec = P('dp', None, 'sp', None)
    replicated = P()
    tcos, tsin = rope_tables()

    def local_block(hidden, pos_ids, block_ids, ctx_len, ln_gamma, ln_beta, w_qkv, b_qkv, w_dense, b_dense):
        w_t = jnp.transpose(w_qkv, (1, 2, 3, 0))
        bias = jnp.broadcast_to(b_qkv.astype(F32)[..., None], (12, 3, HEAD, 128))
        anywhere = pl.BlockSpec(memory_space=pl.ANY)

        def whole(shape):
            return pl.BlockSpec(shape, lambda i: (0,) * len(shape))

        out, keys_t, values_t = pl.pallas_call(
            kernel,
            grid=(ROWS + 1,),
            out_shape=(
                jax.ShapeDtypeStruct((ROWS, PART, HID), BF16),
                jax.ShapeDtypeStruct((ROWS, 3, HEAD, SEQ), BF16),
                jax.ShapeDtypeStruct((ROWS, 3, HEAD, SEQ), BF16),
            ),
            in_specs=[
                anywhere, whole((ROWS, PART)), pl.BlockSpec(memory_space=pltpu.SMEM),
                whole((1, HID)), whole((1, HID)), whole((1, HID)),
                anywhere, anywhere, anywhere, whole((16, SEQ)), whole((16, SEQ)),
            ],
            out_specs=(
                pl.BlockSpec((1, PART, HID), lambda i: (jnp.maximum(i - 1, 0), 0, 0)),
                pl.BlockSpec((1, 3, HEAD, SEQ), lambda i: (jnp.minimum(i, ROWS - 1), 0, 0, 0)),
                pl.BlockSpec((1, 3, HEAD, SEQ), lambda i: (jnp.minimum(i, ROWS - 1), 0, 0, 0)),
            ),
            scratch_shapes=[
                pltpu.VMEM((ROWS, 4, PART, HID), BF16),
                pltpu.VMEM((4, ROWS, 128), jnp.int32),
                pltpu.VMEM((18, HEAD, HID), BF16),
                pltpu.VMEM((18, HEAD, 128), F32),
                pltpu.VMEM((HID, HID), BF16),
                pltpu.VMEM((3 * WIDE, CHIP), F32),
                pltpu.VMEM((WIDE, SEQ), BF16),
                pltpu.VMEM((WIDE, SEQ), BF16),
                pltpu.VMEM((3, SEQ, 128), BF16),
                pltpu.VMEM((3, 128, 2 * CHIP), BF16),
                pltpu.VMEM((32, SEQ), F32),
                pltpu.VMEM((32, SEQ), F32),
                *[pltpu.VMEM((SEQ, PART), F32)] * 4,
                *[pltpu.VMEM((SEQ, PART), BF16)] * 4,
                pltpu.VMEM((4, 8, PART), F32),
                pltpu.VMEM((4, 8, PART), F32),
                pltpu.VMEM((ROWS, 2, WIDE, PART), BF16),
                pltpu.VMEM((ROWS, WIDE, PART), BF16),
                pltpu.SemaphoreType.DMA((ROWS,)),
                pltpu.SemaphoreType.DMA((40,)),
            ] + [pltpu.SemaphoreType.DMA((ROWS,))] * 8 + [pltpu.SemaphoreType.DMA((3,))] * 2,
            compiler_params=pltpu.CompilerParams(
                collective_id=0, has_side_effects=True, vmem_limit_bytes=62 * 1024 * 1024, dimension_semantics=('arbitrary',)),
            name='glm_block',
        )(hidden, pos_ids, ctx_len, ln_gamma.reshape(1, HID), ln_beta.reshape(1, HID), b_dense.reshape(1, HID),
          w_t, bias, w_dense, jnp.asarray(tcos), jnp.asarray(tsin))
        return out, jnp.transpose(keys_t, (0, 3, 1, 2)), jnp.transpose(values_t, (0, 3, 1, 2))

    return jax.shard_map(local_block, mesh=mesh, in_specs=(seq_spec, row_spec, row_spec, P('dp'), replicated, replicated, replicated, replicated, replicated, replicated), out_specs=(seq_spec, head_spec, head_spec), check_vma=False)
```

```python
import functools
import math

import jax
import jax.numpy as jnp
import numpy as np
from jax import lax
from jax.experimental import pallas as pl
from jax.experimental.pallas import tpu as pltpu
from jax.sharding import PartitionSpec as P

ALPHA = math.sqrt(56.0)
ROPE_BASE = 10000.0
LN_EPS = 1e-5
MESH = pl.DeviceIdType.MESH
F32 = jnp.float32
BF16 = jnp.bfloat16

ROWS = 16
PART = 256
SEQ = 1024
HID = 768
HEAD = 64
CHIP = 512
LOCAL = 6
WIDE = LOCAL * HEAD
EXP_SCALE = math.log2(math.e) / math.sqrt(HEAD)
CHUNK = 64


def rope_tables():
    freq = ROPE_BASE ** (-np.arange(0, 32, 2).astype(np.float64) / 32.0)
    angle = freq.astype(np.float32)[:, None] * np.arange(SEQ, dtype=np.float32)[None, :]
    return np.cos(angle.astype(np.float64)).astype(np.float32), np.sin(angle.astype(np.float64)).astype(np.float32)


def nt_dot(a, b):
    return lax.dot_general(a, b, (((1,), (1,)), ((), ())), preferred_element_type=F32)


def kernel(hid_hbm, pos_ref, ctx_ref, gamma_ref, beta_ref, bd_ref, w_hbm, bias_ref, wd_hbm, tcos_ref, tsin_ref,
           out_ref, ko_ref, vo_ref,
           a_all, posr, w_sc, b_sc, wd_sc, y_sc, kt, vt, kk, qbd, ctab, stab, s_0, s_1, s_2, s_3, p_0, p_1, p_2, p_3, top_sc, inv_sc, ctx_buf, ctx_recv,
           hid_sem, w_sem, xs_sem, xr_sem, ds_sem, dr_sem, rs_sem, rr_sem, cs_sem, cr_sem, ps_sem, pr_sem):
    step = pl.program_id(0)
    s_refs, p_refs = (s_0, s_1, s_2, s_3), (p_0, p_1, p_2, p_3)
    me = lax.axis_index('sp')
    core = lax.rem(me, 2)
    chip = me // 2
    other = 1 - chip
    peer_x = other * 2 + core
    peer_d = chip * 2 + 1 - core
    peer_xd = other * 2 + 1 - core

    def send_x(r):
        return pltpu.make_async_remote_copy(a_all.at[r, me], a_all.at[r, me], xs_sem.at[r], xr_sem.at[r], device_id={'sp': peer_x}, device_id_type=MESH)

    def send_d(r):
        return pltpu.make_async_remote_copy(a_all.at[r, me], a_all.at[r, me], ds_sem.at[r], dr_sem.at[r], device_id={'sp': peer_d}, device_id_type=MESH)

    def recv_x(r):
        return pltpu.make_async_remote_copy(a_all.at[r, peer_x], a_all.at[r, peer_x], xs_sem.at[r], xr_sem.at[r], device_id={'sp': peer_x}, device_id_type=MESH)

    def recv_d(r):
        return pltpu.make_async_remote_copy(a_all.at[r, peer_d], a_all.at[r, peer_d], ds_sem.at[r], dr_sem.at[r], device_id={'sp': peer_d}, device_id_type=MESH)

    def relay(r):
        return pltpu.make_async_remote_copy(a_all.at[r, peer_x], a_all.at[r, peer_x], rs_sem.at[r], rr_sem.at[r], device_id={'sp': peer_d}, device_id_type=MESH)

    def recv_relay(r):
        return pltpu.make_async_remote_copy(a_all.at[r, peer_xd], a_all.at[r, peer_xd], rs_sem.at[r], rr_sem.at[r], device_id={'sp': peer_d}, device_id_type=MESH)

    def swap_ctx(r):
        return pltpu.make_async_remote_copy(ctx_buf.at[r, 1 - core], ctx_recv.at[r], cs_sem.at[r], cr_sem.at[r], device_id={'sp': peer_d}, device_id_type=MESH)

    def swap_pos(n, peer):
        return pltpu.make_async_remote_copy(pos_ref.at[:, pl.ds(128, 128)], posr.at[me], ps_sem.at[n], pr_sem.at[n], device_id={'sp': peer}, device_id_type=MESH)

    def recv_pos(n, peer):
        return pltpu.make_async_remote_copy(pos_ref.at[:, pl.ds(128, 128)], posr.at[peer], ps_sem.at[n], pr_sem.at[n], device_id={'sp': peer}, device_id_type=MESH)

    def load_hidden(r):
        return pltpu.make_async_copy(hid_hbm.at[r], a_all.at[r, me], hid_sem.at[r])

    def weight_copies():
        copies = []
        for group, owner in enumerate((me, peer_x)):
            for slot, kind in ((0, 1), (6, 2), (12, 0)):
                for h in range(3):
                    copies.append((w_hbm.at[owner * 3 + h, kind], w_sc.at[slot + 3 * group + h]))
        for slot, owner in enumerate((me, peer_x, peer_d, peer_xd)):
            copies.append((wd_hbm.at[pl.ds(pl.multiple_of(owner * 192, 64), 192)], wd_sc.at[pl.ds(slot * 192, 192)]))
        return [pltpu.make_async_copy(src, dst, w_sem.at[i]) for i, (src, dst) in enumerate(copies)]

    def norm_row(r):
        gamma = gamma_ref[...].astype(F32).reshape(1, HID)
        beta = beta_ref[...].astype(F32).reshape(1, HID)
        for t in range(0, PART, 32):
            wide = a_all[r, me, pl.ds(t, 32), :].astype(F32)
            mean = jnp.sum(wide, axis=-1, keepdims=True) * (1.0 / HID)
            cent = wide - mean
            var = jnp.sum(cent * cent, axis=-1, keepdims=True) * (1.0 / HID)
            a_all[r, me, pl.ds(t, 32), :] = (cent * lax.rsqrt(var + LN_EPS) * gamma + beta).astype(BF16)

    def spread_bias():
        for group, owner in enumerate((me, peer_x)):
            for slot, kind in ((0, 1), (6, 2), (12, 0)):
                for h in range(3):
                    row = bias_ref[owner * 3 + h, kind:kind + 1, :].astype(F32)
                    b_sc[slot + 3 * group + h] = jnp.broadcast_to(row, (128, HEAD)).T

    @pl.when(step == 0)
    def _():
        def fetch(r, c):
            load_hidden(r).start()
            return c

        lax.fori_loop(0, ROWS, fetch, 0)
        for c in weight_copies():
            c.start()
        barrier = pltpu.get_barrier_semaphore()
        for peer in (peer_x, peer_d, peer_xd):
            pl.semaphore_signal(barrier, inc=1, device_id={'sp': peer}, device_id_type=MESH)
        pl.semaphore_wait(barrier, 3)
        for n, peer in enumerate((peer_x, peer_d, peer_xd)):
            swap_pos(n, peer).start()
        posr[me] = pos_ref[:, 128:256]
        qbd[...] = jnp.zeros_like(qbd)
        spread_bias()

        def norm_and_send(r, c):
            load_hidden(r).wait()
            norm_row(r)

            @pl.when(r > 0)
            def _():
                send_x(r - 1).start()
                send_d(r - 1).start()

            return c

        lax.fori_loop(0, ROWS, norm_and_send, 0)
        for c in weight_copies():
            c.wait()
        for n, peer in enumerate((peer_x, peer_d, peer_xd)):
            recv_pos(n, peer).wait()
        send_x(ROWS - 1).start()
        send_d(ROWS - 1).start()

    def build_tables(r):
        tcos = tcos_ref[...]
        tsin = tsin_ref[...]
        lane = lax.broadcasted_iota(jnp.int32, (16, SEQ), 1)
        ctx = ctx_ref[r]
        last = posr[3, pl.ds(r, 1), :]
        last_lane = lax.broadcasted_iota(jnp.int32, (1, 128), 1)
        m_pos = jnp.sum(jnp.where(last_lane == 127, last, 0), axis=1, keepdims=True)

        def pick(table, hit):
            return jnp.sum(jnp.where(hit, table, 0.0), axis=1, keepdims=True)

        at_m = lane == m_pos
        at_c = lane == ctx - 1
        in_ctx = lane < ctx
        cos_c, sin_c = pick(tcos, at_c), pick(tsin, at_c)
        ctab[0:16] = jnp.where(in_ctx, tcos, pick(tcos, at_m))
        stab[0:16] = jnp.where(in_ctx, tsin, pick(tsin, at_m))
        ctab[16:32] = jnp.where(in_ctx, 1.0, tcos * cos_c + tsin * sin_c)
        stab[16:32] = jnp.where(in_ctx, 0.0, tsin * cos_c - tcos * sin_c)

    def project(r, which, with_q):
        rows = 3 * WIDE if with_q else 2 * WIDE
        tokens = a_all[r, pl.ds(2 * which, 2)].reshape(CHIP, HID)
        y_sc[0:rows] = nt_dot(w_sc[0:rows // HEAD].reshape(rows, HID), tokens)
        for lt in range(CHIP // 128):
            cols = pl.ds(pl.multiple_of(which * CHIP + lt * 128, 128), 128)
            ycols = slice(lt * 128, lt * 128 + 128)
            for h in range(LOCAL):
                for half in range(2):
                    cos = ctab[16 * half:16 * half + 16, cols]
                    sin = stab[16 * half:16 * half + 16, cols]

                    def rotated(base):
                        u0 = base + h * HEAD + half * 32
                        b0 = half * 32
                        bias = b_sc.at[base // HEAD + h]
                        u = (y_sc[u0:u0 + 16, ycols] + bias[b0:b0 + 16]).astype(BF16).astype(F32)
                        w = (y_sc[u0 + 16:u0 + 32, ycols] + bias[b0 + 16:b0 + 32]).astype(BF16).astype(F32)
                        return (u * cos - w * sin).astype(BF16), (w * cos + u * sin).astype(BF16)

                    k0 = h * HEAD + half * 32
                    ku, kw = rotated(0)
                    kt[k0:k0 + 16, cols] = ku
                    kt[k0 + 16:k0 + 32, cols] = kw
                    if with_q:
                        qu, qw = rotated(2 * WIDE)
                        q0 = (h % 2) * HEAD + half * 32
                        qc = slice((h % 2) * CHIP + lt * 128, (h % 2) * CHIP + lt * 128 + 128)
                        qbd[h // 2, q0:q0 + 16, qc] = qu
                        qbd[h // 2, q0 + 16:q0 + 32, qc] = qw
                v0 = WIDE + h * HEAD
                vt[h * HEAD:(h + 1) * HEAD, cols] = (y_sc[v0:v0 + HEAD, ycols] + b_sc[6 + h]).astype(BF16)

    def attend(r, this_chip):
        spec = ((768, 256), (768, 256)) if this_chip == 0 else ((768, 512), (1024, 768))

        def score(pair, j):
            for qb in range(2):
                key_len, mask_from = spec[qb]
                q0 = j * CHIP + qb * PART
                scores = jnp.dot(kk[pair, 0:key_len, :], qbd[pair, :, q0:q0 + PART], preferred_element_type=F32)
                q_pos = this_chip * CHIP + qb * PART + lax.broadcasted_iota(jnp.int32, (1, PART), 1)
                limit = jnp.maximum(q_pos, ctx_ref[r] - 1)
                top = None
                for k0 in range(0, key_len, CHUNK):
                    part = scores[k0:k0 + CHUNK]
                    if k0 >= mask_from:
                        k_pos = k0 + lax.broadcasted_iota(jnp.int32, (CHUNK, PART), 0)
                        part = jnp.where(k_pos <= limit, part, -jnp.inf)
                    s_refs[2 * j + qb][k0:k0 + CHUNK] = part
                    peak = jnp.max(part.reshape(CHUNK // 8, 8, PART), axis=0)
                    top = peak if top is None else jnp.maximum(top, peak)
                top_sc[2 * j + qb] = jnp.broadcast_to(jnp.max(top, axis=0, keepdims=True) * EXP_SCALE, (8, PART))

        def weigh(j):
            for qb in range(2):
                key_len = spec[qb][0]
                top = top_sc[2 * j + qb, 0:1]
                total = jnp.zeros((8, PART), F32)
                for k0 in range(0, key_len, CHUNK):
                    prob = jnp.exp2(s_refs[2 * j + qb][k0:k0 + CHUNK] * EXP_SCALE - top)
                    total = total + jnp.sum(prob.reshape(CHUNK // 8, 8, PART), axis=0)
                    p_refs[2 * j + qb][k0:k0 + CHUNK] = prob.astype(BF16)
                inv_sc[2 * j + qb] = jnp.broadcast_to(1.0 / jnp.sum(total, axis=0, keepdims=True), (8, PART))

        def mix(pair, j):
            v_rows = pl.ds(pl.multiple_of((2 * pair + j) * HEAD, HEAD), HEAD)
            for qb in range(2):
                key_len = spec[qb][0]
                mixed = jnp.dot(vt[v_rows, 0:key_len], p_refs[2 * j + qb][0:key_len], preferred_element_type=F32)
                ctx_buf[r, qb, v_rows, :] = (mixed * inv_sc[2 * j + qb, 0:1]).astype(BF16)

        score(0, 0)
        score(0, 1)
        weigh(0)

        def one_pair(pair, c):
            score(pair + 1, 0)
            weigh(1)
            mix(pair, 0)
            score(pair + 1, 1)
            weigh(0)
            mix(pair, 1)
            return c

        lax.fori_loop(0, LOCAL // 2 - 1, one_pair, 0)
        weigh(1)
        mix(LOCAL // 2 - 1, 0)
        mix(LOCAL // 2 - 1, 1)

    def dense(r):
        mixed = jnp.concatenate([ctx_buf[r, core], ctx_recv[r]], axis=0)
        dense_out = lax.dot_general(mixed, wd_sc[...], (((0,), (0,)), ((), ())), preferred_element_type=F32)
        normed = a_all[r, me].astype(F32)
        out_ref[0] = (normed * ALPHA + dense_out + bd_ref[...].astype(F32).reshape(1, HID)).astype(BF16)

    @pl.when(step > 0)
    def _():
        swap_ctx(step - 1).start()

    @pl.when(step < ROWS)
    def _():
        recv_x(step).wait_recv()
        relay(step).start()
        build_tables(step)
        recv_d(step).wait_recv()
        project(step, chip, True)

    @pl.when(step > 0)
    def _():
        swap_ctx(step - 1).wait_recv()
        dense(step - 1)

    @pl.when(step < ROWS)
    def _():
        recv_relay(step).wait_recv()
        project(step, other, False)
        ko_ref[0] = kt[0:192].reshape(3, HEAD, SEQ)
        vo_ref[0] = vt[0:192].reshape(3, HEAD, SEQ)
        for pair in range(LOCAL // 2):
            kk[pair] = kt[pair * 128:(pair + 1) * 128, :].T

    @pl.when(jnp.logical_and(step < ROWS, chip == 0))
    def _():
        attend(step, 0)

    @pl.when(jnp.logical_and(step < ROWS, chip == 1))
    def _():
        attend(step, 1)

    @pl.when(step == ROWS)
    def _():
        def drain(r, c):
            send_x(r).wait_send()
            send_d(r).wait_send()
            relay(r).wait_send()
            swap_ctx(r).wait_send()
            return c

        lax.fori_loop(0, ROWS, drain, 0)


def solution(mesh):
    seq_spec = P('dp', 'sp', None)
    row_spec = P('dp', 'sp')
    head_spec = P('dp', None, 'sp', None)
    replicated = P()
    tcos, tsin = rope_tables()

    def local_block(hidden, pos_ids, block_ids, ctx_len, ln_gamma, ln_beta, w_qkv, b_qkv, w_dense, b_dense):
        w_t = jnp.transpose(w_qkv, (1, 2, 3, 0))
        anywhere = pl.BlockSpec(memory_space=pl.ANY)

        def whole(shape):
            return pl.BlockSpec(shape, lambda i: (0,) * len(shape))

        out, keys_t, values_t = pl.pallas_call(
            kernel,
            grid=(ROWS + 1,),
            out_shape=(
                jax.ShapeDtypeStruct((ROWS, PART, HID), BF16),
                jax.ShapeDtypeStruct((ROWS, 3, HEAD, SEQ), BF16),
                jax.ShapeDtypeStruct((ROWS, 3, HEAD, SEQ), BF16),
            ),
            in_specs=[
                anywhere, whole((ROWS, PART)), pl.BlockSpec(memory_space=pltpu.SMEM),
                whole((HID,)), whole((HID,)), whole((HID,)),
                anywhere, whole((12, 3, HEAD)), anywhere, whole((16, SEQ)), whole((16, SEQ)),
            ],
            out_specs=(
                pl.BlockSpec((1, PART, HID), lambda i: (jnp.maximum(i - 1, 0), 0, 0)),
                pl.BlockSpec((1, 3, HEAD, SEQ), lambda i: (jnp.minimum(i, ROWS - 1), 0, 0, 0)),
                pl.BlockSpec((1, 3, HEAD, SEQ), lambda i: (jnp.minimum(i, ROWS - 1), 0, 0, 0)),
            ),
            scratch_shapes=[
                pltpu.VMEM((ROWS, 4, PART, HID), BF16),
                pltpu.VMEM((4, ROWS, 128), jnp.int32),
                pltpu.VMEM((18, HEAD, HID), BF16),
                pltpu.VMEM((18, HEAD, 128), F32),
                pltpu.VMEM((HID, HID), BF16),
                pltpu.VMEM((3 * WIDE, CHIP), F32),
                pltpu.VMEM((WIDE, SEQ), BF16),
                pltpu.VMEM((WIDE, SEQ), BF16),
                pltpu.VMEM((3, SEQ, 128), BF16),
                pltpu.VMEM((3, 128, 2 * CHIP), BF16),
                pltpu.VMEM((32, SEQ), F32),
                pltpu.VMEM((32, SEQ), F32),
                *[pltpu.VMEM((SEQ, PART), F32)] * 4,
                *[pltpu.VMEM((SEQ, PART), BF16)] * 4,
                pltpu.VMEM((4, 8, PART), F32),
                pltpu.VMEM((4, 8, PART), F32),
                pltpu.VMEM((ROWS, 2, WIDE, PART), BF16),
                pltpu.VMEM((ROWS, WIDE, PART), BF16),
                pltpu.SemaphoreType.DMA((ROWS,)),
                pltpu.SemaphoreType.DMA((22,)),
            ] + [pltpu.SemaphoreType.DMA((ROWS,))] * 8 + [pltpu.SemaphoreType.DMA((3,))] * 2,
            compiler_params=pltpu.CompilerParams(
                collective_id=0, has_side_effects=True, vmem_limit_bytes=62 * 1024 * 1024, dimension_semantics=('arbitrary',)),
            name='glm_block',
        )(hidden, pos_ids, ctx_len, ln_gamma, ln_beta, b_dense,
          w_t, b_qkv, w_dense, jnp.asarray(tcos), jnp.asarray(tsin))
        return out, jnp.transpose(keys_t, (0, 3, 1, 2)), jnp.transpose(values_t, (0, 3, 1, 2))

    return jax.shard_map(local_block, mesh=mesh, in_specs=(seq_spec, row_spec, row_spec, P('dp'), replicated, replicated, replicated, replicated, replicated, replicated), out_specs=(seq_spec, head_spec, head_spec), check_vma=False)
```

```python
import functools
import math

import jax
import jax.numpy as jnp
import numpy as np
from jax import lax
from jax.experimental import pallas as pl
from jax.experimental.pallas import tpu as pltpu
from jax.sharding import PartitionSpec as P

ALPHA = math.sqrt(56.0)
ROPE_BASE = 10000.0
LN_EPS = 1e-5
MESH = pl.DeviceIdType.MESH
F32 = jnp.float32
BF16 = jnp.bfloat16

ROWS = 16
PART = 256
SEQ = 1024
HID = 768
HEAD = 64
CHIP = 512
LOCAL = 6
WIDE = LOCAL * HEAD
EXP_SCALE = math.log2(math.e) / math.sqrt(HEAD)
CHUNK = 64


def rope_tables():
    freq = ROPE_BASE ** (-np.arange(0, 32, 2).astype(np.float64) / 32.0)
    angle = freq.astype(np.float32)[:, None] * np.arange(SEQ, dtype=np.float32)[None, :]
    return np.cos(angle.astype(np.float64)).astype(np.float32), np.sin(angle.astype(np.float64)).astype(np.float32)


def nt_dot(a, b):
    return lax.dot_general(a, b, (((1,), (1,)), ((), ())), preferred_element_type=F32)


def kernel(hid_hbm, pos_ref, ctx_ref, gamma_ref, beta_ref, bd_ref, w_hbm, bias_ref, wd_hbm, tcos_ref, tsin_ref,
           out_ref, ko_ref, vo_ref,
           own, xbuf, dbuf, rbuf, posr, w_sc, b_sc, wd_sc, y_0, y_1, kt, vt, kk, qbd, ctab, stab, s_0, s_1, s_2, s_3, p_0, p_1, p_2, p_3, top_sc, inv_sc, ctx_buf, ctx_recv,
           hid_sem, w_sem, xs_sem, xr_sem, ds_sem, dr_sem, rs_sem, rr_sem, cs_sem, cr_sem, ps_sem, pr_sem):
    step = pl.program_id(0)
    s_refs, p_refs = (s_0, s_1, s_2, s_3), (p_0, p_1, p_2, p_3)
    me = lax.axis_index('sp')
    core = lax.rem(me, 2)
    chip = me // 2
    other = 1 - chip
    peer_x = other * 2 + core
    peer_d = chip * 2 + 1 - core
    peer_xd = other * 2 + 1 - core

    def remote(src, dst, send_sem, recv_sem, peer):
        return pltpu.make_async_remote_copy(src, dst, send_sem, recv_sem, device_id={'sp': peer}, device_id_type=MESH)

    def send_x(r):
        return remote(own.at[r], xbuf.at[r], xs_sem.at[r], xr_sem.at[r], peer_x)

    def send_d(r):
        return remote(own.at[r], dbuf.at[lax.rem(r, 2)], ds_sem.at[r], dr_sem.at[r], peer_d)

    def relay(r):
        return remote(xbuf.at[r], rbuf.at[lax.rem(r, 2)], rs_sem.at[r], rr_sem.at[r], peer_d)

    def swap_ctx(r):
        return remote(ctx_buf.at[lax.rem(r, 2), 1 - core], ctx_recv.at[lax.rem(r, 2)], cs_sem.at[r], cr_sem.at[r], peer_d)

    def swap_pos(n, peer):
        return remote(pos_ref.at[:, pl.ds(128, 128)], posr.at[me], ps_sem.at[n], pr_sem.at[n], peer)

    def recv_pos(n, peer):
        return remote(pos_ref.at[:, pl.ds(128, 128)], posr.at[peer], ps_sem.at[n], pr_sem.at[n], peer)

    def load_hidden(r):
        return pltpu.make_async_copy(hid_hbm.at[r], own.at[r], hid_sem.at[r])

    def weight_copies():
        copies = []
        for group, owner in enumerate((me, peer_x)):
            for slot, kind in ((0, 1), (6, 2), (12, 0)):
                for h in range(3):
                    copies.append((w_hbm.at[owner * 3 + h, kind], w_sc.at[slot + 3 * group + h]))
        for slot, owner in enumerate((me, peer_x, peer_d, peer_xd)):
            copies.append((wd_hbm.at[pl.ds(pl.multiple_of(owner * 192, 64), 192)], wd_sc.at[pl.ds(slot * 192, 192)]))
        return [pltpu.make_async_copy(src, dst, w_sem.at[i]) for i, (src, dst) in enumerate(copies)]

    def norm_row(r):
        gamma = gamma_ref[...].astype(F32).reshape(1, HID)
        beta = beta_ref[...].astype(F32).reshape(1, HID)
        for t in range(0, PART, 32):
            wide = own[r, pl.ds(t, 32), :].astype(F32)
            mean = jnp.sum(wide, axis=-1, keepdims=True) * (1.0 / HID)
            cent = wide - mean
            var = jnp.sum(cent * cent, axis=-1, keepdims=True) * (1.0 / HID)
            own[r, pl.ds(t, 32), :] = (cent * lax.rsqrt(var + LN_EPS) * gamma + beta).astype(BF16)

    def spread_bias():
        for group, owner in enumerate((me, peer_x)):
            for slot, kind in ((0, 1), (6, 2), (12, 0)):
                for h in range(3):
                    row = bias_ref[owner * 3 + h, kind:kind + 1, :].astype(F32)
                    b_sc[slot + 3 * group + h] = jnp.broadcast_to(row, (128, HEAD)).T

    @pl.when(step == 0)
    def _():
        def fetch(r, c):
            load_hidden(r).start()
            return c

        lax.fori_loop(0, ROWS, fetch, 0)
        for c in weight_copies():
            c.start()
        barrier = pltpu.get_barrier_semaphore()
        for peer in (peer_x, peer_d, peer_xd):
            pl.semaphore_signal(barrier, inc=1, device_id={'sp': peer}, device_id_type=MESH)
        pl.semaphore_wait(barrier, 3)
        for n, peer in enumerate((peer_x, peer_d, peer_xd)):
            swap_pos(n, peer).start()
        posr[me] = pos_ref[:, 128:256]

        def norm_and_send(r, c):
            load_hidden(r).wait()
            norm_row(r)

            @pl.when(r > 0)
            def _():
                send_x(r - 1).start()

            return c

        lax.fori_loop(0, ROWS, norm_and_send, 0)
        send_d(0).start()
        qbd[...] = jnp.zeros_like(qbd)
        spread_bias()
        for c in weight_copies():
            c.wait()
        for n, peer in enumerate((peer_x, peer_d, peer_xd)):
            recv_pos(n, peer).wait()
        send_x(ROWS - 1).start()

    def build_tables(r):
        tcos = tcos_ref[...]
        tsin = tsin_ref[...]
        lane = lax.broadcasted_iota(jnp.int32, (16, SEQ), 1)
        ctx = ctx_ref[r]
        last = posr[3, pl.ds(r, 1), :]
        last_lane = lax.broadcasted_iota(jnp.int32, (1, 128), 1)
        m_pos = jnp.sum(jnp.where(last_lane == 127, last, 0), axis=1, keepdims=True)

        def pick(table, hit):
            return jnp.sum(jnp.where(hit, table, 0.0), axis=1, keepdims=True)

        at_m = lane == m_pos
        at_c = lane == ctx - 1
        in_ctx = lane < ctx
        cos_c, sin_c = pick(tcos, at_c), pick(tsin, at_c)
        ctab[0:16] = jnp.where(in_ctx, tcos, pick(tcos, at_m))
        stab[0:16] = jnp.where(in_ctx, tsin, pick(tsin, at_m))
        ctab[16:32] = jnp.where(in_ctx, 1.0, tcos * cos_c + tsin * sin_c)
        stab[16:32] = jnp.where(in_ctx, 0.0, tsin * cos_c - tcos * sin_c)

    def multiply(y_ref, tokens, rows):
        y_ref[0:rows] = nt_dot(w_sc[0:rows // HEAD].reshape(rows, HID), tokens)

    def finish(y_ref, part, with_q):
        for lt in range(PART // 128):
            cols = pl.ds(pl.multiple_of(part * PART + lt * 128, 128), 128)
            ycols = slice(lt * 128, lt * 128 + 128)
            for h in range(LOCAL):
                for half in range(2):
                    cos = ctab[16 * half:16 * half + 16, cols]
                    sin = stab[16 * half:16 * half + 16, cols]

                    def rotated(base):
                        u0 = base + h * HEAD + half * 32
                        b0 = half * 32
                        bias = b_sc.at[base // HEAD + h]
                        u = (y_ref[u0:u0 + 16, ycols] + bias[b0:b0 + 16]).astype(BF16).astype(F32)
                        w = (y_ref[u0 + 16:u0 + 32, ycols] + bias[b0 + 16:b0 + 32]).astype(BF16).astype(F32)
                        return (u * cos - w * sin).astype(BF16), (w * cos + u * sin).astype(BF16)

                    k0 = h * HEAD + half * 32
                    ku, kw = rotated(0)
                    kt[k0:k0 + 16, cols] = ku
                    kt[k0 + 16:k0 + 32, cols] = kw
                    if with_q:
                        qu, qw = rotated(2 * WIDE)
                        q0 = (h % 2) * HEAD + half * 32
                        qc = pl.ds(pl.multiple_of((h % 2) * CHIP + lax.rem(part, 2) * PART + lt * 128, 128), 128)
                        qbd[h // 2, q0:q0 + 16, qc] = qu
                        qbd[h // 2, q0 + 16:q0 + 32, qc] = qw
                v0 = WIDE + h * HEAD
                vt[h * HEAD:(h + 1) * HEAD, cols] = (y_ref[v0:v0 + HEAD, ycols] + b_sc[6 + h]).astype(BF16)

    def project(first, first_part, second, second_part, with_q):
        rows = 3 * WIDE if with_q else 2 * WIDE
        multiply(y_0, first, rows)
        multiply(y_1, second, rows)
        finish(y_0, first_part, with_q)
        finish(y_1, second_part, with_q)

    def attend(r, this_chip):
        spec = ((768, 256), (768, 256)) if this_chip == 0 else ((768, 512), (1024, 768))

        def score(pair, j):
            for qb in range(2):
                key_len, mask_from = spec[qb]
                q0 = j * CHIP + qb * PART
                scores = jnp.dot(kk[pair, 0:key_len, :], qbd[pair, :, q0:q0 + PART], preferred_element_type=F32)
                q_pos = this_chip * CHIP + qb * PART + lax.broadcasted_iota(jnp.int32, (1, PART), 1)
                limit = jnp.maximum(q_pos, ctx_ref[r] - 1)
                top = None
                for k0 in range(0, key_len, CHUNK):
                    part = scores[k0:k0 + CHUNK]
                    if k0 >= mask_from:
                        k_pos = k0 + lax.broadcasted_iota(jnp.int32, (CHUNK, PART), 0)
                        part = jnp.where(k_pos <= limit, part, -jnp.inf)
                    s_refs[2 * j + qb][k0:k0 + CHUNK] = part
                    peak = jnp.max(part.reshape(CHUNK // 8, 8, PART), axis=0)
                    top = peak if top is None else jnp.maximum(top, peak)
                top_sc[2 * j + qb] = jnp.broadcast_to(jnp.max(top, axis=0, keepdims=True) * EXP_SCALE, (8, PART))

        def weigh(j):
            for qb in range(2):
                key_len = spec[qb][0]
                top = top_sc[2 * j + qb, 0:1]
                total = jnp.zeros((8, PART), F32)
                for k0 in range(0, key_len, CHUNK):
                    prob = jnp.exp2(s_refs[2 * j + qb][k0:k0 + CHUNK] * EXP_SCALE - top)
                    total = total + jnp.sum(prob.reshape(CHUNK // 8, 8, PART), axis=0)
                    p_refs[2 * j + qb][k0:k0 + CHUNK] = prob.astype(BF16)
                inv_sc[2 * j + qb] = jnp.broadcast_to(1.0 / jnp.sum(total, axis=0, keepdims=True), (8, PART))

        def mix(pair, j):
            v_rows = pl.ds(pl.multiple_of((2 * pair + j) * HEAD, HEAD), HEAD)
            for qb in range(2):
                key_len = spec[qb][0]
                mixed = jnp.dot(vt[v_rows, 0:key_len], p_refs[2 * j + qb][0:key_len], preferred_element_type=F32)
                ctx_buf[lax.rem(r, 2), qb, v_rows, :] = (mixed * inv_sc[2 * j + qb, 0:1]).astype(BF16)

        score(0, 0)
        score(0, 1)
        weigh(0)

        def one_pair(pair, c):
            score(pair + 1, 0)
            weigh(1)
            mix(pair, 0)
            score(pair + 1, 1)
            weigh(0)
            mix(pair, 1)
            return c

        lax.fori_loop(0, LOCAL // 2 - 1, one_pair, 0)
        weigh(1)
        mix(LOCAL // 2 - 1, 0)
        mix(LOCAL // 2 - 1, 1)

    def dense(r):
        mixed = jnp.concatenate([ctx_buf[lax.rem(r, 2), core], ctx_recv[lax.rem(r, 2)]], axis=0)
        dense_out = lax.dot_general(mixed, wd_sc[...], (((0,), (0,)), ((), ())), preferred_element_type=F32)
        normed = own[r].astype(F32)
        out_ref[r] = (normed * ALPHA + dense_out + bd_ref[...].astype(F32).reshape(1, HID)).astype(BF16)

    @pl.when(step > 0)
    def _():
        swap_ctx(step - 1).start()

    @pl.when(step < ROWS)
    def _():
        send_x(step).wait_recv()
        relay(step).start()
        build_tables(step)
        send_d(step).wait_recv()
        project(own[step], me, dbuf[lax.rem(step, 2)], peer_d, True)

    @pl.when(step > 0)
    def _():
        swap_ctx(step - 1).wait()
        dense(step - 1)

    @pl.when(step < ROWS)
    def _():
        relay(step).wait_recv()

    @pl.when(step < ROWS - 1)
    def _():
        send_d(step + 1).start()

    @pl.when(step < ROWS)
    def _():
        project(xbuf[step], peer_x, rbuf[lax.rem(step, 2)], peer_xd, False)
        ko_ref[step] = kt[0:192].reshape(3, HEAD, SEQ)
        vo_ref[step] = vt[0:192].reshape(3, HEAD, SEQ)
        for pair in range(LOCAL // 2):
            kk[pair] = kt[pair * 128:(pair + 1) * 128, :].T

    @pl.when(jnp.logical_and(step < ROWS, chip == 0))
    def _():
        attend(step, 0)

    @pl.when(jnp.logical_and(step < ROWS, chip == 1))
    def _():
        attend(step, 1)

    @pl.when(step == ROWS)
    def _():
        def drain(r, c):
            send_x(r).wait_send()
            send_d(r).wait_send()
            relay(r).wait_send()
            return c

        lax.fori_loop(0, ROWS, drain, 0)


def put(out_vm, keys_vm, values_vm, out_hbm, keys_hbm, values_hbm, sem):
    copies = [pltpu.make_async_copy(src, dst, sem.at[i]) for i, (src, dst) in enumerate(((out_vm, out_hbm), (keys_vm, keys_hbm), (values_vm, values_hbm)))]
    for c in copies:
        c.start()
    for c in copies:
        c.wait()


def solution(mesh):
    seq_spec = P('dp', 'sp', None)
    row_spec = P('dp', 'sp')
    head_spec = P('dp', None, 'sp', None)
    replicated = P()
    tcos, tsin = rope_tables()

    def local_block(hidden, pos_ids, block_ids, ctx_len, ln_gamma, ln_beta, w_qkv, b_qkv, w_dense, b_dense):
        w_t = jnp.transpose(w_qkv, (1, 2, 3, 0))
        anywhere = pl.BlockSpec(memory_space=pl.ANY)

        def whole(shape):
            return pl.BlockSpec(shape, lambda i: (0,) * len(shape))

        out, keys_t, values_t = pl.pallas_call(
            kernel,
            grid=(ROWS + 1,),
            out_shape=(
                pltpu.VMEM((ROWS, PART, HID), BF16),
                pltpu.VMEM((ROWS, 3, HEAD, SEQ), BF16),
                pltpu.VMEM((ROWS, 3, HEAD, SEQ), BF16),
            ),
            in_specs=[
                anywhere, whole((ROWS, PART)), pl.BlockSpec(memory_space=pltpu.SMEM),
                whole((HID,)), whole((HID,)), whole((HID,)),
                anywhere, whole((12, 3, HEAD)), anywhere, whole((16, SEQ)), whole((16, SEQ)),
            ],
            out_specs=(pl.BlockSpec(memory_space=pltpu.VMEM),) * 3,
            scratch_shapes=[
                pltpu.VMEM((ROWS, PART, HID), BF16),
                pltpu.VMEM((ROWS, PART, HID), BF16),
                pltpu.VMEM((2, PART, HID), BF16),
                pltpu.VMEM((2, PART, HID), BF16),
                pltpu.VMEM((4, ROWS, 128), jnp.int32),
                pltpu.VMEM((18, HEAD, HID), BF16),
                pltpu.VMEM((18, HEAD, 128), F32),
                pltpu.VMEM((HID, HID), BF16),
                pltpu.VMEM((3 * WIDE, PART), F32),
                pltpu.VMEM((3 * WIDE, PART), F32),
                pltpu.VMEM((WIDE, SEQ), BF16),
                pltpu.VMEM((WIDE, SEQ), BF16),
                pltpu.VMEM((3, SEQ, 128), BF16),
                pltpu.VMEM((3, 128, 2 * CHIP), BF16),
                pltpu.VMEM((32, SEQ), F32),
                pltpu.VMEM((32, SEQ), F32),
                *[pltpu.VMEM((SEQ, PART), F32)] * 4,
                *[pltpu.VMEM((SEQ, PART), BF16)] * 4,
                pltpu.VMEM((4, 8, PART), F32),
                pltpu.VMEM((4, 8, PART), F32),
                pltpu.VMEM((2, 2, WIDE, PART), BF16),
                pltpu.VMEM((2, WIDE, PART), BF16),
                pltpu.SemaphoreType.DMA((ROWS,)),
                pltpu.SemaphoreType.DMA((22,)),
            ] + [pltpu.SemaphoreType.DMA((ROWS,))] * 8 + [pltpu.SemaphoreType.DMA((3,))] * 2,
            compiler_params=pltpu.CompilerParams(
                collective_id=0, has_side_effects=True, vmem_limit_bytes=43 * 1024 * 1024, dimension_semantics=('arbitrary',)),
            name='glm_block',
        )(hidden, pos_ids, ctx_len, ln_gamma, ln_beta, b_dense,
          w_t, b_qkv, w_dense, jnp.asarray(tcos), jnp.asarray(tsin))
        held = [pltpu.with_memory_space_constraint(x, pltpu.VMEM) for x in (out, keys_t, values_t)]
        out, keys_t, values_t = pl.pallas_call(
            put,
            out_shape=[jax.ShapeDtypeStruct(x.shape, BF16) for x in held],
            in_specs=[pl.BlockSpec(memory_space=pl.ANY)] * 3,
            out_specs=[anywhere] * 3,
            scratch_shapes=[pltpu.SemaphoreType.DMA((3,))],
            compiler_params=pltpu.CompilerParams(vmem_limit_bytes=1024 * 1024),
            name='put',
        )(*held)
        return out, jnp.transpose(keys_t, (0, 3, 1, 2)), jnp.transpose(values_t, (0, 3, 1, 2))

    return jax.shard_map(local_block, mesh=mesh, in_specs=(seq_spec, row_spec, row_spec, P('dp'), replicated, replicated, replicated, replicated, replicated, replicated), out_specs=(seq_spec, head_spec, head_spec), check_vma=False)
```

```python
import functools
import math

import jax
import jax.numpy as jnp
import numpy as np
from jax import lax
from jax.experimental import pallas as pl
from jax.experimental.pallas import tpu as pltpu
from jax.sharding import PartitionSpec as P

ALPHA = math.sqrt(56.0)
ROPE_BASE = 10000.0
LN_EPS = 1e-5
MESH = pl.DeviceIdType.MESH
F32 = jnp.float32
BF16 = jnp.bfloat16

ROWS = 16
PART = 256
HALF = 128
SEQ = 1024
HID = 768
HEAD = 64
CHIP = 512
LOCAL = 6
WIDE = LOCAL * HEAD
EXP_SCALE = math.log2(math.e) / math.sqrt(HEAD)
CHUNK = 64
MIX = 256


def rope_tables():
    freq = ROPE_BASE ** (-np.arange(0, 32, 2).astype(np.float64) / 32.0)
    angle = freq.astype(np.float32)[:, None] * np.arange(SEQ, dtype=np.float32)[None, :]
    return np.cos(angle.astype(np.float64)).astype(np.float32), np.sin(angle.astype(np.float64)).astype(np.float32)


def nt_dot(a, b):
    return lax.dot_general(a, b, (((1,), (1,)), ((), ())), preferred_element_type=F32)


def kernel(hid_hbm, pos_hbm, ctx_ref, gamma_hbm, beta_hbm, bd_hbm, w_hbm, bias_hbm, wd_hbm, tcos_hbm, tsin_hbm,
           out_ref, ko_ref, vo_ref,
           pos_ref, gamma_ref, beta_ref, bd_ref, bias_ref, tcos_ref, tsin_ref, own, xbuf, dbuf, rbuf, posr, w_sc, b_sc, wd_sc, y_0, y_1, kt_0, kt_1, kt_2, vt, kk, qbd, ctab, stab, s_0, s_1, s_2, s_3, top_sc, ctx_buf, ctx_recv,
           t_sem, hid_sem, w_sem, xs_sem, xr_sem, ds_sem, dr_sem, rs_sem, rr_sem, cs_sem, cr_sem, ps_sem, pr_sem):
    step = pl.program_id(0)
    s_refs, kt_refs = (s_0, s_1, s_2, s_3), (kt_0, kt_1, kt_2)
    me = lax.axis_index('sp')
    core = lax.rem(me, 2)
    chip = me // 2
    other = 1 - chip
    peer_x = other * 2 + core
    peer_d = chip * 2 + 1 - core
    peer_xd = other * 2 + 1 - core

    def remote(src, dst, send_sem, recv_sem, peer):
        return pltpu.make_async_remote_copy(src, dst, send_sem, recv_sem, device_id={'sp': peer}, device_id_type=MESH)

    def piece(i):
        return lax.div(i, 2), pl.ds(pl.multiple_of(lax.rem(i, 2) * HALF, HALF), HALF)

    def send_x(i):
        r, rows = piece(i)
        return remote(own.at[r, rows], xbuf.at[r, rows], xs_sem.at[i], xr_sem.at[i], peer_x)

    def send_d(r):
        return remote(own.at[r], dbuf.at[lax.rem(r, 2)], ds_sem.at[r], dr_sem.at[r], peer_d)

    def relay(i):
        r, rows = piece(i)
        return remote(xbuf.at[r, rows], rbuf.at[lax.rem(r, 2), rows], rs_sem.at[i], rr_sem.at[i], peer_d)

    def swap_ctx(r):
        return remote(ctx_buf.at[lax.rem(r, 2), 1 - core], ctx_recv.at[lax.rem(r, 2)], cs_sem.at[r], cr_sem.at[r], peer_d)

    def swap_pos(n, peer):
        return remote(pos_ref.at[:, pl.ds(128, 128)], posr.at[me], ps_sem.at[n], pr_sem.at[n], peer)

    def recv_pos(n, peer):
        return remote(pos_ref.at[:, pl.ds(128, 128)], posr.at[peer], ps_sem.at[n], pr_sem.at[n], peer)

    def load_hidden(r):
        return pltpu.make_async_copy(hid_hbm.at[r], own.at[r], hid_sem.at[r])

    def small_copies():
        pairs = ((gamma_hbm, gamma_ref), (beta_hbm, beta_ref), (pos_hbm, pos_ref), (bd_hbm, bd_ref), (bias_hbm, bias_ref), (tcos_hbm, tcos_ref), (tsin_hbm, tsin_ref))
        return [pltpu.make_async_copy(src, dst, t_sem.at[i]) for i, (src, dst) in enumerate(pairs)]

    def weight_copies():
        copies = []
        for group, owner in enumerate((me, peer_x)):
            for slot, kind in ((0, 1), (6, 2), (12, 0)):
                for h in range(3):
                    copies.append((w_hbm.at[owner * 3 + h, kind], w_sc.at[slot + 3 * group + h]))
        for slot, owner in enumerate((me, peer_x, peer_d, peer_xd)):
            copies.append((wd_hbm.at[pl.ds(pl.multiple_of(owner * 192, 64), 192)], wd_sc.at[pl.ds(slot * 192, 192)]))
        return [pltpu.make_async_copy(src, dst, w_sem.at[i]) for i, (src, dst) in enumerate(copies)]

    def norm_piece(i):
        r, _ = piece(i)
        first = pl.multiple_of(lax.rem(i, 2) * HALF, HALF)
        gamma = gamma_ref[...].astype(F32).reshape(1, HID)
        beta = beta_ref[...].astype(F32).reshape(1, HID)
        for t in range(0, HALF, 32):
            rows = pl.ds(first + t, 32)
            wide = own[r, rows, :].astype(F32)
            mean = jnp.sum(wide, axis=-1, keepdims=True) * (1.0 / HID)
            cent = wide - mean
            var = jnp.sum(cent * cent, axis=-1, keepdims=True) * (1.0 / HID)
            own[r, rows, :] = (cent * lax.rsqrt(var + LN_EPS) * gamma + beta).astype(BF16)

    def spread_bias():
        for group, owner in enumerate((me, peer_x)):
            for slot, kind in ((0, 1), (6, 2), (12, 0)):
                for h in range(3):
                    row = bias_ref[owner * 3 + h, kind:kind + 1, :].astype(F32)
                    b_sc[slot + 3 * group + h] = jnp.broadcast_to(row, (128, HEAD)).T

    @pl.when(step == 0)
    def _():
        small = small_copies()
        for c in small[:2]:
            c.start()

        def fetch(r, c):
            load_hidden(r).start()
            return c

        lax.fori_loop(0, ROWS, fetch, 0)
        barrier = pltpu.get_barrier_semaphore()
        for peer in (peer_x, peer_d, peer_xd):
            pl.semaphore_signal(barrier, inc=1, device_id={'sp': peer}, device_id_type=MESH)
        for c in small[2:] + weight_copies():
            c.start()
        for c in small[:2]:
            c.wait()
        load_hidden(0).wait()
        norm_piece(0)
        pl.semaphore_wait(barrier, 3)

        def norm_and_send(i, c):
            @pl.when(lax.rem(i, 2) == 0)
            def _():
                load_hidden(lax.div(i, 2)).wait()

            norm_piece(i)
            send_x(i - 1).start()
            return c

        lax.fori_loop(1, 2 * ROWS, norm_and_send, 0)
        for c in small[2:]:
            c.wait()
        for n, peer in enumerate((peer_x, peer_d, peer_xd)):
            swap_pos(n, peer).start()
        send_d(0).start()
        posr[me] = pos_ref[:, 128:256]
        qbd[...] = jnp.zeros_like(qbd)
        spread_bias()
        for c in weight_copies():
            c.wait()
        for n, peer in enumerate((peer_x, peer_d, peer_xd)):
            recv_pos(n, peer).wait()
        send_x(2 * ROWS - 1).start()

    def build_tables(r):
        tcos = tcos_ref[...]
        tsin = tsin_ref[...]
        lane = lax.broadcasted_iota(jnp.int32, (16, SEQ), 1)
        ctx = ctx_ref[r]
        last = posr[3, pl.ds(r, 1), :]
        last_lane = lax.broadcasted_iota(jnp.int32, (1, 128), 1)
        m_pos = jnp.sum(jnp.where(last_lane == 127, last, 0), axis=1, keepdims=True)

        def pick(table, hit):
            return jnp.sum(jnp.where(hit, table, 0.0), axis=1, keepdims=True)

        at_m = lane == m_pos
        at_c = lane == ctx - 1
        in_ctx = lane < ctx
        cos_c, sin_c = pick(tcos, at_c), pick(tsin, at_c)
        ctab[0:16] = jnp.where(in_ctx, tcos, pick(tcos, at_m))
        stab[0:16] = jnp.where(in_ctx, tsin, pick(tsin, at_m))
        ctab[16:32] = jnp.where(in_ctx, 1.0, tcos * cos_c + tsin * sin_c)
        stab[16:32] = jnp.where(in_ctx, 0.0, tsin * cos_c - tcos * sin_c)

    def multiply(y_ref, tokens, rows):
        y_ref[0:rows] = nt_dot(w_sc[0:rows // HEAD].reshape(rows, HID), tokens)

    def finish(y_ref, part, with_q):
        for h in range(LOCAL):
            for lt in range(PART // 128):
                cols = pl.ds(pl.multiple_of(part * PART + lt * 128, 128), 128)
                ycols = slice(lt * 128, lt * 128 + 128)
                for half in range(2):
                    cos = ctab[16 * half:16 * half + 16, cols]
                    sin = stab[16 * half:16 * half + 16, cols]

                    def rotated(base):
                        u0 = base + h * HEAD + half * 32
                        b0 = half * 32
                        bias = b_sc.at[base // HEAD + h]
                        u = (y_ref[u0:u0 + 16, ycols] + bias[b0:b0 + 16]).astype(BF16).astype(F32)
                        w = (y_ref[u0 + 16:u0 + 32, ycols] + bias[b0 + 16:b0 + 32]).astype(BF16).astype(F32)
                        return (u * cos - w * sin).astype(BF16), (w * cos + u * sin).astype(BF16)

                    k0 = (h % 2) * HEAD + half * 32
                    ku, kw = rotated(0)
                    kt_refs[h // 2][k0:k0 + 16, cols] = ku
                    kt_refs[h // 2][k0 + 16:k0 + 32, cols] = kw
                    if with_q:
                        qu, qw = rotated(2 * WIDE)
                        q0 = (h % 2) * HEAD + half * 32
                        qc = pl.ds(pl.multiple_of((h % 2) * CHIP + lax.rem(part, 2) * PART + lt * 128, 128), 128)
                        qbd[h // 2, q0:q0 + 16, qc] = qu
                        qbd[h // 2, q0 + 16:q0 + 32, qc] = qw
                v0 = WIDE + h * HEAD
                vt[h * HEAD:(h + 1) * HEAD, cols] = (y_ref[v0:v0 + HEAD, ycols] + b_sc[6 + h]).astype(BF16)

    def project(first, first_part, second, second_part, with_q):
        rows = 3 * WIDE if with_q else 2 * WIDE
        multiply(y_0, first, rows)
        multiply(y_1, second, rows)
        finish(y_0, first_part, with_q)
        finish(y_1, second_part, with_q)

    def attend(r, this_chip):
        spec = ((768, 256), (768, 256)) if this_chip == 0 else ((768, 512), (1024, 768))

        def score(pair, j):
            for qb in range(2):
                key_len, mask_from = spec[qb]
                q0 = j * CHIP + qb * PART
                scores = jnp.dot(kk[pair, 0:key_len, :], qbd[pair, :, q0:q0 + PART], preferred_element_type=F32)
                q_pos = this_chip * CHIP + qb * PART + lax.broadcasted_iota(jnp.int32, (1, PART), 1)
                limit = jnp.maximum(q_pos, ctx_ref[r] - 1)
                top = None
                for k0 in range(0, key_len, CHUNK):
                    part = scores[k0:k0 + CHUNK]
                    if k0 >= mask_from:
                        k_pos = k0 + lax.broadcasted_iota(jnp.int32, (CHUNK, PART), 0)
                        part = jnp.where(k_pos <= limit, part, -jnp.inf)
                    s_refs[2 * j + qb][k0:k0 + CHUNK] = part
                    peak = jnp.max(part.reshape(CHUNK // 8, 8, PART), axis=0)
                    top = peak if top is None else jnp.maximum(top, peak)
                top_sc[2 * j + qb] = jnp.broadcast_to(jnp.max(top, axis=0, keepdims=True) * EXP_SCALE, (8, PART))

        def mix(pair, j):
            v_rows = pl.ds(pl.multiple_of((2 * pair + j) * HEAD, HEAD), HEAD)
            for qb in range(2):
                top = top_sc[2 * j + qb, 0:1]
                total = jnp.zeros((8, PART), F32)
                mixed = None
                for k0 in range(0, spec[qb][0], MIX):
                    probs = []
                    for k1 in range(k0, k0 + MIX, CHUNK):
                        prob = jnp.exp2(s_refs[2 * j + qb][k1:k1 + CHUNK] * EXP_SCALE - top)
                        total = total + jnp.sum(prob.reshape(CHUNK // 8, 8, PART), axis=0)
                        probs.append(prob.astype(BF16))
                    some = jnp.dot(vt[v_rows, k0:k0 + MIX], jnp.concatenate(probs, axis=0), preferred_element_type=F32)
                    mixed = some if mixed is None else mixed + some
                inv = 1.0 / jnp.sum(total, axis=0, keepdims=True)
                ctx_buf[lax.rem(r, 2), qb, v_rows, :] = (mixed * inv).astype(BF16)

        score(0, 0)

        def one_pair(pair, c):
            score(pair, 1)
            mix(pair, 0)
            score(pair + 1, 0)
            mix(pair, 1)
            return c

        lax.fori_loop(0, LOCAL // 2 - 1, one_pair, 0)
        score(LOCAL // 2 - 1, 1)
        mix(LOCAL // 2 - 1, 0)
        mix(LOCAL // 2 - 1, 1)

    def dense(r):
        mixed = jnp.concatenate([ctx_buf[lax.rem(r, 2), core], ctx_recv[lax.rem(r, 2)]], axis=0)
        dense_out = lax.dot_general(mixed, wd_sc[...], (((0,), (0,)), ((), ())), preferred_element_type=F32)
        normed = own[r].astype(F32)
        out_ref[r] = (normed * ALPHA + dense_out + bd_ref[...].astype(F32).reshape(1, HID)).astype(BF16)

    @pl.when(step > 0)
    def _():
        swap_ctx(step - 1).start()

    @pl.when(step < ROWS)
    def _():
        for n in range(2):
            send_x(2 * step + n).wait_recv()
            relay(2 * step + n).start()
        build_tables(step)
        send_d(step).wait_recv()
        project(own[step], me, dbuf[lax.rem(step, 2)], peer_d, True)

    @pl.when(step > 0)
    def _():
        swap_ctx(step - 1).wait()
        dense(step - 1)

    @pl.when(step < ROWS)
    def _():
        for n in range(2):
            relay(2 * step + n).wait_recv()

    @pl.when(step < ROWS - 1)
    def _():
        send_d(step + 1).start()

    @pl.when(step < ROWS)
    def _():
        multiply(y_0, xbuf[step], 2 * WIDE)
        multiply(y_1, rbuf[lax.rem(step, 2)], 2 * WIDE)

    def rest(r, this_chip):
        finish(y_0, peer_x, False)
        finish(y_1, peer_xd, False)
        ko_ref[r, 0:2] = kt_0[...].reshape(2, HEAD, SEQ)
        ko_ref[r, 2] = kt_1[0:HEAD]
        vo_ref[r] = vt[0:192].reshape(3, HEAD, SEQ)
        for pair in range(LOCAL // 2):
            kk[pair] = kt_refs[pair][...].T
        attend(r, this_chip)

    for this_chip in range(2):
        @pl.when(jnp.logical_and(step < ROWS, chip == this_chip))
        def _():
            rest(step, this_chip)

    @pl.when(step == ROWS)
    def _():
        def drain(r, c):
            for n in range(2):
                send_x(2 * r + n).wait_send()
                relay(2 * r + n).wait_send()
            send_d(r).wait_send()
            return c

        lax.fori_loop(0, ROWS, drain, 0)


def put(out_vm, keys_vm, values_vm, out_hbm, keys_hbm, values_hbm, sem):
    copies = [pltpu.make_async_copy(src, dst, sem.at[i]) for i, (src, dst) in enumerate(((out_vm, out_hbm), (keys_vm, keys_hbm), (values_vm, values_hbm)))]
    for c in copies:
        c.start()
    for c in copies:
        c.wait()


def solution(mesh):
    seq_spec = P('dp', 'sp', None)
    row_spec = P('dp', 'sp')
    head_spec = P('dp', None, 'sp', None)
    replicated = P()
    tcos, tsin = rope_tables()

    def local_block(hidden, pos_ids, block_ids, ctx_len, ln_gamma, ln_beta, w_qkv, b_qkv, w_dense, b_dense):
        w_t = jnp.transpose(w_qkv, (1, 2, 3, 0))
        anywhere = pl.BlockSpec(memory_space=pl.ANY)

        out, keys_t, values_t = pl.pallas_call(
            kernel,
            grid=(ROWS + 1,),
            out_shape=(
                pltpu.VMEM((ROWS, PART, HID), BF16),
                pltpu.VMEM((ROWS, 3, HEAD, SEQ), BF16),
                pltpu.VMEM((ROWS, 3, HEAD, SEQ), BF16),
            ),
            in_specs=[anywhere, anywhere, pl.BlockSpec(memory_space=pltpu.SMEM)] + [anywhere] * 8,
            out_specs=(pl.BlockSpec(memory_space=pltpu.VMEM),) * 3,
            scratch_shapes=[
                pltpu.VMEM((ROWS, PART), jnp.int32),
                pltpu.VMEM((HID,), BF16),
                pltpu.VMEM((HID,), BF16),
                pltpu.VMEM((HID,), BF16),
                pltpu.VMEM((12, 3, HEAD), BF16),
                pltpu.VMEM((16, SEQ), F32),
                pltpu.VMEM((16, SEQ), F32),
                pltpu.VMEM((ROWS, PART, HID), BF16),
                pltpu.VMEM((ROWS, PART, HID), BF16),
                pltpu.VMEM((2, PART, HID), BF16),
                pltpu.VMEM((2, PART, HID), BF16),
                pltpu.VMEM((4, ROWS, 128), jnp.int32),
                pltpu.VMEM((18, HEAD, HID), BF16),
                pltpu.VMEM((18, HEAD, 128), F32),
                pltpu.VMEM((HID, HID), BF16),
                pltpu.VMEM((3 * WIDE, PART), F32),
                pltpu.VMEM((3 * WIDE, PART), F32),
                *[pltpu.VMEM((2 * HEAD, SEQ), BF16)] * 3,
                pltpu.VMEM((WIDE, SEQ), BF16),
                pltpu.VMEM((3, SEQ, 128), BF16),
                pltpu.VMEM((3, 128, 2 * CHIP), BF16),
                pltpu.VMEM((32, SEQ), F32),
                pltpu.VMEM((32, SEQ), F32),
                *[pltpu.VMEM((SEQ, PART), F32)] * 4,
                pltpu.VMEM((4, 8, PART), F32),
                pltpu.VMEM((2, 2, WIDE, PART), BF16),
                pltpu.VMEM((2, WIDE, PART), BF16),
                pltpu.SemaphoreType.DMA((7,)),
                pltpu.SemaphoreType.DMA((ROWS,)),
                pltpu.SemaphoreType.DMA((22,)),
            ] + [pltpu.SemaphoreType.DMA((n * ROWS,)) for n in (2, 2, 1, 1, 2, 2, 1, 1)] + [pltpu.SemaphoreType.DMA((3,))] * 2,
            compiler_params=pltpu.CompilerParams(
                collective_id=0, has_side_effects=True, vmem_limit_bytes=43 * 1024 * 1024, dimension_semantics=('arbitrary',)),
            name='glm_block',
        )(hidden, pos_ids, ctx_len, ln_gamma, ln_beta, b_dense,
          w_t, b_qkv, w_dense, jnp.asarray(tcos), jnp.asarray(tsin))
        held = [pltpu.with_memory_space_constraint(x, pltpu.VMEM) for x in (out, keys_t, values_t)]
        out, keys_t, values_t = pl.pallas_call(
            put,
            out_shape=[jax.ShapeDtypeStruct(x.shape, BF16) for x in held],
            in_specs=[pl.BlockSpec(memory_space=pl.ANY)] * 3,
            out_specs=[anywhere] * 3,
            scratch_shapes=[pltpu.SemaphoreType.DMA((3,))],
            compiler_params=pltpu.CompilerParams(vmem_limit_bytes=1024 * 1024),
            name='put',
        )(*held)
        return out, jnp.transpose(keys_t, (0, 3, 1, 2)), jnp.transpose(values_t, (0, 3, 1, 2))

    return jax.shard_map(local_block, mesh=mesh, in_specs=(seq_spec, row_spec, row_spec, P('dp'), replicated, replicated, replicated, replicated, replicated, replicated), out_specs=(seq_spec, head_spec, head_spec), check_vma=False)
```

```python
import functools
import math

import jax
import jax.numpy as jnp
import numpy as np
from jax import lax
from jax.experimental import pallas as pl
from jax.experimental.pallas import tpu as pltpu
from jax.sharding import PartitionSpec as P

ALPHA = math.sqrt(56.0)
ROPE_BASE = 10000.0
LN_EPS = 1e-5
MESH = pl.DeviceIdType.MESH
F32 = jnp.float32
BF16 = jnp.bfloat16

ROWS = 16
PART = 256
HALF = 128
AHEAD = 4
SEQ = 1024
HID = 768
HEAD = 64
CHIP = 512
LOCAL = 6
WIDE = LOCAL * HEAD
EXP_SCALE = math.log2(math.e) / math.sqrt(HEAD)
CHUNK = 64
MIX = 256


def rope_tables():
    freq = ROPE_BASE ** (-np.arange(0, 32, 2).astype(np.float64) / 32.0)
    angle = freq.astype(np.float32)[:, None] * np.arange(SEQ, dtype=np.float32)[None, :]
    return np.cos(angle.astype(np.float64)).astype(np.float32), np.sin(angle.astype(np.float64)).astype(np.float32)


def nt_dot(a, b):
    return lax.dot_general(a, b, (((1,), (1,)), ((), ())), preferred_element_type=F32)


def kernel(hid_hbm, pos_hbm, ctx_ref, gamma_hbm, beta_hbm, bd_hbm, w_hbm, bias_hbm, wd_hbm, tcos_hbm, tsin_hbm,
           out_ref, ko_ref, vo_ref,
           pos_ref, gamma_ref, beta_ref, bd_ref, bias_ref, tcos_ref, tsin_ref, own, xbuf, dbuf, rbuf, posr, w_sc, b_sc, wd_sc, y_0, y_1, kt_0, kt_1, kt_2, vt, kk, qbd, ctab, stab, s_0, s_1, s_2, s_3, top_sc, ctx_buf, ctx_recv,
           t_sem, hid_sem, w_sem, xs_sem, xr_sem, ds_sem, dr_sem, rs_sem, rr_sem, cs_sem, cr_sem, ps_sem, pr_sem):
    step = pl.program_id(0)
    s_refs, kt_refs = (s_0, s_1, s_2, s_3), (kt_0, kt_1, kt_2)
    me = lax.axis_index('sp')
    core = lax.rem(me, 2)
    chip = me // 2
    other = 1 - chip
    peer_x = other * 2 + core
    peer_d = chip * 2 + 1 - core
    peer_xd = other * 2 + 1 - core

    def remote(src, dst, send_sem, recv_sem, peer):
        return pltpu.make_async_remote_copy(src, dst, send_sem, recv_sem, device_id={'sp': peer}, device_id_type=MESH)

    def piece(i):
        return lax.div(i, 2), pl.ds(pl.multiple_of(lax.rem(i, 2) * HALF, HALF), HALF)

    def send_x(i):
        r, rows = piece(i)
        return remote(own.at[r, rows], xbuf.at[r, rows], xs_sem.at[i], xr_sem.at[i], peer_x)

    def send_d(r):
        return remote(own.at[r], dbuf.at[lax.rem(r, 2)], ds_sem.at[r], dr_sem.at[r], peer_d)

    def relay(i):
        r, rows = piece(i)
        return remote(xbuf.at[r, rows], rbuf.at[lax.rem(r, 2), rows], rs_sem.at[i], rr_sem.at[i], peer_d)

    def swap_ctx(r):
        return remote(ctx_buf.at[lax.rem(r, 2), 1 - core], ctx_recv.at[lax.rem(r, 2)], cs_sem.at[r], cr_sem.at[r], peer_d)

    def swap_pos(n, peer):
        return remote(pos_ref.at[:, pl.ds(128, 128)], posr.at[me], ps_sem.at[n], pr_sem.at[n], peer)

    def recv_pos(n, peer):
        return remote(pos_ref.at[:, pl.ds(128, 128)], posr.at[peer], ps_sem.at[n], pr_sem.at[n], peer)

    def load_hidden(r):
        return pltpu.make_async_copy(hid_hbm.at[r], own.at[r], hid_sem.at[r])

    def small_copies():
        pairs = ((gamma_hbm, gamma_ref), (beta_hbm, beta_ref), (pos_hbm, pos_ref), (bd_hbm, bd_ref), (bias_hbm, bias_ref), (tcos_hbm, tcos_ref), (tsin_hbm, tsin_ref))
        return [pltpu.make_async_copy(src, dst, t_sem.at[i]) for i, (src, dst) in enumerate(pairs)]

    def weight_copies():
        copies = []
        for group, owner in enumerate((me, peer_x)):
            for slot, kind in ((0, 1), (6, 2), (12, 0)):
                for h in range(3):
                    copies.append((w_hbm.at[owner * 3 + h, kind], w_sc.at[slot + 3 * group + h]))
        for slot, owner in enumerate((me, peer_x, peer_d, peer_xd)):
            copies.append((wd_hbm.at[pl.ds(pl.multiple_of(owner * 192, 64), 192)], wd_sc.at[pl.ds(slot * 192, 192)]))
        return [pltpu.make_async_copy(src, dst, w_sem.at[i]) for i, (src, dst) in enumerate(copies)]

    def norm_piece(i):
        r, _ = piece(i)
        first = pl.multiple_of(lax.rem(i, 2) * HALF, HALF)
        gamma = gamma_ref[...].astype(F32).reshape(1, HID)
        beta = beta_ref[...].astype(F32).reshape(1, HID)
        for t in range(0, HALF, 32):
            rows = pl.ds(first + t, 32)
            wide = own[r, rows, :].astype(F32)
            mean = jnp.sum(wide, axis=-1, keepdims=True) * (1.0 / HID)
            cent = wide - mean
            var = jnp.sum(cent * cent, axis=-1, keepdims=True) * (1.0 / HID)
            own[r, rows, :] = (cent * lax.rsqrt(var + LN_EPS) * gamma + beta).astype(BF16)

    def spread_bias():
        for group, owner in enumerate((me, peer_x)):
            for slot, kind in ((0, 1), (6, 2), (12, 0)):
                for h in range(3):
                    row = bias_ref[owner * 3 + h, kind:kind + 1, :].astype(F32)
                    b_sc[slot + 3 * group + h] = jnp.broadcast_to(row, (128, HEAD)).T

    @pl.when(step == 0)
    def _():
        small = small_copies()
        for c in small[:2]:
            c.start()

        def fetch(r, c):
            load_hidden(r).start()
            return c

        lax.fori_loop(0, ROWS, fetch, 0)
        barrier = pltpu.get_barrier_semaphore()
        for peer in (peer_x, peer_d, peer_xd):
            pl.semaphore_signal(barrier, inc=1, device_id={'sp': peer}, device_id_type=MESH)
        for c in small[2:] + weight_copies():
            c.start()
        for c in small[:2]:
            c.wait()
        load_hidden(0).wait()
        norm_piece(0)
        pl.semaphore_wait(barrier, 3)

        def norm_and_send(i, c):
            @pl.when(lax.rem(i, 2) == 0)
            def _():
                load_hidden(lax.div(i, 2)).wait()

            norm_piece(i)

            @pl.when(i <= 2 * AHEAD)
            def _():
                send_x(i - 1).start()

            return c

        lax.fori_loop(1, 2 * ROWS, norm_and_send, 0)
        for c in small[2:]:
            c.wait()
        for n, peer in enumerate((peer_x, peer_d, peer_xd)):
            swap_pos(n, peer).start()
        send_d(0).start()
        posr[me] = pos_ref[:, 128:256]
        qbd[...] = jnp.zeros_like(qbd)
        spread_bias()
        for c in weight_copies():
            c.wait()
        for n, peer in enumerate((peer_x, peer_d, peer_xd)):
            recv_pos(n, peer).wait()

    def build_tables(r):
        tcos = tcos_ref[...]
        tsin = tsin_ref[...]
        lane = lax.broadcasted_iota(jnp.int32, (16, SEQ), 1)
        ctx = ctx_ref[r]
        last = posr[3, pl.ds(r, 1), :]
        last_lane = lax.broadcasted_iota(jnp.int32, (1, 128), 1)
        m_pos = jnp.sum(jnp.where(last_lane == 127, last, 0), axis=1, keepdims=True)

        def pick(table, hit):
            return jnp.sum(jnp.where(hit, table, 0.0), axis=1, keepdims=True)

        at_m = lane == m_pos
        at_c = lane == ctx - 1
        in_ctx = lane < ctx
        cos_c, sin_c = pick(tcos, at_c), pick(tsin, at_c)
        ctab[0:16] = jnp.where(in_ctx, tcos, pick(tcos, at_m))
        stab[0:16] = jnp.where(in_ctx, tsin, pick(tsin, at_m))
        ctab[16:32] = jnp.where(in_ctx, 1.0, tcos * cos_c + tsin * sin_c)
        stab[16:32] = jnp.where(in_ctx, 0.0, tsin * cos_c - tcos * sin_c)

    def multiply(y_ref, tokens, rows):
        y_ref[0:rows] = nt_dot(w_sc[0:rows // HEAD].reshape(rows, HID), tokens)

    def finish(y_ref, part, with_q):
        for h in range(LOCAL):
            for lt in range(PART // 128):
                cols = pl.ds(pl.multiple_of(part * PART + lt * 128, 128), 128)
                ycols = slice(lt * 128, lt * 128 + 128)
                for half in range(2):
                    cos = ctab[16 * half:16 * half + 16, cols]
                    sin = stab[16 * half:16 * half + 16, cols]

                    def rotated(base):
                        u0 = base + h * HEAD + half * 32
                        b0 = half * 32
                        bias = b_sc.at[base // HEAD + h]
                        u = (y_ref[u0:u0 + 16, ycols] + bias[b0:b0 + 16]).astype(BF16).astype(F32)
                        w = (y_ref[u0 + 16:u0 + 32, ycols] + bias[b0 + 16:b0 + 32]).astype(BF16).astype(F32)
                        return (u * cos - w * sin).astype(BF16), (w * cos + u * sin).astype(BF16)

                    k0 = (h % 2) * HEAD + half * 32
                    ku, kw = rotated(0)
                    kt_refs[h // 2][k0:k0 + 16, cols] = ku
                    kt_refs[h // 2][k0 + 16:k0 + 32, cols] = kw
                    if with_q:
                        qu, qw = rotated(2 * WIDE)
                        q0 = (h % 2) * HEAD + half * 32
                        qc = pl.ds(pl.multiple_of((h % 2) * CHIP + lax.rem(part, 2) * PART + lt * 128, 128), 128)
                        qbd[h // 2, q0:q0 + 16, qc] = qu
                        qbd[h // 2, q0 + 16:q0 + 32, qc] = qw
                v0 = WIDE + h * HEAD
                vt[h * HEAD:(h + 1) * HEAD, cols] = (y_ref[v0:v0 + HEAD, ycols] + b_sc[6 + h]).astype(BF16)

    def project(first, first_part, second, second_part, with_q):
        rows = 3 * WIDE if with_q else 2 * WIDE
        multiply(y_0, first, rows)
        multiply(y_1, second, rows)
        finish(y_0, first_part, with_q)
        finish(y_1, second_part, with_q)

    def attend(r, this_chip):
        spec = ((768, 256), (768, 256)) if this_chip == 0 else ((768, 512), (1024, 768))

        def score(pair, j):
            for qb in range(2):
                key_len, mask_from = spec[qb]
                q0 = j * CHIP + qb * PART
                scores = jnp.dot(kk[pair, 0:key_len, :], qbd[pair, :, q0:q0 + PART], preferred_element_type=F32)
                q_pos = this_chip * CHIP + qb * PART + lax.broadcasted_iota(jnp.int32, (1, PART), 1)
                limit = jnp.maximum(q_pos, ctx_ref[r] - 1)
                top = None
                for k0 in range(0, key_len, CHUNK):
                    part = scores[k0:k0 + CHUNK]
                    if k0 >= mask_from:
                        k_pos = k0 + lax.broadcasted_iota(jnp.int32, (CHUNK, PART), 0)
                        part = jnp.where(k_pos <= limit, part, -jnp.inf)
                    s_refs[2 * j + qb][k0:k0 + CHUNK] = part
                    peak = jnp.max(part.reshape(CHUNK // 8, 8, PART), axis=0)
                    top = peak if top is None else jnp.maximum(top, peak)
                top_sc[2 * j + qb] = jnp.broadcast_to(jnp.max(top, axis=0, keepdims=True) * EXP_SCALE, (8, PART))

        def mix(pair, j):
            v_rows = pl.ds(pl.multiple_of((2 * pair + j) * HEAD, HEAD), HEAD)
            for qb in range(2):
                top = top_sc[2 * j + qb, 0:1]
                total = jnp.zeros((8, PART), F32)
                mixed = None
                for k0 in range(0, spec[qb][0], MIX):
                    probs = []
                    for k1 in range(k0, k0 + MIX, CHUNK):
                        prob = jnp.exp2(s_refs[2 * j + qb][k1:k1 + CHUNK] * EXP_SCALE - top)
                        total = total + jnp.sum(prob.reshape(CHUNK // 8, 8, PART), axis=0)
                        probs.append(prob.astype(BF16))
                    some = jnp.dot(vt[v_rows, k0:k0 + MIX], jnp.concatenate(probs, axis=0), preferred_element_type=F32)
                    mixed = some if mixed is None else mixed + some
                inv = 1.0 / jnp.sum(total, axis=0, keepdims=True)
                ctx_buf[lax.rem(r, 2), qb, v_rows, :] = (mixed * inv).astype(BF16)

        score(0, 0)

        def one_pair(pair, c):
            score(pair, 1)
            mix(pair, 0)
            score(pair + 1, 0)
            mix(pair, 1)
            return c

        lax.fori_loop(0, LOCAL // 2 - 1, one_pair, 0)
        score(LOCAL // 2 - 1, 1)
        mix(LOCAL // 2 - 1, 0)
        mix(LOCAL // 2 - 1, 1)

    def dense(r):
        mixed = jnp.concatenate([ctx_buf[lax.rem(r, 2), core], ctx_recv[lax.rem(r, 2)]], axis=0)
        dense_out = lax.dot_general(mixed, wd_sc[...], (((0,), (0,)), ((), ())), preferred_element_type=F32)
        normed = own[r].astype(F32)
        out_ref[r] = (normed * ALPHA + dense_out + bd_ref[...].astype(F32).reshape(1, HID)).astype(BF16)

    @pl.when(step > 0)
    def _():
        swap_ctx(step - 1).start()

    @pl.when(step < ROWS)
    def _():
        for n in range(2):
            send_x(2 * step + n).wait_recv()
            relay(2 * step + n).start()

    @pl.when(step < ROWS - AHEAD)
    def _():
        for n in range(2):
            send_x(2 * (step + AHEAD) + n).start()

    @pl.when(step < ROWS)
    def _():
        build_tables(step)
        send_d(step).wait_recv()
        project(own[step], me, dbuf[lax.rem(step, 2)], peer_d, True)

    @pl.when(step > 0)
    def _():
        swap_ctx(step - 1).wait()
        dense(step - 1)

    @pl.when(step < ROWS)
    def _():
        for n in range(2):
            relay(2 * step + n).wait_recv()

    @pl.when(step < ROWS - 1)
    def _():
        send_d(step + 1).start()

    @pl.when(step < ROWS)
    def _():
        multiply(y_0, xbuf[step], 2 * WIDE)
        multiply(y_1, rbuf[lax.rem(step, 2)], 2 * WIDE)

    def rest(r, this_chip):
        finish(y_0, peer_x, False)
        finish(y_1, peer_xd, False)
        ko_ref[r, 0:2] = kt_0[...].reshape(2, HEAD, SEQ)
        ko_ref[r, 2] = kt_1[0:HEAD]
        vo_ref[r] = vt[0:192].reshape(3, HEAD, SEQ)
        for pair in range(LOCAL // 2):
            kk[pair] = kt_refs[pair][...].T
        attend(r, this_chip)

    for this_chip in range(2):
        @pl.when(jnp.logical_and(step < ROWS, chip == this_chip))
        def _():
            rest(step, this_chip)

    @pl.when(step == ROWS)
    def _():
        def drain(r, c):
            for n in range(2):
                send_x(2 * r + n).wait_send()
                relay(2 * r + n).wait_send()
            send_d(r).wait_send()
            return c

        lax.fori_loop(0, ROWS, drain, 0)


def put(out_vm, keys_vm, values_vm, out_hbm, keys_hbm, values_hbm, sem):
    copies = [pltpu.make_async_copy(src, dst, sem.at[i]) for i, (src, dst) in enumerate(((out_vm, out_hbm), (keys_vm, keys_hbm), (values_vm, values_hbm)))]
    for c in copies:
        c.start()
    for c in copies:
        c.wait()


def solution(mesh):
    seq_spec = P('dp', 'sp', None)
    row_spec = P('dp', 'sp')
    head_spec = P('dp', None, 'sp', None)
    replicated = P()
    tcos, tsin = rope_tables()

    def local_block(hidden, pos_ids, block_ids, ctx_len, ln_gamma, ln_beta, w_qkv, b_qkv, w_dense, b_dense):
        w_t = jnp.transpose(w_qkv, (1, 2, 3, 0))
        anywhere = pl.BlockSpec(memory_space=pl.ANY)

        out, keys_t, values_t = pl.pallas_call(
            kernel,
            grid=(ROWS + 1,),
            out_shape=(
                pltpu.VMEM((ROWS, PART, HID), BF16),
                pltpu.VMEM((ROWS, 3, HEAD, SEQ), BF16),
                pltpu.VMEM((ROWS, 3, HEAD, SEQ), BF16),
            ),
            in_specs=[anywhere, anywhere, pl.BlockSpec(memory_space=pltpu.SMEM)] + [anywhere] * 8,
            out_specs=(pl.BlockSpec(memory_space=pltpu.VMEM),) * 3,
            scratch_shapes=[
                pltpu.VMEM((ROWS, PART), jnp.int32),
                pltpu.VMEM((HID,), BF16),
                pltpu.VMEM((HID,), BF16),
                pltpu.VMEM((HID,), BF16),
                pltpu.VMEM((12, 3, HEAD), BF16),
                pltpu.VMEM((16, SEQ), F32),
                pltpu.VMEM((16, SEQ), F32),
                pltpu.VMEM((ROWS, PART, HID), BF16),
                pltpu.VMEM((ROWS, PART, HID), BF16),
                pltpu.VMEM((2, PART, HID), BF16),
                pltpu.VMEM((2, PART, HID), BF16),
                pltpu.VMEM((4, ROWS, 128), jnp.int32),
                pltpu.VMEM((18, HEAD, HID), BF16),
                pltpu.VMEM((18, HEAD, 128), F32),
                pltpu.VMEM((HID, HID), BF16),
                pltpu.VMEM((3 * WIDE, PART), F32),
                pltpu.VMEM((3 * WIDE, PART), F32),
                *[pltpu.VMEM((2 * HEAD, SEQ), BF16)] * 3,
                pltpu.VMEM((WIDE, SEQ), BF16),
                pltpu.VMEM((3, SEQ, 128), BF16),
                pltpu.VMEM((3, 128, 2 * CHIP), BF16),
                pltpu.VMEM((32, SEQ), F32),
                pltpu.VMEM((32, SEQ), F32),
                *[pltpu.VMEM((SEQ, PART), F32)] * 4,
                pltpu.VMEM((4, 8, PART), F32),
                pltpu.VMEM((2, 2, WIDE, PART), BF16),
                pltpu.VMEM((2, WIDE, PART), BF16),
                pltpu.SemaphoreType.DMA((7,)),
                pltpu.SemaphoreType.DMA((ROWS,)),
                pltpu.SemaphoreType.DMA((22,)),
            ] + [pltpu.SemaphoreType.DMA((n * ROWS,)) for n in (2, 2, 1, 1, 2, 2, 1, 1)] + [pltpu.SemaphoreType.DMA((3,))] * 2,
            compiler_params=pltpu.CompilerParams(
                collective_id=0, has_side_effects=True, vmem_limit_bytes=43 * 1024 * 1024, dimension_semantics=('arbitrary',)),
            name='glm_block',
        )(hidden, pos_ids, ctx_len, ln_gamma, ln_beta, b_dense,
          w_t, b_qkv, w_dense, jnp.asarray(tcos), jnp.asarray(tsin))
        held = [pltpu.with_memory_space_constraint(x, pltpu.VMEM) for x in (out, keys_t, values_t)]
        out, keys_t, values_t = pl.pallas_call(
            put,
            out_shape=[jax.ShapeDtypeStruct(x.shape, BF16) for x in held],
            in_specs=[pl.BlockSpec(memory_space=pl.ANY)] * 3,
            out_specs=[anywhere] * 3,
            scratch_shapes=[pltpu.SemaphoreType.DMA((3,))],
            compiler_params=pltpu.CompilerParams(vmem_limit_bytes=1024 * 1024),
            name='put',
        )(*held)
        return out, jnp.transpose(keys_t, (0, 3, 1, 2)), jnp.transpose(values_t, (0, 3, 1, 2))

    return jax.shard_map(local_block, mesh=mesh, in_specs=(seq_spec, row_spec, row_spec, P('dp'), replicated, replicated, replicated, replicated, replicated, replicated), out_specs=(seq_spec, head_spec, head_spec), check_vma=False)
```

```python
import functools
import math

import jax
import jax.numpy as jnp
import numpy as np
from jax import lax
from jax.experimental import pallas as pl
from jax.experimental.pallas import tpu as pltpu
from jax.sharding import PartitionSpec as P

ALPHA = math.sqrt(56.0)
ROPE_BASE = 10000.0
LN_EPS = 1e-5
MESH = pl.DeviceIdType.MESH
F32 = jnp.float32
BF16 = jnp.bfloat16

ROWS = 16
PART = 256
AHEAD = 4
SEQ = 1024
HID = 768
HEAD = 64
CHIP = 512
LOCAL = 6
WIDE = LOCAL * HEAD
EXP_SCALE = math.log2(math.e) / math.sqrt(HEAD)
CHUNK = 64
MIX = 256


def rope_tables():
    freq = ROPE_BASE ** (-np.arange(0, 32, 2).astype(np.float64) / 32.0)
    angle = freq.astype(np.float32)[:, None] * np.arange(SEQ, dtype=np.float32)[None, :]
    return np.cos(angle.astype(np.float64)).astype(np.float32), np.sin(angle.astype(np.float64)).astype(np.float32)


def nt_dot(a, b):
    return lax.dot_general(a, b, (((1,), (1,)), ((), ())), preferred_element_type=F32)


def kernel(hid_hbm, pos_hbm, ctx_ref, gamma_hbm, beta_hbm, bd_hbm, w_hbm, bias_hbm, wd_hbm, tcos_hbm, tsin_hbm,
           out_ref, ko_ref, vo_ref,
           pos_ref, gamma_ref, beta_ref, bd_ref, bias_ref, tcos_ref, tsin_ref, own, xbuf, dbuf, rbuf, posr, w_sc, b_sc, wd_sc, y_0, y_1, kt_0, kt_1, kt_2, vt, kk, qbd, ctab, stab, s_0, s_1, s_2, s_3, top_sc, ctx_buf, ctx_recv,
           t_sem, hid_sem, w_sem, xs_sem, xr_sem, ds_sem, dr_sem, rs_sem, rr_sem, cs_sem, cr_sem, ps_sem, pr_sem):
    step = pl.program_id(0)
    s_refs, kt_refs = (s_0, s_1, s_2, s_3), (kt_0, kt_1, kt_2)
    me = lax.axis_index('sp')
    core = lax.rem(me, 2)
    chip = me // 2
    other = 1 - chip
    peer_x = other * 2 + core
    peer_d = chip * 2 + 1 - core
    peer_xd = other * 2 + 1 - core

    def remote(src, dst, send_sem, recv_sem, peer):
        return pltpu.make_async_remote_copy(src, dst, send_sem, recv_sem, device_id={'sp': peer}, device_id_type=MESH)

    def send_x(r):
        return remote(own.at[r], xbuf.at[r], xs_sem.at[r], xr_sem.at[r], peer_x)

    def send_d(r):
        return remote(own.at[r], dbuf.at[lax.rem(r, 2)], ds_sem.at[r], dr_sem.at[r], peer_d)

    def relay(r):
        return remote(xbuf.at[r], rbuf.at[lax.rem(r, 2)], rs_sem.at[r], rr_sem.at[r], peer_d)

    def swap_ctx(r):
        return remote(ctx_buf.at[lax.rem(r, 2), 1 - core], ctx_recv.at[lax.rem(r, 2)], cs_sem.at[r], cr_sem.at[r], peer_d)

    def swap_pos(n, peer):
        return remote(pos_ref.at[:, pl.ds(128, 128)], posr.at[me], ps_sem.at[n], pr_sem.at[n], peer)

    def recv_pos(n, peer):
        return remote(pos_ref.at[:, pl.ds(128, 128)], posr.at[peer], ps_sem.at[n], pr_sem.at[n], peer)

    def load_hidden(r):
        return pltpu.make_async_copy(hid_hbm.at[r], own.at[r], hid_sem.at[r])

    def small_copies():
        pairs = ((gamma_hbm, gamma_ref), (beta_hbm, beta_ref), (pos_hbm, pos_ref), (bd_hbm, bd_ref), (bias_hbm, bias_ref), (tcos_hbm, tcos_ref), (tsin_hbm, tsin_ref))
        return [pltpu.make_async_copy(src, dst, t_sem.at[i]) for i, (src, dst) in enumerate(pairs)]

    def weight_copies():
        copies = []
        for group, owner in enumerate((me, peer_x)):
            for slot, kind in ((0, 1), (6, 2), (12, 0)):
                for h in range(3):
                    copies.append((w_hbm.at[owner * 3 + h, kind], w_sc.at[slot + 3 * group + h]))
        for slot, owner in enumerate((me, peer_x, peer_d, peer_xd)):
            copies.append((wd_hbm.at[pl.ds(pl.multiple_of(owner * 192, 64), 192)], wd_sc.at[pl.ds(slot * 192, 192)]))
        return [pltpu.make_async_copy(src, dst, w_sem.at[i]) for i, (src, dst) in enumerate(copies)]

    def norm_row(r):
        gamma = gamma_ref[...].astype(F32).reshape(1, HID)
        beta = beta_ref[...].astype(F32).reshape(1, HID)
        for t in range(0, PART, 32):
            rows = pl.ds(t, 32)
            wide = own[r, rows, :].astype(F32)
            mean = jnp.sum(wide, axis=-1, keepdims=True) * (1.0 / HID)
            cent = wide - mean
            var = jnp.sum(cent * cent, axis=-1, keepdims=True) * (1.0 / HID)
            own[r, rows, :] = (cent * lax.rsqrt(var + LN_EPS) * gamma + beta).astype(BF16)

    def spread_bias():
        for group, owner in enumerate((me, peer_x)):
            for slot, kind in ((0, 1), (6, 2), (12, 0)):
                for h in range(3):
                    row = bias_ref[owner * 3 + h, kind:kind + 1, :].astype(F32)
                    b_sc[slot + 3 * group + h] = jnp.broadcast_to(row, (128, HEAD)).T

    @pl.when(step == 0)
    def _():
        small = small_copies()
        for c in small[:2]:
            c.start()

        def fetch(r, c):
            load_hidden(r).start()
            return c

        lax.fori_loop(0, ROWS, fetch, 0)
        barrier = pltpu.get_barrier_semaphore()
        for peer in (peer_x, peer_d, peer_xd):
            pl.semaphore_signal(barrier, inc=1, device_id={'sp': peer}, device_id_type=MESH)
        for c in small[2:] + weight_copies():
            c.start()
        for c in small[:2]:
            c.wait()
        load_hidden(0).wait()
        norm_row(0)
        pl.semaphore_wait(barrier, 3)
        load_hidden(1).wait()
        norm_row(1)
        send_x(0).start()

        def norm_and_send(r, c):
            load_hidden(r).wait()
            norm_row(r)

            @pl.when(r <= AHEAD)
            def _():
                send_x(r - 1).start()

            return c

        lax.fori_loop(2, ROWS, norm_and_send, 0)
        for c in small[2:]:
            c.wait()
        for n, peer in enumerate((peer_x, peer_d, peer_xd)):
            swap_pos(n, peer).start()
        send_d(0).start()
        posr[me] = pos_ref[:, 128:256]
        qbd[...] = jnp.zeros_like(qbd)
        spread_bias()
        for c in weight_copies():
            c.wait()
        for n, peer in enumerate((peer_x, peer_d, peer_xd)):
            recv_pos(n, peer).wait()

    def build_tables(r):
        tcos = tcos_ref[...]
        tsin = tsin_ref[...]
        lane = lax.broadcasted_iota(jnp.int32, (16, SEQ), 1)
        ctx = ctx_ref[r]
        last = posr[3, pl.ds(r, 1), :]
        last_lane = lax.broadcasted_iota(jnp.int32, (1, 128), 1)
        m_pos = jnp.sum(jnp.where(last_lane == 127, last, 0), axis=1, keepdims=True)

        def pick(table, hit):
            return jnp.sum(jnp.where(hit, table, 0.0), axis=1, keepdims=True)

        at_m = lane == m_pos
        at_c = lane == ctx - 1
        in_ctx = lane < ctx
        cos_c, sin_c = pick(tcos, at_c), pick(tsin, at_c)
        ctab[0:16] = jnp.where(in_ctx, tcos, pick(tcos, at_m))
        stab[0:16] = jnp.where(in_ctx, tsin, pick(tsin, at_m))
        ctab[16:32] = jnp.where(in_ctx, 1.0, tcos * cos_c + tsin * sin_c)
        stab[16:32] = jnp.where(in_ctx, 0.0, tsin * cos_c - tcos * sin_c)

    def multiply(y_ref, tokens, rows):
        y_ref[0:rows] = nt_dot(w_sc[0:rows // HEAD].reshape(rows, HID), tokens)

    def finish(y_ref, part, with_q):
        for h in range(LOCAL):
            for lt in range(PART // 128):
                cols = pl.ds(pl.multiple_of(part * PART + lt * 128, 128), 128)
                ycols = slice(lt * 128, lt * 128 + 128)
                for half in range(2):
                    cos = ctab[16 * half:16 * half + 16, cols]
                    sin = stab[16 * half:16 * half + 16, cols]

                    def rotated(base):
                        u0 = base + h * HEAD + half * 32
                        b0 = half * 32
                        bias = b_sc.at[base // HEAD + h]
                        u = (y_ref[u0:u0 + 16, ycols] + bias[b0:b0 + 16]).astype(BF16).astype(F32)
                        w = (y_ref[u0 + 16:u0 + 32, ycols] + bias[b0 + 16:b0 + 32]).astype(BF16).astype(F32)
                        return (u * cos - w * sin).astype(BF16), (w * cos + u * sin).astype(BF16)

                    k0 = (h % 2) * HEAD + half * 32
                    ku, kw = rotated(0)
                    kt_refs[h // 2][k0:k0 + 16, cols] = ku
                    kt_refs[h // 2][k0 + 16:k0 + 32, cols] = kw
                    if with_q:
                        qu, qw = rotated(2 * WIDE)
                        q0 = (h % 2) * HEAD + half * 32
                        qc = pl.ds(pl.multiple_of((h % 2) * CHIP + lax.rem(part, 2) * PART + lt * 128, 128), 128)
                        qbd[h // 2, q0:q0 + 16, qc] = qu
                        qbd[h // 2, q0 + 16:q0 + 32, qc] = qw
                v0 = WIDE + h * HEAD
                vt[h * HEAD:(h + 1) * HEAD, cols] = (y_ref[v0:v0 + HEAD, ycols] + b_sc[6 + h]).astype(BF16)

    def project(first, first_part, second, second_part, with_q):
        rows = 3 * WIDE if with_q else 2 * WIDE
        multiply(y_0, first, rows)
        multiply(y_1, second, rows)
        finish(y_0, first_part, with_q)
        finish(y_1, second_part, with_q)

    def attend(r, this_chip):
        spec = ((768, 256), (768, 256)) if this_chip == 0 else ((768, 512), (1024, 768))

        def score(pair, j):
            for qb in range(2):
                key_len, mask_from = spec[qb]
                q0 = j * CHIP + qb * PART
                scores = jnp.dot(kk[pair, 0:key_len, :], qbd[pair, :, q0:q0 + PART], preferred_element_type=F32)
                q_pos = this_chip * CHIP + qb * PART + lax.broadcasted_iota(jnp.int32, (1, PART), 1)
                limit = jnp.maximum(q_pos, ctx_ref[r] - 1)
                top = None
                for k0 in range(0, key_len, CHUNK):
                    part = scores[k0:k0 + CHUNK]
                    if k0 >= mask_from:
                        k_pos = k0 + lax.broadcasted_iota(jnp.int32, (CHUNK, PART), 0)
                        part = jnp.where(k_pos <= limit, part, -jnp.inf)
                    s_refs[2 * j + qb][k0:k0 + CHUNK] = part
                    peak = jnp.max(part.reshape(CHUNK // 8, 8, PART), axis=0)
                    top = peak if top is None else jnp.maximum(top, peak)
                top_sc[2 * j + qb] = jnp.broadcast_to(jnp.max(top, axis=0, keepdims=True) * EXP_SCALE, (8, PART))

        def mix(pair, j):
            v_rows = pl.ds(pl.multiple_of((2 * pair + j) * HEAD, HEAD), HEAD)
            for qb in range(2):
                top = top_sc[2 * j + qb, 0:1]
                total = jnp.zeros((8, PART), F32)
                mixed = None
                for k0 in range(0, spec[qb][0], MIX):
                    probs = []
                    for k1 in range(k0, k0 + MIX, CHUNK):
                        prob = jnp.exp2(s_refs[2 * j + qb][k1:k1 + CHUNK] * EXP_SCALE - top)
                        total = total + jnp.sum(prob.reshape(CHUNK // 8, 8, PART), axis=0)
                        probs.append(prob.astype(BF16))
                    some = jnp.dot(vt[v_rows, k0:k0 + MIX], jnp.concatenate(probs, axis=0), preferred_element_type=F32)
                    mixed = some if mixed is None else mixed + some
                inv = 1.0 / jnp.sum(total, axis=0, keepdims=True)
                ctx_buf[lax.rem(r, 2), qb, v_rows, :] = (mixed * inv).astype(BF16)

        score(0, 0)

        def one_pair(pair, c):
            score(pair, 1)
            mix(pair, 0)
            score(pair + 1, 0)
            mix(pair, 1)
            return c

        lax.fori_loop(0, LOCAL // 2 - 1, one_pair, 0)
        score(LOCAL // 2 - 1, 1)
        mix(LOCAL // 2 - 1, 0)
        mix(LOCAL // 2 - 1, 1)

    def dense(r):
        mixed = jnp.concatenate([ctx_buf[lax.rem(r, 2), core], ctx_recv[lax.rem(r, 2)]], axis=0)
        dense_out = lax.dot_general(mixed, wd_sc[...], (((0,), (0,)), ((), ())), preferred_element_type=F32)
        normed = own[r].astype(F32)
        out_ref[r] = (normed * ALPHA + dense_out + bd_ref[...].astype(F32).reshape(1, HID)).astype(BF16)

    @pl.when(step > 0)
    def _():
        swap_ctx(step - 1).start()

    @pl.when(step < ROWS)
    def _():
        send_x(step).wait_recv()
        relay(step).start()

    @pl.when(step < ROWS - AHEAD)
    def _():
        send_x(step + AHEAD).start()

    @pl.when(step < ROWS)
    def _():
        build_tables(step)
        send_d(step).wait_recv()
        project(own[step], me, dbuf[lax.rem(step, 2)], peer_d, True)

    @pl.when(step > 0)
    def _():
        swap_ctx(step - 1).wait()
        dense(step - 1)

    @pl.when(step < ROWS)
    def _():
        relay(step).wait_recv()

    @pl.when(step < ROWS - 1)
    def _():
        send_d(step + 1).start()

    @pl.when(step < ROWS)
    def _():
        multiply(y_0, xbuf[step], 2 * WIDE)
        multiply(y_1, rbuf[lax.rem(step, 2)], 2 * WIDE)

    def rest(r, this_chip):
        finish(y_0, peer_x, False)
        finish(y_1, peer_xd, False)
        ko_ref[r, 0:2] = kt_0[...].reshape(2, HEAD, SEQ)
        ko_ref[r, 2] = kt_1[0:HEAD]
        vo_ref[r] = vt[0:192].reshape(3, HEAD, SEQ)
        for pair in range(LOCAL // 2):
            kk[pair] = kt_refs[pair][...].T
        attend(r, this_chip)

    for this_chip in range(2):
        @pl.when(jnp.logical_and(step < ROWS, chip == this_chip))
        def _():
            rest(step, this_chip)

    @pl.when(step == ROWS)
    def _():
        def drain(r, c):
            send_x(r).wait_send()
            relay(r).wait_send()
            send_d(r).wait_send()
            return c

        lax.fori_loop(0, ROWS, drain, 0)


def put(out_vm, keys_vm, values_vm, out_hbm, keys_hbm, values_hbm, sem):
    copies = [pltpu.make_async_copy(src, dst, sem.at[i]) for i, (src, dst) in enumerate(((out_vm, out_hbm), (keys_vm, keys_hbm), (values_vm, values_hbm)))]
    for c in copies:
        c.start()
    for c in copies:
        c.wait()


def solution(mesh):
    seq_spec = P('dp', 'sp', None)
    row_spec = P('dp', 'sp')
    head_spec = P('dp', None, 'sp', None)
    replicated = P()
    tcos, tsin = rope_tables()

    def local_block(hidden, pos_ids, block_ids, ctx_len, ln_gamma, ln_beta, w_qkv, b_qkv, w_dense, b_dense):
        w_t = jnp.transpose(w_qkv, (1, 2, 3, 0))
        anywhere = pl.BlockSpec(memory_space=pl.ANY)

        out, keys_t, values_t = pl.pallas_call(
            kernel,
            grid=(ROWS + 1,),
            out_shape=(
                pltpu.VMEM((ROWS, PART, HID), BF16),
                pltpu.VMEM((ROWS, 3, HEAD, SEQ), BF16),
                pltpu.VMEM((ROWS, 3, HEAD, SEQ), BF16),
            ),
            in_specs=[anywhere, anywhere, pl.BlockSpec(memory_space=pltpu.SMEM)] + [anywhere] * 8,
            out_specs=(pl.BlockSpec(memory_space=pltpu.VMEM),) * 3,
            scratch_shapes=[
                pltpu.VMEM((ROWS, PART), jnp.int32),
                pltpu.VMEM((HID,), BF16),
                pltpu.VMEM((HID,), BF16),
                pltpu.VMEM((HID,), BF16),
                pltpu.VMEM((12, 3, HEAD), BF16),
                pltpu.VMEM((16, SEQ), F32),
                pltpu.VMEM((16, SEQ), F32),
                pltpu.VMEM((ROWS, PART, HID), BF16),
                pltpu.VMEM((ROWS, PART, HID), BF16),
                pltpu.VMEM((2, PART, HID), BF16),
                pltpu.VMEM((2, PART, HID), BF16),
                pltpu.VMEM((4, ROWS, 128), jnp.int32),
                pltpu.VMEM((18, HEAD, HID), BF16),
                pltpu.VMEM((18, HEAD, 128), F32),
                pltpu.VMEM((HID, HID), BF16),
                pltpu.VMEM((3 * WIDE, PART), F32),
                pltpu.VMEM((3 * WIDE, PART), F32),
                *[pltpu.VMEM((2 * HEAD, SEQ), BF16)] * 3,
                pltpu.VMEM((WIDE, SEQ), BF16),
                pltpu.VMEM((3, SEQ, 128), BF16),
                pltpu.VMEM((3, 128, 2 * CHIP), BF16),
                pltpu.VMEM((32, SEQ), F32),
                pltpu.VMEM((32, SEQ), F32),
                *[pltpu.VMEM((SEQ, PART), F32)] * 4,
                pltpu.VMEM((4, 8, PART), F32),
                pltpu.VMEM((2, 2, WIDE, PART), BF16),
                pltpu.VMEM((2, WIDE, PART), BF16),
                pltpu.SemaphoreType.DMA((7,)),
                pltpu.SemaphoreType.DMA((ROWS,)),
                pltpu.SemaphoreType.DMA((22,)),
            ] + [pltpu.SemaphoreType.DMA((ROWS,))] * 8 + [pltpu.SemaphoreType.DMA((3,))] * 2,
            compiler_params=pltpu.CompilerParams(
                collective_id=0, has_side_effects=True, vmem_limit_bytes=43 * 1024 * 1024, dimension_semantics=('arbitrary',)),
            name='glm_block',
        )(hidden, pos_ids, ctx_len, ln_gamma, ln_beta, b_dense,
          w_t, b_qkv, w_dense, jnp.asarray(tcos), jnp.asarray(tsin))
        held = [pltpu.with_memory_space_constraint(x, pltpu.VMEM) for x in (out, keys_t, values_t)]
        out, keys_t, values_t = pl.pallas_call(
            put,
            out_shape=[jax.ShapeDtypeStruct(x.shape, BF16) for x in held],
            in_specs=[pl.BlockSpec(memory_space=pl.ANY)] * 3,
            out_specs=[anywhere] * 3,
            scratch_shapes=[pltpu.SemaphoreType.DMA((3,))],
            compiler_params=pltpu.CompilerParams(vmem_limit_bytes=1024 * 1024),
            name='put',
        )(*held)
        return out, jnp.transpose(keys_t, (0, 3, 1, 2)), jnp.transpose(values_t, (0, 3, 1, 2))

    return jax.shard_map(local_block, mesh=mesh, in_specs=(seq_spec, row_spec, row_spec, P('dp'), replicated, replicated, replicated, replicated, replicated, replicated), out_specs=(seq_spec, head_spec, head_spec), check_vma=False)
```

```python
import functools
import math

import jax
import jax.numpy as jnp
import numpy as np
from jax import lax
from jax.experimental import pallas as pl
from jax.experimental.pallas import tpu as pltpu
from jax.sharding import PartitionSpec as P

ALPHA = math.sqrt(56.0)
ROPE_BASE = 10000.0
LN_EPS = 1e-5
MESH = pl.DeviceIdType.MESH
F32 = jnp.float32
BF16 = jnp.bfloat16

ROWS = 16
PART = 256
AHEAD = 4
SEQ = 1024
LAST = ROWS - 1
HID = 768
HEAD = 64
CHIP = 512
LOCAL = 6
WIDE = LOCAL * HEAD
EXP_SCALE = math.log2(math.e) / math.sqrt(HEAD)
CHUNK = 64
MIX = 256


def rope_tables():
    freq = ROPE_BASE ** (-np.arange(0, 32, 2).astype(np.float64) / 32.0)
    angle = freq.astype(np.float32)[:, None] * np.arange(SEQ, dtype=np.float32)[None, :]
    return np.cos(angle.astype(np.float64)).astype(np.float32), np.sin(angle.astype(np.float64)).astype(np.float32)


def nt_dot(a, b):
    return lax.dot_general(a, b, (((1,), (1,)), ((), ())), preferred_element_type=F32)


def multiply(y_ref, w_ref, base, rows, tokens):
    y_ref[0:rows] = nt_dot(w_ref[base:base + rows // HEAD].reshape(rows, HID), tokens)


def finish(y_ref, b_ref, base, part, q_col, ctab, stab, kt_refs, vt, qbd):
    for h in range(LOCAL):
        for lt in range(PART // 128):
            cols = pl.ds(pl.multiple_of(part * PART + lt * 128, 128), 128)
            ycols = slice(lt * 128, lt * 128 + 128)
            for half in range(2):
                cos = ctab[16 * half:16 * half + 16, cols]
                sin = stab[16 * half:16 * half + 16, cols]

                def rotated(kind):
                    u0 = kind * WIDE + h * HEAD + half * 32
                    b0 = half * 32
                    bias = b_ref.at[base + kind * LOCAL + h]
                    u = (y_ref[u0:u0 + 16, ycols] + bias[b0:b0 + 16]).astype(BF16).astype(F32)
                    w = (y_ref[u0 + 16:u0 + 32, ycols] + bias[b0 + 16:b0 + 32]).astype(BF16).astype(F32)
                    return (u * cos - w * sin).astype(BF16), (w * cos + u * sin).astype(BF16)

                k0 = (h % 2) * HEAD + half * 32
                ku, kw = rotated(0)
                kt_refs[h // 2][k0:k0 + 16, cols] = ku
                kt_refs[h // 2][k0 + 16:k0 + 32, cols] = kw
                if q_col is not None:
                    qu, qw = rotated(2)
                    q_width = qbd.shape[2] // 2
                    qc = pl.ds(pl.multiple_of((h % 2) * q_width + q_col + lt * 128, 128), 128)
                    qbd[h // 2, k0:k0 + 16, qc] = qu
                    qbd[h // 2, k0 + 16:k0 + 32, qc] = qw
            v0 = WIDE + h * HEAD
            vt[h * HEAD:(h + 1) * HEAD, cols] = (y_ref[v0:v0 + HEAD, ycols] + b_ref[base + LOCAL + h]).astype(BF16)


def attend(spec, q_first, ctx, kk, qbd, vt, s_refs, top_sc, store):
    def score(pair, j):
        for qb, (key_len, mask_from) in enumerate(spec):
            q0 = (j * len(spec) + qb) * PART
            scores = jnp.dot(kk[pair, 0:key_len, :], qbd[pair, :, q0:q0 + PART], preferred_element_type=F32)
            q_pos = q_first + qb * PART + lax.broadcasted_iota(jnp.int32, (1, PART), 1)
            limit = jnp.maximum(q_pos, ctx - 1)
            top = None
            for k0 in range(0, key_len, CHUNK):
                part = scores[k0:k0 + CHUNK]
                if k0 >= mask_from:
                    k_pos = k0 + lax.broadcasted_iota(jnp.int32, (CHUNK, PART), 0)
                    part = jnp.where(k_pos <= limit, part, -jnp.inf)
                s_refs[2 * j + qb][k0:k0 + CHUNK] = part
                peak = jnp.max(part.reshape(CHUNK // 8, 8, PART), axis=0)
                top = peak if top is None else jnp.maximum(top, peak)
            top_sc[2 * j + qb] = jnp.broadcast_to(jnp.max(top, axis=0, keepdims=True) * EXP_SCALE, (8, PART))

    def mix(pair, j):
        v_rows = pl.ds(pl.multiple_of((2 * pair + j) * HEAD, HEAD), HEAD)
        for qb, (key_len, _) in enumerate(spec):
            top = top_sc[2 * j + qb, 0:1]
            total = jnp.zeros((8, PART), F32)
            mixed = None
            for k0 in range(0, key_len, MIX):
                probs = []
                for k1 in range(k0, k0 + MIX, CHUNK):
                    prob = jnp.exp2(s_refs[2 * j + qb][k1:k1 + CHUNK] * EXP_SCALE - top)
                    total = total + jnp.sum(prob.reshape(CHUNK // 8, 8, PART), axis=0)
                    probs.append(prob.astype(BF16))
                some = jnp.dot(vt[v_rows, k0:k0 + MIX], jnp.concatenate(probs, axis=0), preferred_element_type=F32)
                mixed = some if mixed is None else mixed + some
            store(qb, v_rows, (mixed * (1.0 / jnp.sum(total, axis=0, keepdims=True))).astype(BF16))

    score(0, 0)

    def one_pair(pair, c):
        score(pair, 1)
        mix(pair, 0)
        score(pair + 1, 0)
        mix(pair, 1)
        return c

    lax.fori_loop(0, LOCAL // 2 - 1, one_pair, 0)
    score(LOCAL // 2 - 1, 1)
    mix(LOCAL // 2 - 1, 0)
    mix(LOCAL // 2 - 1, 1)


def project_out(mixed, wd, normed, bd_ref):
    dense_out = lax.dot_general(mixed, wd, (((0,), (0,)), ((), ())), preferred_element_type=F32)
    return (normed.astype(F32) * ALPHA + dense_out + bd_ref[...].astype(F32).reshape(1, HID)).astype(BF16)


def kernel(hid_hbm, pos_hbm, ctx_ref, gamma_hbm, beta_hbm, bd_hbm, w_hbm, bias_hbm, wd_hbm, tcos_hbm, tsin_hbm,
           out_ref, ko_ref, vo_ref, a_last, w_sc, b_sc, wd_sc, ctab, stab,
           pos_ref, gamma_ref, beta_ref, bd_ref, bias_ref, tcos_ref, tsin_ref, own, xbuf, dbuf, rbuf, posr, y_0, y_1, kt_0, kt_1, kt_2, vt, kk, qbd, s_0, s_1, s_2, s_3, top_sc, ctx_buf, ctx_recv,
           t_sem, hid_sem, w_sem, xs_sem, xr_sem, ds_sem, dr_sem, rs_sem, rr_sem, cs_sem, cr_sem, ps_sem, pr_sem):
    step = pl.program_id(0)
    s_refs, kt_refs = (s_0, s_1, s_2, s_3), (kt_0, kt_1, kt_2)
    me = lax.axis_index('sp')
    core = lax.rem(me, 2)
    chip = me // 2
    other = 1 - chip
    peer_x = other * 2 + core
    peer_d = chip * 2 + 1 - core
    peer_xd = other * 2 + 1 - core

    def remote(src, dst, send_sem, recv_sem, peer):
        return pltpu.make_async_remote_copy(src, dst, send_sem, recv_sem, device_id={'sp': peer}, device_id_type=MESH)

    def send_x(r):
        return remote(own.at[r], xbuf.at[r], xs_sem.at[r], xr_sem.at[r], peer_x)

    def send_d(r):
        return remote(own.at[r], dbuf.at[lax.rem(r, 2)], ds_sem.at[r], dr_sem.at[r], peer_d)

    def relay(r):
        return remote(xbuf.at[r], rbuf.at[lax.rem(r, 2)], rs_sem.at[r], rr_sem.at[r], peer_d)

    def swap_ctx(r):
        return remote(ctx_buf.at[lax.rem(r, 2), 1 - core], ctx_recv.at[lax.rem(r, 2)], cs_sem.at[r], cr_sem.at[r], peer_d)

    def swap_pos(n, peer):
        return remote(pos_ref.at[:, pl.ds(128, 128)], posr.at[me], ps_sem.at[n], pr_sem.at[n], peer)

    def recv_pos(n, peer):
        return remote(pos_ref.at[:, pl.ds(128, 128)], posr.at[peer], ps_sem.at[n], pr_sem.at[n], peer)

    def load_hidden(r):
        return pltpu.make_async_copy(hid_hbm.at[r], own.at[r], hid_sem.at[r])

    def small_copies():
        pairs = ((gamma_hbm, gamma_ref), (beta_hbm, beta_ref), (pos_hbm, pos_ref), (bd_hbm, bd_ref), (bias_hbm, bias_ref), (tcos_hbm, tcos_ref), (tsin_hbm, tsin_ref))
        return [pltpu.make_async_copy(src, dst, t_sem.at[i]) for i, (src, dst) in enumerate(pairs)]

    def weight_copies():
        copies = []
        for group, owner in enumerate((me, peer_x, peer_d, peer_xd)):
            for slot, kind in ((0, 1), (6, 2), (12, 0)):
                copies.append((w_hbm.at[pl.ds(owner * 3, 3), kind], w_sc.at[pl.ds(18 * (group // 2) + slot + 3 * (group % 2), 3)]))
        for slot, owner in enumerate((me, peer_x, peer_d, peer_xd)):
            copies.append((wd_hbm.at[pl.ds(pl.multiple_of(owner * 192, 64), 192)], wd_sc.at[pl.ds(slot * 192, 192)]))
        return [pltpu.make_async_copy(src, dst, w_sem.at[i]) for i, (src, dst) in enumerate(copies)]

    def norm_row(r):
        gamma = gamma_ref[...].astype(F32).reshape(1, HID)
        beta = beta_ref[...].astype(F32).reshape(1, HID)
        for t in range(0, PART, 32):
            rows = pl.ds(t, 32)
            wide = own[r, rows, :].astype(F32)
            mean = jnp.sum(wide, axis=-1, keepdims=True) * (1.0 / HID)
            cent = wide - mean
            var = jnp.sum(cent * cent, axis=-1, keepdims=True) * (1.0 / HID)
            own[r, rows, :] = (cent * lax.rsqrt(var + LN_EPS) * gamma + beta).astype(BF16)

    def spread_bias():
        for group, owner in enumerate((me, peer_x, peer_d, peer_xd)):
            for slot, kind in ((0, 1), (6, 2), (12, 0)):
                for h in range(3):
                    row = bias_ref[owner * 3 + h, kind:kind + 1, :].astype(F32)
                    b_sc[18 * (group // 2) + slot + 3 * (group % 2) + h] = jnp.broadcast_to(row, (128, HEAD)).T

    @pl.when(step == 0)
    def _():
        small = small_copies()
        for c in small[:2]:
            c.start()

        def fetch(r, c):
            load_hidden(r).start()
            return c

        lax.fori_loop(0, ROWS, fetch, 0)
        barrier = pltpu.get_barrier_semaphore()
        for peer in (peer_x, peer_d, peer_xd):
            pl.semaphore_signal(barrier, inc=1, device_id={'sp': peer}, device_id_type=MESH)
        for c in small[2:] + weight_copies():
            c.start()
        for c in small[:2]:
            c.wait()
        load_hidden(0).wait()
        norm_row(0)
        pl.semaphore_wait(barrier, 3)
        load_hidden(1).wait()
        norm_row(1)
        send_x(0).start()

        def norm_and_send(r, c):
            load_hidden(r).wait()
            norm_row(r)

            @pl.when(r <= AHEAD)
            def _():
                send_x(r - 1).start()

            return c

        lax.fori_loop(2, ROWS, norm_and_send, 0)
        for c in small[2:]:
            c.wait()
        for n, peer in enumerate((peer_x, peer_d, peer_xd)):
            swap_pos(n, peer).start()
        send_d(0).start()
        posr[me] = pos_ref[:, 128:256]
        qbd[...] = jnp.zeros_like(qbd)
        spread_bias()
        for c in weight_copies():
            c.wait()
        for n, peer in enumerate((peer_x, peer_d, peer_xd)):
            recv_pos(n, peer).wait()

    def build_tables(r):
        tcos = tcos_ref[...]
        tsin = tsin_ref[...]
        lane = lax.broadcasted_iota(jnp.int32, (16, SEQ), 1)
        ctx = ctx_ref[r]
        last = posr[3, pl.ds(r, 1), :]
        last_lane = lax.broadcasted_iota(jnp.int32, (1, 128), 1)
        m_pos = jnp.sum(jnp.where(last_lane == 127, last, 0), axis=1, keepdims=True)

        def pick(table, hit):
            return jnp.sum(jnp.where(hit, table, 0.0), axis=1, keepdims=True)

        at_m = lane == m_pos
        at_c = lane == ctx - 1
        in_ctx = lane < ctx
        cos_c, sin_c = pick(tcos, at_c), pick(tsin, at_c)
        ctab[0:16] = jnp.where(in_ctx, tcos, pick(tcos, at_m))
        stab[0:16] = jnp.where(in_ctx, tsin, pick(tsin, at_m))
        ctab[16:32] = jnp.where(in_ctx, 1.0, tcos * cos_c + tsin * sin_c)
        stab[16:32] = jnp.where(in_ctx, 0.0, tsin * cos_c - tcos * sin_c)

    def dense(r):
        mixed = jnp.concatenate([ctx_buf[lax.rem(r, 2), core], ctx_recv[lax.rem(r, 2)]], axis=0)
        out_ref[r] = project_out(mixed, wd_sc[...], own[r], bd_ref)

    @pl.when(step > 0)
    def _():
        swap_ctx(step - 1).start()

    @pl.when(step < ROWS)
    def _():
        send_x(step).wait_recv()
        relay(step).start()

    @pl.when(step < ROWS - AHEAD)
    def _():
        send_x(step + AHEAD).start()

    @pl.when(step < ROWS)
    def _():
        build_tables(step)
        send_d(step).wait_recv()

    @pl.when(step < LAST)
    def _():
        multiply(y_0, w_sc, 0, 3 * WIDE, own[step])
        multiply(y_1, w_sc, 0, 3 * WIDE, dbuf[lax.rem(step, 2)])
        finish(y_0, b_sc, 0, me, core * PART, ctab, stab, kt_refs, vt, qbd)
        finish(y_1, b_sc, 0, peer_d, (1 - core) * PART, ctab, stab, kt_refs, vt, qbd)

    @pl.when(step == LAST)
    def _():
        a_last[me] = own[LAST]
        a_last[peer_d] = dbuf[LAST % 2]

    @pl.when(step > 0)
    def _():
        swap_ctx(step - 1).wait()
        dense(step - 1)

    @pl.when(step < ROWS)
    def _():
        relay(step).wait_recv()

    @pl.when(step < ROWS - 1)
    def _():
        send_d(step + 1).start()

    @pl.when(step < LAST)
    def _():
        multiply(y_0, w_sc, 0, 2 * WIDE, xbuf[step])
        multiply(y_1, w_sc, 0, 2 * WIDE, rbuf[lax.rem(step, 2)])

    def rest(r, this_chip):
        finish(y_0, b_sc, 0, peer_x, None, ctab, stab, kt_refs, vt, qbd)
        finish(y_1, b_sc, 0, peer_xd, None, ctab, stab, kt_refs, vt, qbd)
        ko_ref[r, 0:2] = kt_0[...].reshape(2, HEAD, SEQ)
        ko_ref[r, 2] = kt_1[0:HEAD]
        vo_ref[r] = vt[0:192].reshape(3, HEAD, SEQ)
        for pair in range(LOCAL // 2):
            kk[pair] = kt_refs[pair][...].T

        def store(qb, v_rows, value):
            ctx_buf[lax.rem(r, 2), qb, v_rows, :] = value

        spec = ((768, 256), (768, 256)) if this_chip == 0 else ((768, 512), (1024, 768))
        attend(spec, this_chip * CHIP, ctx_ref[r], kk, qbd, vt, s_refs, top_sc, store)

    for this_chip in range(2):
        @pl.when(jnp.logical_and(step < LAST, chip == this_chip))
        def _():
            rest(step, this_chip)

    @pl.when(step == LAST)
    def _():
        a_last[peer_x] = xbuf[LAST]
        a_last[peer_xd] = rbuf[LAST % 2]

        def drain(r, c):
            send_x(r).wait_send()
            relay(r).wait_send()
            send_d(r).wait_send()
            return c

        lax.fori_loop(0, ROWS, drain, 0)


def last_row(ctx_ref, bd_hbm, out_vm, keys_vm, values_vm, a_last, w_sc, b_sc, wd_sc, ctab, stab,
             out_hbm, keys_hbm, values_hbm,
             bd_ref, y_0, y_1, y_2, y_3, kt_0, kt_1, kt_2, vt, kk, qbd, s_0, s_2, top_sc, ctx_buf, out_row, key_row, value_row, sem, row_sem):
    me = lax.axis_index('sp')
    bulk = []
    for i, (src, dst) in enumerate(((keys_vm, keys_hbm), (values_vm, values_hbm), (out_vm, out_hbm))):
        for n in range(3):
            bulk.append(pltpu.make_async_copy(src.at[pl.ds(5 * n, 5)], dst.at[pl.ds(5 * n, 5)], sem.at[3 * i + n]))
    bd_copy = pltpu.make_async_copy(bd_hbm, bd_ref, row_sem.at[3])
    bd_copy.start()
    for c in bulk:
        c.start()
    kt_refs = (kt_0, kt_1, kt_2)
    s_refs = (s_0, None, s_2, None)
    qbd[...] = jnp.zeros_like(qbd)
    row_copies = [pltpu.make_async_copy(src, dst.at[LAST], row_sem.at[i]) for i, (src, dst) in enumerate(((out_row, out_hbm), (key_row, keys_hbm), (value_row, values_hbm)))]
    for group in range(2):
        base = 3 * LOCAL * group
        parts = [me] + [lax.rem(me + n, 4) for n in range(1, 4)]
        y_refs = (y_0, y_1, y_2, y_3)
        for n in range(4):
            multiply(y_refs[n], w_sc, base, 3 * WIDE if n == 0 else 2 * WIDE, a_last[parts[n]])
        for n in range(4):
            finish(y_refs[n], b_sc, base, parts[n], 0 if n == 0 else None, ctab, stab, kt_refs, vt, qbd)
        if group == 0:
            key_row[0:2] = kt_0[...].reshape(2, HEAD, SEQ)
            key_row[2] = kt_1[0:HEAD]
            value_row[...] = vt[0:192].reshape(3, HEAD, SEQ)
        for pair in range(LOCAL // 2):
            kk[pair] = kt_refs[pair][...].T

        def store(qb, v_rows, value):
            ctx_buf[group, v_rows, :] = value

        for live, spec in ((me < 2, (768, 256)), (me == 2, (768, 512)), (me == 3, (1024, 768))):
            @pl.when(live)
            def _():
                attend((spec,), me * PART, ctx_ref[LAST], kk, qbd, vt, s_refs, top_sc, store)

        if group == 0:
            row_copies[1].start()
            row_copies[2].start()
    bd_copy.wait()
    out_row[...] = project_out(ctx_buf[...].reshape(HID, PART), wd_sc[...], a_last[me], bd_ref)
    row_copies[0].start()
    for c in bulk + row_copies:
        c.wait()


def solution(mesh):
    seq_spec = P('dp', 'sp', None)
    row_spec = P('dp', 'sp')
    head_spec = P('dp', None, 'sp', None)
    replicated = P()
    tcos, tsin = rope_tables()

    def local_block(hidden, pos_ids, block_ids, ctx_len, ln_gamma, ln_beta, w_qkv, b_qkv, w_dense, b_dense):
        w_t = jnp.transpose(w_qkv, (1, 2, 3, 0))
        anywhere = pl.BlockSpec(memory_space=pltpu.HBM)

        held = pl.pallas_call(
            kernel,
            grid=(ROWS,),
            out_shape=(
                pltpu.VMEM((ROWS, PART, HID), BF16),
                pltpu.VMEM((ROWS, 3, HEAD, SEQ), BF16),
                pltpu.VMEM((ROWS, 3, HEAD, SEQ), BF16),
                pltpu.VMEM((4, PART, HID), BF16),
                pltpu.VMEM((36, HEAD, HID), BF16),
                pltpu.VMEM((36, HEAD, 128), F32),
                pltpu.VMEM((HID, HID), BF16),
                pltpu.VMEM((32, SEQ), F32),
                pltpu.VMEM((32, SEQ), F32),
            ),
            in_specs=[anywhere, anywhere, pl.BlockSpec(memory_space=pltpu.SMEM)] + [anywhere] * 8,
            out_specs=(pl.BlockSpec(memory_space=pltpu.VMEM),) * 9,
            scratch_shapes=[
                pltpu.VMEM((ROWS, PART), jnp.int32),
                pltpu.VMEM((HID,), BF16),
                pltpu.VMEM((HID,), BF16),
                pltpu.VMEM((HID,), BF16),
                pltpu.VMEM((12, 3, HEAD), BF16),
                pltpu.VMEM((16, SEQ), F32),
                pltpu.VMEM((16, SEQ), F32),
                pltpu.VMEM((ROWS, PART, HID), BF16),
                pltpu.VMEM((ROWS, PART, HID), BF16),
                pltpu.VMEM((2, PART, HID), BF16),
                pltpu.VMEM((2, PART, HID), BF16),
                pltpu.VMEM((4, ROWS, 128), jnp.int32),
                pltpu.VMEM((3 * WIDE, PART), F32),
                pltpu.VMEM((3 * WIDE, PART), F32),
                *[pltpu.VMEM((2 * HEAD, SEQ), BF16)] * 3,
                pltpu.VMEM((WIDE, SEQ), BF16),
                pltpu.VMEM((3, SEQ, 128), BF16),
                pltpu.VMEM((3, 128, 2 * CHIP), BF16),
                *[pltpu.VMEM((SEQ, PART), F32)] * 4,
                pltpu.VMEM((4, 8, PART), F32),
                pltpu.VMEM((2, 2, WIDE, PART), BF16),
                pltpu.VMEM((2, WIDE, PART), BF16),
                pltpu.SemaphoreType.DMA((7,)),
                pltpu.SemaphoreType.DMA((ROWS,)),
                pltpu.SemaphoreType.DMA((16,)),
            ] + [pltpu.SemaphoreType.DMA((ROWS,))] * 8 + [pltpu.SemaphoreType.DMA((3,))] * 2,
            compiler_params=pltpu.CompilerParams(
                collective_id=0, has_side_effects=True, vmem_limit_bytes=34 * 1024 * 1024, dimension_semantics=('arbitrary',)),
            name='glm_block',
        )(hidden, pos_ids, ctx_len, ln_gamma, ln_beta, b_dense,
          w_t, b_qkv, w_dense, jnp.asarray(tcos), jnp.asarray(tsin))
        held = [pltpu.with_memory_space_constraint(x, pltpu.VMEM) for x in held]
        out, keys_t, values_t = pl.pallas_call(
            last_row,
            out_shape=[jax.ShapeDtypeStruct(x.shape, BF16) for x in held[:3]],
            in_specs=[pl.BlockSpec(memory_space=pltpu.SMEM), anywhere] + [pl.BlockSpec(memory_space=pl.ANY)] * 3 + [pl.BlockSpec(memory_space=pltpu.VMEM)] * 6,
            out_specs=[anywhere] * 3,
            scratch_shapes=[
                pltpu.VMEM((HID,), BF16),
                *[pltpu.VMEM((3 * WIDE, PART), F32)] * 4,
                *[pltpu.VMEM((2 * HEAD, SEQ), BF16)] * 3,
                pltpu.VMEM((WIDE, SEQ), BF16),
                pltpu.VMEM((3, SEQ, 128), BF16),
                pltpu.VMEM((3, 128, 2 * PART), BF16),
                *[pltpu.VMEM((SEQ, PART), F32)] * 2,
                pltpu.VMEM((4, 8, PART), F32),
                pltpu.VMEM((2, WIDE, PART), BF16),
                pltpu.VMEM((PART, HID), BF16),
                pltpu.VMEM((3, HEAD, SEQ), BF16),
                pltpu.VMEM((3, HEAD, SEQ), BF16),
                pltpu.SemaphoreType.DMA((9,)),
                pltpu.SemaphoreType.DMA((4,)),
            ],
            compiler_params=pltpu.CompilerParams(vmem_limit_bytes=34 * 1024 * 1024),
            name='last_row',
        )(ctx_len, b_dense, *held)
        return out, jnp.transpose(keys_t, (0, 3, 1, 2)), jnp.transpose(values_t, (0, 3, 1, 2))

    return jax.shard_map(local_block, mesh=mesh, in_specs=(seq_spec, row_spec, row_spec, P('dp'), replicated, replicated, replicated, replicated, replicated, replicated), out_specs=(seq_spec, head_spec, head_spec), check_vma=False)
```

```python
import functools
import math

import jax
import jax.numpy as jnp
import numpy as np
from jax import lax
from jax.experimental import pallas as pl
from jax.experimental.pallas import tpu as pltpu
from jax.sharding import PartitionSpec as P

ALPHA = math.sqrt(56.0)
ROPE_BASE = 10000.0
LN_EPS = 1e-5
MESH = pl.DeviceIdType.MESH
F32 = jnp.float32
BF16 = jnp.bfloat16

ROWS = 16
PART = 256
AHEAD = 4
SEQ = 1024
LAST = ROWS - 1
HID = 768
HEAD = 64
CHIP = 512
LOCAL = 6
WIDE = LOCAL * HEAD
EXP_SCALE = math.log2(math.e) / math.sqrt(HEAD)
CHUNK = 64
MIX = 256


def rope_tables():
    freq = ROPE_BASE ** (-np.arange(0, 32, 2).astype(np.float64) / 32.0)
    angle = freq.astype(np.float32)[:, None] * np.arange(SEQ, dtype=np.float32)[None, :]
    return np.cos(angle.astype(np.float64)).astype(np.float32), np.sin(angle.astype(np.float64)).astype(np.float32)


def nt_dot(a, b):
    return lax.dot_general(a, b, (((1,), (1,)), ((), ())), preferred_element_type=F32)


def multiply(y_ref, w_ref, base, rows, tokens):
    y_ref[0:rows] = nt_dot(w_ref[base:base + rows // HEAD].reshape(rows, HID), tokens)


def finish(y_ref, b_ref, base, part, q_col, ctab, stab, kt_refs, vt, qbd):
    for h in range(LOCAL):
        for lt in range(PART // 128):
            cols = pl.ds(pl.multiple_of(part * PART + lt * 128, 128), 128)
            ycols = slice(lt * 128, lt * 128 + 128)
            for half in range(2):
                cos = ctab[16 * half:16 * half + 16, cols]
                sin = stab[16 * half:16 * half + 16, cols]

                def rotated(kind):
                    u0 = kind * WIDE + h * HEAD + half * 32
                    b0 = half * 32
                    bias = b_ref.at[base + kind * LOCAL + h]
                    u = (y_ref[u0:u0 + 16, ycols] + bias[b0:b0 + 16]).astype(BF16).astype(F32)
                    w = (y_ref[u0 + 16:u0 + 32, ycols] + bias[b0 + 16:b0 + 32]).astype(BF16).astype(F32)
                    return (u * cos - w * sin).astype(BF16), (w * cos + u * sin).astype(BF16)

                k0 = (h % 2) * HEAD + half * 32
                ku, kw = rotated(0)
                kt_refs[h // 2][k0:k0 + 16, cols] = ku
                kt_refs[h // 2][k0 + 16:k0 + 32, cols] = kw
                if q_col is not None:
                    qu, qw = rotated(2)
                    q_width = qbd.shape[2] // 2
                    qc = pl.ds(pl.multiple_of((h % 2) * q_width + q_col + lt * 128, 128), 128)
                    qbd[h // 2, k0:k0 + 16, qc] = qu
                    qbd[h // 2, k0 + 16:k0 + 32, qc] = qw
            v0 = WIDE + h * HEAD
            vt[h * HEAD:(h + 1) * HEAD, cols] = (y_ref[v0:v0 + HEAD, ycols] + b_ref[base + LOCAL + h]).astype(BF16)


def attend(spec, q_first, ctx, kk, qbd, vt, s_refs, top_sc, store):
    def score(pair, j):
        for qb, (key_len, mask_from) in enumerate(spec):
            q0 = (j * len(spec) + qb) * PART
            scores = jnp.dot(kk[pair, 0:key_len, :], qbd[pair, :, q0:q0 + PART], preferred_element_type=F32)
            q_pos = q_first + qb * PART + lax.broadcasted_iota(jnp.int32, (1, PART), 1)
            limit = jnp.maximum(q_pos, ctx - 1)
            top = None
            for k0 in range(0, key_len, CHUNK):
                part = scores[k0:k0 + CHUNK]
                if k0 >= mask_from:
                    k_pos = k0 + lax.broadcasted_iota(jnp.int32, (CHUNK, PART), 0)
                    part = jnp.where(k_pos <= limit, part, -jnp.inf)
                s_refs[2 * j + qb][k0:k0 + CHUNK] = part
                peak = jnp.max(part.reshape(CHUNK // 8, 8, PART), axis=0)
                top = peak if top is None else jnp.maximum(top, peak)
            top_sc[2 * j + qb] = jnp.broadcast_to(jnp.max(top, axis=0, keepdims=True) * EXP_SCALE, (8, PART))

    def mix(pair, j):
        v_rows = pl.ds(pl.multiple_of((2 * pair + j) * HEAD, HEAD), HEAD)
        for qb, (key_len, _) in enumerate(spec):
            top = top_sc[2 * j + qb, 0:1]
            total = jnp.zeros((8, PART), F32)
            mixed = None
            for k0 in range(0, key_len, MIX):
                probs = []
                for k1 in range(k0, k0 + MIX, CHUNK):
                    prob = jnp.exp2(s_refs[2 * j + qb][k1:k1 + CHUNK] * EXP_SCALE - top)
                    total = total + jnp.sum(prob.reshape(CHUNK // 8, 8, PART), axis=0)
                    probs.append(prob.astype(BF16))
                some = jnp.dot(vt[v_rows, k0:k0 + MIX], jnp.concatenate(probs, axis=0), preferred_element_type=F32)
                mixed = some if mixed is None else mixed + some
            store(qb, v_rows, (mixed * (1.0 / jnp.sum(total, axis=0, keepdims=True))).astype(BF16))

    score(0, 0)

    def one_pair(pair, c):
        score(pair, 1)
        mix(pair, 0)
        score(pair + 1, 0)
        mix(pair, 1)
        return c

    lax.fori_loop(0, LOCAL // 2 - 1, one_pair, 0)
    score(LOCAL // 2 - 1, 1)
    mix(LOCAL // 2 - 1, 0)
    mix(LOCAL // 2 - 1, 1)


def project_out(mixed, wd, normed, bd_ref):
    dense_out = lax.dot_general(mixed, wd, (((0,), (0,)), ((), ())), preferred_element_type=F32)
    return (normed.astype(F32) * ALPHA + dense_out + bd_ref[...].astype(F32).reshape(1, HID)).astype(BF16)


def kernel(hid_hbm, pos_hbm, ctx_ref, gamma_hbm, beta_hbm, bd_hbm, w_hbm, bias_hbm, wd_hbm, tcos_hbm, tsin_hbm,
           out_ref, ko_ref, vo_ref, a_last, w_sc, b_sc, wd_sc, ctab, stab, k_last, v_last, q_last,
           pos_ref, gamma_ref, beta_ref, bd_ref, bias_ref, tcos_ref, tsin_ref, own, xbuf, dbuf, rbuf, posr, y_0, y_1, kt_0, kt_1, kt_2, vt, kk, qbd, s_0, s_1, s_2, s_3, top_sc, ctx_buf, ctx_recv,
           t_sem, hid_sem, w_sem, xs_sem, xr_sem, ds_sem, dr_sem, rs_sem, rr_sem, cs_sem, cr_sem, ps_sem, pr_sem):
    step = pl.program_id(0)
    s_refs, kt_refs = (s_0, s_1, s_2, s_3), (kt_0, kt_1, kt_2)
    me = lax.axis_index('sp')
    core = lax.rem(me, 2)
    chip = me // 2
    other = 1 - chip
    peer_x = other * 2 + core
    peer_d = chip * 2 + 1 - core
    peer_xd = other * 2 + 1 - core

    def remote(src, dst, send_sem, recv_sem, peer):
        return pltpu.make_async_remote_copy(src, dst, send_sem, recv_sem, device_id={'sp': peer}, device_id_type=MESH)

    def send_x(r):
        return remote(own.at[r], xbuf.at[r], xs_sem.at[r], xr_sem.at[r], peer_x)

    def send_d(r):
        return remote(own.at[r], dbuf.at[lax.rem(r, 2)], ds_sem.at[r], dr_sem.at[r], peer_d)

    def relay(r):
        return remote(xbuf.at[r], rbuf.at[lax.rem(r, 2)], rs_sem.at[r], rr_sem.at[r], peer_d)

    def swap_ctx(r):
        return remote(ctx_buf.at[lax.rem(r, 2), 1 - core], ctx_recv.at[lax.rem(r, 2)], cs_sem.at[r], cr_sem.at[r], peer_d)

    def swap_pos(n, peer):
        return remote(pos_ref.at[:, pl.ds(128, 128)], posr.at[me], ps_sem.at[n], pr_sem.at[n], peer)

    def recv_pos(n, peer):
        return remote(pos_ref.at[:, pl.ds(128, 128)], posr.at[peer], ps_sem.at[n], pr_sem.at[n], peer)

    def load_hidden(r):
        return pltpu.make_async_copy(hid_hbm.at[r], own.at[r], hid_sem.at[r])

    def small_copies():
        pairs = ((gamma_hbm, gamma_ref), (beta_hbm, beta_ref), (pos_hbm, pos_ref), (bd_hbm, bd_ref), (bias_hbm, bias_ref), (tcos_hbm, tcos_ref), (tsin_hbm, tsin_ref))
        return [pltpu.make_async_copy(src, dst, t_sem.at[i]) for i, (src, dst) in enumerate(pairs)]

    def weight_copies():
        copies = []
        for group, owner in enumerate((me, peer_x, peer_d, peer_xd)):
            for slot, kind in ((0, 1), (6, 2), (12, 0)):
                copies.append((w_hbm.at[pl.ds(owner * 3, 3), kind], w_sc.at[pl.ds(18 * (group // 2) + slot + 3 * (group % 2), 3)]))
        for slot, owner in enumerate((me, peer_x, peer_d, peer_xd)):
            copies.append((wd_hbm.at[pl.ds(pl.multiple_of(owner * 192, 64), 192)], wd_sc.at[pl.ds(slot * 192, 192)]))
        return [pltpu.make_async_copy(src, dst, w_sem.at[i]) for i, (src, dst) in enumerate(copies)]

    def norm_row(r):
        gamma = gamma_ref[...].astype(F32).reshape(1, HID)
        beta = beta_ref[...].astype(F32).reshape(1, HID)
        for t in range(0, PART, 32):
            rows = pl.ds(t, 32)
            wide = own[r, rows, :].astype(F32)
            mean = jnp.sum(wide, axis=-1, keepdims=True) * (1.0 / HID)
            cent = wide - mean
            var = jnp.sum(cent * cent, axis=-1, keepdims=True) * (1.0 / HID)
            own[r, rows, :] = (cent * lax.rsqrt(var + LN_EPS) * gamma + beta).astype(BF16)

    def spread_bias():
        for group, owner in enumerate((me, peer_x, peer_d, peer_xd)):
            for slot, kind in ((0, 1), (6, 2), (12, 0)):
                for h in range(3):
                    row = bias_ref[owner * 3 + h, kind:kind + 1, :].astype(F32)
                    b_sc[18 * (group // 2) + slot + 3 * (group % 2) + h] = jnp.broadcast_to(row, (128, HEAD)).T

    @pl.when(step == 0)
    def _():
        small = small_copies()
        for c in small[:2]:
            c.start()

        def fetch(r, c):
            load_hidden(r).start()
            return c

        lax.fori_loop(0, ROWS, fetch, 0)
        barrier = pltpu.get_barrier_semaphore()
        for peer in (peer_x, peer_d, peer_xd):
            pl.semaphore_signal(barrier, inc=1, device_id={'sp': peer}, device_id_type=MESH)
        for c in small[2:] + weight_copies():
            c.start()
        for c in small[:2]:
            c.wait()
        load_hidden(0).wait()
        norm_row(0)
        pl.semaphore_wait(barrier, 3)
        load_hidden(1).wait()
        norm_row(1)
        send_x(0).start()

        def norm_and_send(r, c):
            load_hidden(r).wait()
            norm_row(r)

            @pl.when(r <= AHEAD)
            def _():
                send_x(r - 1).start()

            return c

        lax.fori_loop(2, ROWS, norm_and_send, 0)
        for c in small[2:]:
            c.wait()
        for n, peer in enumerate((peer_x, peer_d, peer_xd)):
            swap_pos(n, peer).start()
        send_d(0).start()
        posr[me] = pos_ref[:, 128:256]
        qbd[...] = jnp.zeros_like(qbd)
        spread_bias()
        for c in weight_copies():
            c.wait()
        for n, peer in enumerate((peer_x, peer_d, peer_xd)):
            recv_pos(n, peer).wait()

    def build_tables(r):
        tcos = tcos_ref[...]
        tsin = tsin_ref[...]
        lane = lax.broadcasted_iota(jnp.int32, (16, SEQ), 1)
        ctx = ctx_ref[r]
        last = posr[3, pl.ds(r, 1), :]
        last_lane = lax.broadcasted_iota(jnp.int32, (1, 128), 1)
        m_pos = jnp.sum(jnp.where(last_lane == 127, last, 0), axis=1, keepdims=True)

        def pick(table, hit):
            return jnp.sum(jnp.where(hit, table, 0.0), axis=1, keepdims=True)

        at_m = lane == m_pos
        at_c = lane == ctx - 1
        in_ctx = lane < ctx
        cos_c, sin_c = pick(tcos, at_c), pick(tsin, at_c)
        ctab[0:16] = jnp.where(in_ctx, tcos, pick(tcos, at_m))
        stab[0:16] = jnp.where(in_ctx, tsin, pick(tsin, at_m))
        ctab[16:32] = jnp.where(in_ctx, 1.0, tcos * cos_c + tsin * sin_c)
        stab[16:32] = jnp.where(in_ctx, 0.0, tsin * cos_c - tcos * sin_c)

    def dense(r):
        mixed = jnp.concatenate([ctx_buf[lax.rem(r, 2), core], ctx_recv[lax.rem(r, 2)]], axis=0)
        out_ref[r] = project_out(mixed, wd_sc[...], own[r], bd_ref)

    @pl.when(step > 0)
    def _():
        swap_ctx(step - 1).start()

    @pl.when(step == LAST)
    def _():
        build_tables(step)
        send_d(step).wait_recv()
        q_last[...] = jnp.zeros_like(q_last)
        for group in range(2):
            base = 3 * LOCAL * group
            multiply(y_0, w_sc, base, 3 * WIDE, own[LAST])
            multiply(y_1, w_sc, base, 2 * WIDE, dbuf[LAST % 2])
            last_refs = [k_last.at[group, pair] for pair in range(LOCAL // 2)]
            finish(y_0, b_sc, base, me, 0, ctab, stab, last_refs, v_last.at[group], q_last.at[group])
            finish(y_1, b_sc, base, peer_d, None, ctab, stab, last_refs, v_last.at[group], None)

    send_x(step).wait_recv()
    relay(step).start()

    @pl.when(step < ROWS - AHEAD)
    def _():
        send_x(step + AHEAD).start()

    @pl.when(step < LAST)
    def _():
        build_tables(step)
        send_d(step).wait_recv()
        multiply(y_0, w_sc, 0, 3 * WIDE, own[step])
        multiply(y_1, w_sc, 0, 3 * WIDE, dbuf[lax.rem(step, 2)])
        finish(y_0, b_sc, 0, me, core * PART, ctab, stab, kt_refs, vt, qbd)
        finish(y_1, b_sc, 0, peer_d, (1 - core) * PART, ctab, stab, kt_refs, vt, qbd)

    @pl.when(step == LAST)
    def _():
        a_last[0] = own[LAST]
        multiply(y_0, w_sc, 0, 2 * WIDE, xbuf[LAST])
        multiply(y_1, w_sc, 3 * LOCAL, 2 * WIDE, xbuf[LAST])
        for group in range(2):
            last_refs = [k_last.at[group, pair] for pair in range(LOCAL // 2)]
            finish((y_0, y_1)[group], b_sc, 3 * LOCAL * group, peer_x, None, ctab, stab, last_refs, v_last.at[group], None)

    @pl.when(step > 0)
    def _():
        swap_ctx(step - 1).wait()
        dense(step - 1)

    @pl.when(step < ROWS)
    def _():
        relay(step).wait_recv()

    @pl.when(step < ROWS - 1)
    def _():
        send_d(step + 1).start()

    @pl.when(step < LAST)
    def _():
        multiply(y_0, w_sc, 0, 2 * WIDE, xbuf[step])
        multiply(y_1, w_sc, 0, 2 * WIDE, rbuf[lax.rem(step, 2)])

    def rest(r, this_chip):
        finish(y_0, b_sc, 0, peer_x, None, ctab, stab, kt_refs, vt, qbd)
        finish(y_1, b_sc, 0, peer_xd, None, ctab, stab, kt_refs, vt, qbd)
        ko_ref[r, 0:2] = kt_0[...].reshape(2, HEAD, SEQ)
        ko_ref[r, 2] = kt_1[0:HEAD]
        vo_ref[r] = vt[0:192].reshape(3, HEAD, SEQ)
        for pair in range(LOCAL // 2):
            kk[pair] = kt_refs[pair][...].T

        def store(qb, v_rows, value):
            ctx_buf[lax.rem(r, 2), qb, v_rows, :] = value

        spec = ((768, 256), (768, 256)) if this_chip == 0 else ((768, 512), (1024, 768))
        attend(spec, this_chip * CHIP, ctx_ref[r], kk, qbd, vt, s_refs, top_sc, store)

    for this_chip in range(2):
        @pl.when(jnp.logical_and(step < LAST, chip == this_chip))
        def _():
            rest(step, this_chip)

    @pl.when(step == LAST)
    def _():
        a_last[1] = rbuf[LAST % 2]

        def drain(r, c):
            send_x(r).wait_send()
            relay(r).wait_send()
            send_d(r).wait_send()
            return c

        lax.fori_loop(0, ROWS, drain, 0)


def last_row(ctx_ref, bd_hbm, out_vm, keys_vm, values_vm, a_last, w_sc, b_sc, wd_sc, ctab, stab, k_last, v_last, q_last,
             out_hbm, keys_hbm, values_hbm,
             bd_ref, y_0, y_1, kt_0, kt_1, kt_2, vt, kk, s_0, s_2, top_sc, ctx_buf, out_row, key_row, value_row, sem, row_sem):
    me = lax.axis_index('sp')
    bulk = []
    for i, (src, dst) in enumerate(((keys_vm, keys_hbm), (values_vm, values_hbm), (out_vm, out_hbm))):
        for n in range(3):
            bulk.append(pltpu.make_async_copy(src.at[pl.ds(5 * n, 5)], dst.at[pl.ds(5 * n, 5)], sem.at[3 * i + n]))
    bd_copy = pltpu.make_async_copy(bd_hbm, bd_ref, row_sem.at[3])
    bd_copy.start()
    for c in bulk:
        c.start()
    kt_refs = (kt_0, kt_1, kt_2)
    s_refs = (s_0, None, s_2, None)
    row_copies = [pltpu.make_async_copy(src, dst.at[LAST], row_sem.at[i]) for i, (src, dst) in enumerate(((out_row, out_hbm), (key_row, keys_hbm), (value_row, values_hbm)))]
    far = 3 - me
    for group in range(2):
        multiply((y_0, y_1)[group], w_sc, 3 * LOCAL * group, 2 * WIDE, a_last[1])
    for group in range(2):
        for pair in range(LOCAL // 2):
            kt_refs[pair][...] = k_last[group, pair]
        vt[...] = v_last[group]
        finish((y_0, y_1)[group], b_sc, 3 * LOCAL * group, far, None, ctab, stab, kt_refs, vt, None)
        if group == 0:
            key_row[0:2] = kt_0[...].reshape(2, HEAD, SEQ)
            key_row[2] = kt_1[0:HEAD]
            value_row[...] = vt[0:192].reshape(3, HEAD, SEQ)
        for pair in range(LOCAL // 2):
            kk[pair] = kt_refs[pair][...].T

        def store(qb, v_rows, value):
            ctx_buf[group, v_rows, :] = value

        for live, spec in ((me < 2, (768, 256)), (me == 2, (768, 512)), (me == 3, (1024, 768))):
            @pl.when(live)
            def _():
                attend((spec,), me * PART, ctx_ref[LAST], kk, q_last.at[group], vt, s_refs, top_sc, store)

        if group == 0:
            row_copies[1].start()
            row_copies[2].start()
    bd_copy.wait()
    out_row[...] = project_out(ctx_buf[...].reshape(HID, PART), wd_sc[...], a_last[0], bd_ref)
    row_copies[0].start()
    for c in bulk + row_copies:
        c.wait()


def solution(mesh):
    seq_spec = P('dp', 'sp', None)
    row_spec = P('dp', 'sp')
    head_spec = P('dp', None, 'sp', None)
    replicated = P()
    tcos, tsin = rope_tables()

    def local_block(hidden, pos_ids, block_ids, ctx_len, ln_gamma, ln_beta, w_qkv, b_qkv, w_dense, b_dense):
        w_t = jnp.transpose(w_qkv, (1, 2, 3, 0))
        anywhere = pl.BlockSpec(memory_space=pltpu.HBM)

        held = pl.pallas_call(
            kernel,
            grid=(ROWS,),
            out_shape=(
                pltpu.VMEM((ROWS, PART, HID), BF16),
                pltpu.VMEM((ROWS, 3, HEAD, SEQ), BF16),
                pltpu.VMEM((ROWS, 3, HEAD, SEQ), BF16),
                pltpu.VMEM((2, PART, HID), BF16),
                pltpu.VMEM((36, HEAD, HID), BF16),
                pltpu.VMEM((36, HEAD, 128), F32),
                pltpu.VMEM((HID, HID), BF16),
                pltpu.VMEM((32, SEQ), F32),
                pltpu.VMEM((32, SEQ), F32),
                pltpu.VMEM((2, LOCAL // 2, 2 * HEAD, SEQ), BF16),
                pltpu.VMEM((2, WIDE, SEQ), BF16),
                pltpu.VMEM((2, LOCAL // 2, 2 * HEAD, 2 * PART), BF16),
            ),
            in_specs=[anywhere, anywhere, pl.BlockSpec(memory_space=pltpu.SMEM)] + [anywhere] * 8,
            out_specs=(pl.BlockSpec(memory_space=pltpu.VMEM),) * 12,
            scratch_shapes=[
                pltpu.VMEM((ROWS, PART), jnp.int32),
                pltpu.VMEM((HID,), BF16),
                pltpu.VMEM((HID,), BF16),
                pltpu.VMEM((HID,), BF16),
                pltpu.VMEM((12, 3, HEAD), BF16),
                pltpu.VMEM((16, SEQ), F32),
                pltpu.VMEM((16, SEQ), F32),
                pltpu.VMEM((ROWS, PART, HID), BF16),
                pltpu.VMEM((ROWS, PART, HID), BF16),
                pltpu.VMEM((2, PART, HID), BF16),
                pltpu.VMEM((2, PART, HID), BF16),
                pltpu.VMEM((4, ROWS, 128), jnp.int32),
                pltpu.VMEM((3 * WIDE, PART), F32),
                pltpu.VMEM((3 * WIDE, PART), F32),
                *[pltpu.VMEM((2 * HEAD, SEQ), BF16)] * 3,
                pltpu.VMEM((WIDE, SEQ), BF16),
                pltpu.VMEM((3, SEQ, 128), BF16),
                pltpu.VMEM((3, 128, 2 * CHIP), BF16),
                *[pltpu.VMEM((SEQ, PART), F32)] * 4,
                pltpu.VMEM((4, 8, PART), F32),
                pltpu.VMEM((2, 2, WIDE, PART), BF16),
                pltpu.VMEM((2, WIDE, PART), BF16),
                pltpu.SemaphoreType.DMA((7,)),
                pltpu.SemaphoreType.DMA((ROWS,)),
                pltpu.SemaphoreType.DMA((16,)),
            ] + [pltpu.SemaphoreType.DMA((ROWS,))] * 8 + [pltpu.SemaphoreType.DMA((3,))] * 2,
            compiler_params=pltpu.CompilerParams(
                collective_id=0, has_side_effects=True, vmem_limit_bytes=32 * 1024 * 1024, dimension_semantics=('arbitrary',)),
            name='glm_block',
        )(hidden, pos_ids, ctx_len, ln_gamma, ln_beta, b_dense,
          w_t, b_qkv, w_dense, jnp.asarray(tcos), jnp.asarray(tsin))
        held = [pltpu.with_memory_space_constraint(x, pltpu.VMEM) for x in held]
        out, keys_t, values_t = pl.pallas_call(
            last_row,
            out_shape=[jax.ShapeDtypeStruct(x.shape, BF16) for x in held[:3]],
            in_specs=[pl.BlockSpec(memory_space=pltpu.SMEM), anywhere] + [pl.BlockSpec(memory_space=pl.ANY)] * 3 + [pl.BlockSpec(memory_space=pltpu.VMEM)] * 9,
            out_specs=[anywhere] * 3,
            scratch_shapes=[
                pltpu.VMEM((HID,), BF16),
                *[pltpu.VMEM((2 * WIDE, PART), F32)] * 2,
                *[pltpu.VMEM((2 * HEAD, SEQ), BF16)] * 3,
                pltpu.VMEM((WIDE, SEQ), BF16),
                pltpu.VMEM((3, SEQ, 128), BF16),
                *[pltpu.VMEM((SEQ, PART), F32)] * 2,
                pltpu.VMEM((4, 8, PART), F32),
                pltpu.VMEM((2, WIDE, PART), BF16),
                pltpu.VMEM((PART, HID), BF16),
                pltpu.VMEM((3, HEAD, SEQ), BF16),
                pltpu.VMEM((3, HEAD, SEQ), BF16),
                pltpu.SemaphoreType.DMA((9,)),
                pltpu.SemaphoreType.DMA((4,)),
            ],
            compiler_params=pltpu.CompilerParams(vmem_limit_bytes=32 * 1024 * 1024),
            name='last_row',
        )(ctx_len, b_dense, *held)
        return out, jnp.transpose(keys_t, (0, 3, 1, 2)), jnp.transpose(values_t, (0, 3, 1, 2))

    return jax.shard_map(local_block, mesh=mesh, in_specs=(seq_spec, row_spec, row_spec, P('dp'), replicated, replicated, replicated, replicated, replicated, replicated), out_specs=(seq_spec, head_spec, head_spec), check_vma=False)
```

```python
import functools
import math

import jax
import jax.numpy as jnp
import numpy as np
from jax import lax
from jax.experimental import pallas as pl
from jax.experimental.pallas import tpu as pltpu
from jax.sharding import PartitionSpec as P

ALPHA = math.sqrt(56.0)
ROPE_BASE = 10000.0
LN_EPS = 1e-5
MESH = pl.DeviceIdType.MESH
F32 = jnp.float32
BF16 = jnp.bfloat16

ROWS = 16
PART = 256
AHEAD = 4
SEQ = 1024
LAST = ROWS - 1
HID = 768
HEAD = 64
CHIP = 512
LOCAL = 6
WIDE = LOCAL * HEAD
EXP_SCALE = math.log2(math.e) / math.sqrt(HEAD)
CHUNK = 64
MIX = 256


def rope_tables():
    freq = ROPE_BASE ** (-np.arange(0, 32, 2).astype(np.float64) / 32.0)
    angle = freq.astype(np.float32)[:, None] * np.arange(SEQ, dtype=np.float32)[None, :]
    return np.cos(angle.astype(np.float64)).astype(np.float32), np.sin(angle.astype(np.float64)).astype(np.float32)


def nt_dot(a, b):
    return lax.dot_general(a, b, (((1,), (1,)), ((), ())), preferred_element_type=F32)


def multiply(y_ref, w_ref, base, rows, tokens):
    y_ref[0:rows] = nt_dot(w_ref[base:base + rows // HEAD].reshape(rows, HID), tokens)


def finish(y_ref, b_ref, base, part, q_col, ctab, stab, kt_refs, vt, qbd):
    for h in range(LOCAL):
        for lt in range(PART // 128):
            cols = pl.ds(pl.multiple_of(part * PART + lt * 128, 128), 128)
            ycols = slice(lt * 128, lt * 128 + 128)
            for half in range(2):
                cos = ctab[16 * half:16 * half + 16, cols]
                sin = stab[16 * half:16 * half + 16, cols]

                def rotated(kind):
                    u0 = kind * WIDE + h * HEAD + half * 32
                    b0 = half * 32
                    bias = b_ref.at[base + kind * LOCAL + h]
                    u = (y_ref[u0:u0 + 16, ycols] + bias[b0:b0 + 16]).astype(BF16).astype(F32)
                    w = (y_ref[u0 + 16:u0 + 32, ycols] + bias[b0 + 16:b0 + 32]).astype(BF16).astype(F32)
                    return (u * cos - w * sin).astype(BF16), (w * cos + u * sin).astype(BF16)

                k0 = (h % 2) * HEAD + half * 32
                ku, kw = rotated(0)
                kt_refs[h // 2][k0:k0 + 16, cols] = ku
                kt_refs[h // 2][k0 + 16:k0 + 32, cols] = kw
                if q_col is not None:
                    qu, qw = rotated(2)
                    q_width = qbd.shape[2] // 2
                    qc = pl.ds(pl.multiple_of((h % 2) * q_width + q_col + lt * 128, 128), 128)
                    qbd[h // 2, k0:k0 + 16, qc] = qu
                    qbd[h // 2, k0 + 16:k0 + 32, qc] = qw
            v0 = WIDE + h * HEAD
            vt[h * HEAD:(h + 1) * HEAD, cols] = (y_ref[v0:v0 + HEAD, ycols] + b_ref[base + LOCAL + h]).astype(BF16)


def attend(spec, q_first, ctx, kk, qbd, vt, s_refs, top_sc, store):
    def score(pair, j):
        for qb, (key_len, mask_from) in enumerate(spec):
            q0 = (j * len(spec) + qb) * PART
            scores = jnp.dot(kk[pair, 0:key_len, :], qbd[pair, :, q0:q0 + PART], preferred_element_type=F32)
            q_pos = q_first + qb * PART + lax.broadcasted_iota(jnp.int32, (1, PART), 1)
            limit = jnp.maximum(q_pos, ctx - 1)
            top = None
            for k0 in range(0, key_len, CHUNK):
                part = scores[k0:k0 + CHUNK]
                if k0 >= mask_from:
                    k_pos = k0 + lax.broadcasted_iota(jnp.int32, (CHUNK, PART), 0)
                    part = jnp.where(k_pos <= limit, part, -jnp.inf)
                s_refs[2 * j + qb][k0:k0 + CHUNK] = part
                peak = jnp.max(part.reshape(CHUNK // 8, 8, PART), axis=0)
                top = peak if top is None else jnp.maximum(top, peak)
            top_sc[2 * j + qb] = jnp.broadcast_to(jnp.max(top, axis=0, keepdims=True) * EXP_SCALE, (8, PART))

    def mix(pair, j):
        v_rows = pl.ds(pl.multiple_of((2 * pair + j) * HEAD, HEAD), HEAD)
        for qb, (key_len, _) in enumerate(spec):
            top = top_sc[2 * j + qb, 0:1]
            total = jnp.zeros((8, PART), F32)
            mixed = None
            for k0 in range(0, key_len, MIX):
                probs = []
                for k1 in range(k0, k0 + MIX, CHUNK):
                    prob = jnp.exp2(s_refs[2 * j + qb][k1:k1 + CHUNK] * EXP_SCALE - top)
                    total = total + jnp.sum(prob.reshape(CHUNK // 8, 8, PART), axis=0)
                    probs.append(prob.astype(BF16))
                some = jnp.dot(vt[v_rows, k0:k0 + MIX], jnp.concatenate(probs, axis=0), preferred_element_type=F32)
                mixed = some if mixed is None else mixed + some
            store(qb, v_rows, (mixed * (1.0 / jnp.sum(total, axis=0, keepdims=True))).astype(BF16))

    score(0, 0)

    def one_pair(pair, c):
        score(pair, 1)
        mix(pair, 0)
        score(pair + 1, 0)
        mix(pair, 1)
        return c

    lax.fori_loop(0, LOCAL // 2 - 1, one_pair, 0)
    score(LOCAL // 2 - 1, 1)
    mix(LOCAL // 2 - 1, 0)
    mix(LOCAL // 2 - 1, 1)


def project_out(mixed, wd, normed, bd_ref):
    dense_out = lax.dot_general(mixed, wd, (((0,), (0,)), ((), ())), preferred_element_type=F32)
    return (normed.astype(F32) * ALPHA + dense_out + bd_ref[...].astype(F32).reshape(1, HID)).astype(BF16)


def kernel(hid_hbm, pos_hbm, ctx_ref, gamma_hbm, beta_hbm, bd_hbm, w_hbm, bias_hbm, wd_hbm, tcos_hbm, tsin_hbm,
           out_ref, ko_ref, vo_ref, a_last, w_sc, b_sc, wd_sc, ctab, stab, k_last, v_last, q_last,
           pos_ref, gamma_ref, beta_ref, bd_ref, bias_ref, tcos_ref, tsin_ref, own, xbuf, dbuf, rbuf, posr, y_0, y_1, kt_0, kt_1, kt_2, vt, kk, qbd, s_0, s_1, s_2, s_3, top_sc, ctx_buf, ctx_recv,
           t_sem, hid_sem, w_sem, xs_sem, xr_sem, ds_sem, dr_sem, rs_sem, rr_sem, cs_sem, cr_sem, ps_sem, pr_sem):
    step = pl.program_id(0)
    s_refs, kt_refs = (s_0, s_1, s_2, s_3), (kt_0, kt_1, kt_2)
    me = lax.axis_index('sp')
    core = lax.rem(me, 2)
    chip = me // 2
    other = 1 - chip
    peer_x = other * 2 + core
    peer_d = chip * 2 + 1 - core
    peer_xd = other * 2 + 1 - core

    def remote(src, dst, send_sem, recv_sem, peer):
        return pltpu.make_async_remote_copy(src, dst, send_sem, recv_sem, device_id={'sp': peer}, device_id_type=MESH)

    def send_x(r):
        return remote(own.at[r], xbuf.at[r], xs_sem.at[r], xr_sem.at[r], peer_x)

    def send_d(r):
        return remote(own.at[r], dbuf.at[lax.rem(r, 2)], ds_sem.at[r], dr_sem.at[r], peer_d)

    def send_d_last():
        return remote(own.at[LAST], dbuf.at[2], ds_sem.at[LAST], dr_sem.at[LAST], peer_d)

    def relay(r):
        return remote(xbuf.at[r], rbuf.at[lax.rem(r, 2)], rs_sem.at[r], rr_sem.at[r], peer_d)

    def swap_ctx(r):
        return remote(ctx_buf.at[lax.rem(r, 2), 1 - core], ctx_recv.at[lax.rem(r, 2)], cs_sem.at[r], cr_sem.at[r], peer_d)

    def swap_pos(n, peer):
        return remote(pos_ref.at[:, pl.ds(128, 128)], posr.at[me], ps_sem.at[n], pr_sem.at[n], peer)

    def recv_pos(n, peer):
        return remote(pos_ref.at[:, pl.ds(128, 128)], posr.at[peer], ps_sem.at[n], pr_sem.at[n], peer)

    def load_hidden(r):
        return pltpu.make_async_copy(hid_hbm.at[r], own.at[r], hid_sem.at[r])

    def small_copies():
        pairs = ((gamma_hbm, gamma_ref), (beta_hbm, beta_ref), (pos_hbm, pos_ref), (bd_hbm, bd_ref), (bias_hbm, bias_ref), (tcos_hbm, tcos_ref), (tsin_hbm, tsin_ref))
        return [pltpu.make_async_copy(src, dst, t_sem.at[i]) for i, (src, dst) in enumerate(pairs)]

    def weight_copies():
        copies = []
        for group, owner in enumerate((me, peer_x, peer_d, peer_xd)):
            for slot, kind in ((0, 1), (6, 2), (12, 0)):
                copies.append((w_hbm.at[pl.ds(owner * 3, 3), kind], w_sc.at[pl.ds(18 * (group // 2) + slot + 3 * (group % 2), 3)]))
        for slot, owner in enumerate((me, peer_x, peer_d, peer_xd)):
            copies.append((wd_hbm.at[pl.ds(pl.multiple_of(owner * 192, 64), 192)], wd_sc.at[pl.ds(slot * 192, 192)]))
        return [pltpu.make_async_copy(src, dst, w_sem.at[i]) for i, (src, dst) in enumerate(copies)]

    def norm_row(r):
        gamma = gamma_ref[...].astype(F32).reshape(1, HID)
        beta = beta_ref[...].astype(F32).reshape(1, HID)
        for t in range(0, PART, 32):
            rows = pl.ds(t, 32)
            wide = own[r, rows, :].astype(F32)
            mean = jnp.sum(wide, axis=-1, keepdims=True) * (1.0 / HID)
            cent = wide - mean
            var = jnp.sum(cent * cent, axis=-1, keepdims=True) * (1.0 / HID)
            own[r, rows, :] = (cent * lax.rsqrt(var + LN_EPS) * gamma + beta).astype(BF16)

    def spread_bias():
        for group, owner in enumerate((me, peer_x, peer_d, peer_xd)):
            for slot, kind in ((0, 1), (6, 2), (12, 0)):
                for h in range(3):
                    row = bias_ref[owner * 3 + h, kind:kind + 1, :].astype(F32)
                    b_sc[18 * (group // 2) + slot + 3 * (group % 2) + h] = jnp.broadcast_to(row, (128, HEAD)).T

    @pl.when(step == 0)
    def _():
        small = small_copies()
        for c in small[:2]:
            c.start()

        def fetch(r, c):
            load_hidden(r).start()
            return c

        lax.fori_loop(0, ROWS, fetch, 0)
        barrier = pltpu.get_barrier_semaphore()
        for peer in (peer_x, peer_d, peer_xd):
            pl.semaphore_signal(barrier, inc=1, device_id={'sp': peer}, device_id_type=MESH)
        for c in small[:2]:
            c.wait()
        load_hidden(0).wait()
        norm_row(0)
        for c in small[2:] + weight_copies():
            c.start()
        pl.semaphore_wait(barrier, 3)
        send_x(0).start()
        load_hidden(1).wait()
        norm_row(1)

        def norm_and_send(r, c):
            load_hidden(r).wait()
            norm_row(r)

            @pl.when(r <= AHEAD)
            def _():
                send_x(r - 1).start()

            return c

        lax.fori_loop(2, ROWS, norm_and_send, 0)
        for c in small[2:]:
            c.wait()
        for n, peer in enumerate((peer_x, peer_d, peer_xd)):
            swap_pos(n, peer).start()
        send_d(0).start()
        send_d_last().start()
        posr[me] = pos_ref[:, 128:256]
        qbd[...] = jnp.zeros_like(qbd)
        spread_bias()
        for c in weight_copies():
            c.wait()
        for n, peer in enumerate((peer_x, peer_d, peer_xd)):
            recv_pos(n, peer).wait()

    def build_tables(r):
        tcos = tcos_ref[...]
        tsin = tsin_ref[...]
        lane = lax.broadcasted_iota(jnp.int32, (16, SEQ), 1)
        ctx = ctx_ref[r]
        last = posr[3, pl.ds(r, 1), :]
        last_lane = lax.broadcasted_iota(jnp.int32, (1, 128), 1)
        m_pos = jnp.sum(jnp.where(last_lane == 127, last, 0), axis=1, keepdims=True)

        def pick(table, hit):
            return jnp.sum(jnp.where(hit, table, 0.0), axis=1, keepdims=True)

        at_m = lane == m_pos
        at_c = lane == ctx - 1
        in_ctx = lane < ctx
        cos_c, sin_c = pick(tcos, at_c), pick(tsin, at_c)
        ctab[0:16] = jnp.where(in_ctx, tcos, pick(tcos, at_m))
        stab[0:16] = jnp.where(in_ctx, tsin, pick(tsin, at_m))
        ctab[16:32] = jnp.where(in_ctx, 1.0, tcos * cos_c + tsin * sin_c)
        stab[16:32] = jnp.where(in_ctx, 0.0, tsin * cos_c - tcos * sin_c)

    def dense(r):
        mixed = jnp.concatenate([ctx_buf[lax.rem(r, 2), core], ctx_recv[lax.rem(r, 2)]], axis=0)
        out_ref[r] = project_out(mixed, wd_sc[...], own[r], bd_ref)

    @pl.when(step > 0)
    def _():
        swap_ctx(step - 1).start()

    @pl.when(step == 0)
    def _():
        build_tables(LAST)
        send_d_last().wait_recv()
        q_last[...] = jnp.zeros_like(q_last)
        for group in range(2):
            base = 3 * LOCAL * group
            multiply(y_0, w_sc, base, 3 * WIDE, own[LAST])
            multiply(y_1, w_sc, base, 2 * WIDE, dbuf[2])
            last_refs = [k_last.at[group, pair] for pair in range(LOCAL // 2)]
            finish(y_0, b_sc, base, me, 0, ctab, stab, last_refs, v_last.at[group], q_last.at[group])
            finish(y_1, b_sc, base, peer_d, None, ctab, stab, last_refs, v_last.at[group], None)

    @pl.when(step == LAST)
    def _():
        build_tables(LAST)

    send_x(step).wait_recv()
    relay(step).start()

    @pl.when(step < ROWS - AHEAD)
    def _():
        send_x(step + AHEAD).start()

    @pl.when(step < LAST)
    def _():
        build_tables(step)
        send_d(step).wait_recv()
        multiply(y_0, w_sc, 0, 3 * WIDE, own[step])
        multiply(y_1, w_sc, 0, 3 * WIDE, dbuf[lax.rem(step, 2)])
        finish(y_0, b_sc, 0, me, core * PART, ctab, stab, kt_refs, vt, qbd)
        finish(y_1, b_sc, 0, peer_d, (1 - core) * PART, ctab, stab, kt_refs, vt, qbd)

    @pl.when(step == LAST)
    def _():
        a_last[0] = own[LAST]
        multiply(y_0, w_sc, 0, 2 * WIDE, xbuf[LAST])
        multiply(y_1, w_sc, 3 * LOCAL, 2 * WIDE, xbuf[LAST])
        for group in range(2):
            last_refs = [k_last.at[group, pair] for pair in range(LOCAL // 2)]
            finish((y_0, y_1)[group], b_sc, 3 * LOCAL * group, peer_x, None, ctab, stab, last_refs, v_last.at[group], None)

    @pl.when(step > 0)
    def _():
        swap_ctx(step - 1).wait()
        dense(step - 1)

    @pl.when(step < ROWS)
    def _():
        relay(step).wait_recv()

    @pl.when(step < LAST - 1)
    def _():
        send_d(step + 1).start()

    @pl.when(step < LAST)
    def _():
        multiply(y_0, w_sc, 0, 2 * WIDE, xbuf[step])
        multiply(y_1, w_sc, 0, 2 * WIDE, rbuf[lax.rem(step, 2)])

    def rest(r, this_chip):
        finish(y_0, b_sc, 0, peer_x, None, ctab, stab, kt_refs, vt, qbd)
        finish(y_1, b_sc, 0, peer_xd, None, ctab, stab, kt_refs, vt, qbd)
        ko_ref[r, 0:2] = kt_0[...].reshape(2, HEAD, SEQ)
        ko_ref[r, 2] = kt_1[0:HEAD]
        vo_ref[r] = vt[0:192].reshape(3, HEAD, SEQ)
        for pair in range(LOCAL // 2):
            kk[pair] = kt_refs[pair][...].T

        def store(qb, v_rows, value):
            ctx_buf[lax.rem(r, 2), qb, v_rows, :] = value

        spec = ((768, 256), (768, 256)) if this_chip == 0 else ((768, 512), (1024, 768))
        attend(spec, this_chip * CHIP, ctx_ref[r], kk, qbd, vt, s_refs, top_sc, store)

    for this_chip in range(2):
        @pl.when(jnp.logical_and(step < LAST, chip == this_chip))
        def _():
            rest(step, this_chip)

    @pl.when(step == LAST)
    def _():
        a_last[1] = rbuf[LAST % 2]

        def drain(r, c):
            send_x(r).wait_send()
            relay(r).wait_send()
            send_d(r).wait_send()
            return c

        lax.fori_loop(0, LAST, drain, 0)
        send_x(LAST).wait_send()
        relay(LAST).wait_send()
        send_d_last().wait_send()


def last_row(ctx_ref, bd_hbm, out_vm, keys_vm, values_vm, a_last, w_sc, b_sc, wd_sc, ctab, stab, k_last, v_last, q_last,
             out_hbm, keys_hbm, values_hbm,
             bd_ref, y_0, y_1, kt_0, kt_1, kt_2, vt, kk, s_0, s_2, top_sc, ctx_buf, out_row, key_row, value_row, sem, row_sem):
    me = lax.axis_index('sp')
    bulk = []
    for i, (src, dst) in enumerate(((keys_vm, keys_hbm), (values_vm, values_hbm), (out_vm, out_hbm))):
        for n in range(3):
            bulk.append(pltpu.make_async_copy(src.at[pl.ds(5 * n, 5)], dst.at[pl.ds(5 * n, 5)], sem.at[3 * i + n]))
    bd_copy = pltpu.make_async_copy(bd_hbm, bd_ref, row_sem.at[3])
    bd_copy.start()
    for c in bulk:
        c.start()
    kt_refs = (kt_0, kt_1, kt_2)
    s_refs = (s_0, None, s_2, None)
    row_copies = [pltpu.make_async_copy(src, dst.at[LAST], row_sem.at[i]) for i, (src, dst) in enumerate(((out_row, out_hbm), (key_row, keys_hbm), (value_row, values_hbm)))]
    far = 3 - me
    for group in range(2):
        multiply((y_0, y_1)[group], w_sc, 3 * LOCAL * group, 2 * WIDE, a_last[1])
    for group in range(2):
        for pair in range(LOCAL // 2):
            kt_refs[pair][...] = k_last[group, pair]
        vt[...] = v_last[group]
        finish((y_0, y_1)[group], b_sc, 3 * LOCAL * group, far, None, ctab, stab, kt_refs, vt, None)
        if group == 0:
            key_row[0:2] = kt_0[...].reshape(2, HEAD, SEQ)
            key_row[2] = kt_1[0:HEAD]
            value_row[...] = vt[0:192].reshape(3, HEAD, SEQ)
        for pair in range(LOCAL // 2):
            kk[pair] = kt_refs[pair][...].T

        def store(qb, v_rows, value):
            ctx_buf[group, v_rows, :] = value

        for live, spec in ((me < 2, (768, 256)), (me == 2, (768, 512)), (me == 3, (1024, 768))):
            @pl.when(live)
            def _():
                attend((spec,), me * PART, ctx_ref[LAST], kk, q_last.at[group], vt, s_refs, top_sc, store)

        if group == 0:
            row_copies[1].start()
            row_copies[2].start()
    bd_copy.wait()
    out_row[...] = project_out(ctx_buf[...].reshape(HID, PART), wd_sc[...], a_last[0], bd_ref)
    row_copies[0].start()
    for c in bulk + row_copies:
        c.wait()


def solution(mesh):
    seq_spec = P('dp', 'sp', None)
    row_spec = P('dp', 'sp')
    head_spec = P('dp', None, 'sp', None)
    replicated = P()
    tcos, tsin = rope_tables()

    def local_block(hidden, pos_ids, block_ids, ctx_len, ln_gamma, ln_beta, w_qkv, b_qkv, w_dense, b_dense):
        w_t = jnp.transpose(w_qkv, (1, 2, 3, 0))
        anywhere = pl.BlockSpec(memory_space=pltpu.HBM)

        held = pl.pallas_call(
            kernel,
            grid=(ROWS,),
            out_shape=(
                pltpu.VMEM((ROWS, PART, HID), BF16),
                pltpu.VMEM((ROWS, 3, HEAD, SEQ), BF16),
                pltpu.VMEM((ROWS, 3, HEAD, SEQ), BF16),
                pltpu.VMEM((2, PART, HID), BF16),
                pltpu.VMEM((36, HEAD, HID), BF16),
                pltpu.VMEM((36, HEAD, 128), F32),
                pltpu.VMEM((HID, HID), BF16),
                pltpu.VMEM((32, SEQ), F32),
                pltpu.VMEM((32, SEQ), F32),
                pltpu.VMEM((2, LOCAL // 2, 2 * HEAD, SEQ), BF16),
                pltpu.VMEM((2, WIDE, SEQ), BF16),
                pltpu.VMEM((2, LOCAL // 2, 2 * HEAD, 2 * PART), BF16),
            ),
            in_specs=[anywhere, anywhere, pl.BlockSpec(memory_space=pltpu.SMEM)] + [anywhere] * 8,
            out_specs=(pl.BlockSpec(memory_space=pltpu.VMEM),) * 12,
            scratch_shapes=[
                pltpu.VMEM((ROWS, PART), jnp.int32),
                pltpu.VMEM((HID,), BF16),
                pltpu.VMEM((HID,), BF16),
                pltpu.VMEM((HID,), BF16),
                pltpu.VMEM((12, 3, HEAD), BF16),
                pltpu.VMEM((16, SEQ), F32),
                pltpu.VMEM((16, SEQ), F32),
                pltpu.VMEM((ROWS, PART, HID), BF16),
                pltpu.VMEM((ROWS, PART, HID), BF16),
                pltpu.VMEM((3, PART, HID), BF16),
                pltpu.VMEM((2, PART, HID), BF16),
                pltpu.VMEM((4, ROWS, 128), jnp.int32),
                pltpu.VMEM((3 * WIDE, PART), F32),
                pltpu.VMEM((3 * WIDE, PART), F32),
                *[pltpu.VMEM((2 * HEAD, SEQ), BF16)] * 3,
                pltpu.VMEM((WIDE, SEQ), BF16),
                pltpu.VMEM((3, SEQ, 128), BF16),
                pltpu.VMEM((3, 128, 2 * CHIP), BF16),
                *[pltpu.VMEM((SEQ, PART), F32)] * 4,
                pltpu.VMEM((4, 8, PART), F32),
                pltpu.VMEM((2, 2, WIDE, PART), BF16),
                pltpu.VMEM((2, WIDE, PART), BF16),
                pltpu.SemaphoreType.DMA((7,)),
                pltpu.SemaphoreType.DMA((ROWS,)),
                pltpu.SemaphoreType.DMA((16,)),
            ] + [pltpu.SemaphoreType.DMA((ROWS,))] * 8 + [pltpu.SemaphoreType.DMA((3,))] * 2,
            compiler_params=pltpu.CompilerParams(
                collective_id=0, has_side_effects=True, vmem_limit_bytes=32 * 1024 * 1024, dimension_semantics=('arbitrary',)),
            name='glm_block',
        )(hidden, pos_ids, ctx_len, ln_gamma, ln_beta, b_dense,
          w_t, b_qkv, w_dense, jnp.asarray(tcos), jnp.asarray(tsin))
        held = [pltpu.with_memory_space_constraint(x, pltpu.VMEM) for x in held]
        out, keys_t, values_t = pl.pallas_call(
            last_row,
            out_shape=[jax.ShapeDtypeStruct(x.shape, BF16) for x in held[:3]],
            in_specs=[pl.BlockSpec(memory_space=pltpu.SMEM), anywhere] + [pl.BlockSpec(memory_space=pl.ANY)] * 3 + [pl.BlockSpec(memory_space=pltpu.VMEM)] * 9,
            out_specs=[anywhere] * 3,
            scratch_shapes=[
                pltpu.VMEM((HID,), BF16),
                *[pltpu.VMEM((2 * WIDE, PART), F32)] * 2,
                *[pltpu.VMEM((2 * HEAD, SEQ), BF16)] * 3,
                pltpu.VMEM((WIDE, SEQ), BF16),
                pltpu.VMEM((3, SEQ, 128), BF16),
                *[pltpu.VMEM((SEQ, PART), F32)] * 2,
                pltpu.VMEM((4, 8, PART), F32),
                pltpu.VMEM((2, WIDE, PART), BF16),
                pltpu.VMEM((PART, HID), BF16),
                pltpu.VMEM((3, HEAD, SEQ), BF16),
                pltpu.VMEM((3, HEAD, SEQ), BF16),
                pltpu.SemaphoreType.DMA((9,)),
                pltpu.SemaphoreType.DMA((4,)),
            ],
            compiler_params=pltpu.CompilerParams(vmem_limit_bytes=32 * 1024 * 1024),
            name='last_row',
        )(ctx_len, b_dense, *held)
        return out, jnp.transpose(keys_t, (0, 3, 1, 2)), jnp.transpose(values_t, (0, 3, 1, 2))

    return jax.shard_map(local_block, mesh=mesh, in_specs=(seq_spec, row_spec, row_spec, P('dp'), replicated, replicated, replicated, replicated, replicated, replicated), out_specs=(seq_spec, head_spec, head_spec), check_vma=False)
```

```python
import functools
import math

import jax
import jax.numpy as jnp
import numpy as np
from jax import lax
from jax.experimental import pallas as pl
from jax.experimental.pallas import tpu as pltpu
from jax.sharding import PartitionSpec as P

ALPHA = math.sqrt(56.0)
ROPE_BASE = 10000.0
LN_EPS = 1e-5
MESH = pl.DeviceIdType.MESH
F32 = jnp.float32
BF16 = jnp.bfloat16

ROWS = 16
PART = 256
AHEAD = 15
SEQ = 1024
LAST = ROWS - 1
HID = 768
HEAD = 64
CHIP = 512
LOCAL = 6
WIDE = LOCAL * HEAD
EXP_SCALE = math.log2(math.e) / math.sqrt(HEAD)
CHUNK = 64
MIX = 256


def rope_tables():
    freq = ROPE_BASE ** (-np.arange(0, 32, 2).astype(np.float64) / 32.0)
    angle = freq.astype(np.float32)[:, None] * np.arange(SEQ, dtype=np.float32)[None, :]
    return np.cos(angle.astype(np.float64)).astype(np.float32), np.sin(angle.astype(np.float64)).astype(np.float32)


def nt_dot(a, b):
    return lax.dot_general(a, b, (((1,), (1,)), ((), ())), preferred_element_type=F32)


def multiply(y_ref, w_ref, base, rows, tokens):
    y_ref[0:rows] = nt_dot(w_ref[base:base + rows // HEAD].reshape(rows, HID), tokens)


def finish(y_ref, b_ref, base, part, q_col, ctab, stab, kt_refs, vt, qbd):
    for h in range(LOCAL):
        for lt in range(PART // 128):
            cols = pl.ds(pl.multiple_of(part * PART + lt * 128, 128), 128)
            ycols = slice(lt * 128, lt * 128 + 128)
            for half in range(2):
                cos = ctab[16 * half:16 * half + 16, cols]
                sin = stab[16 * half:16 * half + 16, cols]

                def rotated(kind):
                    u0 = kind * WIDE + h * HEAD + half * 32
                    b0 = half * 32
                    bias = b_ref.at[base + kind * LOCAL + h]
                    u = (y_ref[u0:u0 + 16, ycols] + bias[b0:b0 + 16]).astype(BF16).astype(F32)
                    w = (y_ref[u0 + 16:u0 + 32, ycols] + bias[b0 + 16:b0 + 32]).astype(BF16).astype(F32)
                    return (u * cos - w * sin).astype(BF16), (w * cos + u * sin).astype(BF16)

                k0 = (h % 2) * HEAD + half * 32
                ku, kw = rotated(0)
                kt_refs[h // 2][k0:k0 + 16, cols] = ku
                kt_refs[h // 2][k0 + 16:k0 + 32, cols] = kw
                if q_col is not None:
                    qu, qw = rotated(2)
                    q_width = qbd.shape[2] // 2
                    qc = pl.ds(pl.multiple_of((h % 2) * q_width + q_col + lt * 128, 128), 128)
                    qbd[h // 2, k0:k0 + 16, qc] = qu
                    qbd[h // 2, k0 + 16:k0 + 32, qc] = qw
            v0 = WIDE + h * HEAD
            vt[h * HEAD:(h + 1) * HEAD, cols] = (y_ref[v0:v0 + HEAD, ycols] + b_ref[base + LOCAL + h]).astype(BF16)


def attend(spec, q_first, ctx, kk, qbd, vt, s_refs, top_sc, store):
    def score(pair, j):
        for qb, (key_len, mask_from) in enumerate(spec):
            q0 = (j * len(spec) + qb) * PART
            scores = jnp.dot(kk[pair, 0:key_len, :], qbd[pair, :, q0:q0 + PART], preferred_element_type=F32)
            q_pos = q_first + qb * PART + lax.broadcasted_iota(jnp.int32, (1, PART), 1)
            limit = jnp.maximum(q_pos, ctx - 1)
            top = None
            for k0 in range(0, key_len, CHUNK):
                part = scores[k0:k0 + CHUNK]
                if k0 >= mask_from:
                    k_pos = k0 + lax.broadcasted_iota(jnp.int32, (CHUNK, PART), 0)
                    part = jnp.where(k_pos <= limit, part, -jnp.inf)
                s_refs[2 * j + qb][k0:k0 + CHUNK] = part
                peak = jnp.max(part.reshape(CHUNK // 8, 8, PART), axis=0)
                top = peak if top is None else jnp.maximum(top, peak)
            top_sc[2 * j + qb] = jnp.broadcast_to(jnp.max(top, axis=0, keepdims=True) * EXP_SCALE, (8, PART))

    def mix(pair, j):
        v_rows = pl.ds(pl.multiple_of((2 * pair + j) * HEAD, HEAD), HEAD)
        for qb, (key_len, _) in enumerate(spec):
            top = top_sc[2 * j + qb, 0:1]
            total = jnp.zeros((8, PART), F32)
            mixed = None
            for k0 in range(0, key_len, MIX):
                probs = []
                for k1 in range(k0, k0 + MIX, CHUNK):
                    prob = jnp.exp2(s_refs[2 * j + qb][k1:k1 + CHUNK] * EXP_SCALE - top)
                    total = total + jnp.sum(prob.reshape(CHUNK // 8, 8, PART), axis=0)
                    probs.append(prob.astype(BF16))
                some = jnp.dot(vt[v_rows, k0:k0 + MIX], jnp.concatenate(probs, axis=0), preferred_element_type=F32)
                mixed = some if mixed is None else mixed + some
            store(qb, v_rows, (mixed * (1.0 / jnp.sum(total, axis=0, keepdims=True))).astype(BF16))

    score(0, 0)

    def one_pair(pair, c):
        score(pair, 1)
        mix(pair, 0)
        score(pair + 1, 0)
        mix(pair, 1)
        return c

    lax.fori_loop(0, LOCAL // 2 - 1, one_pair, 0)
    score(LOCAL // 2 - 1, 1)
    mix(LOCAL // 2 - 1, 0)
    mix(LOCAL // 2 - 1, 1)


def project_out(mixed, wd, normed, bd_ref):
    dense_out = lax.dot_general(mixed, wd, (((0,), (0,)), ((), ())), preferred_element_type=F32)
    return (normed.astype(F32) * ALPHA + dense_out + bd_ref[...].astype(F32).reshape(1, HID)).astype(BF16)


def kernel(hid_hbm, pos_hbm, ctx_ref, gamma_hbm, beta_hbm, bd_hbm, w_hbm, bias_hbm, wd_hbm, tcos_hbm, tsin_hbm,
           out_ref, ko_ref, vo_ref, a_last, w_sc, b_sc, wd_sc, ctab, stab, k_last, v_last, q_last,
           pos_ref, gamma_ref, beta_ref, bd_ref, bias_ref, tcos_ref, tsin_ref, own, xbuf, dbuf, rbuf, posr, y_0, y_1, kt_0, kt_1, kt_2, vt, kk, qbd, s_0, s_1, s_2, s_3, top_sc, ctx_buf, ctx_recv,
           t_sem, hid_sem, w_sem, xs_sem, xr_sem, ds_sem, dr_sem, rs_sem, rr_sem, cs_sem, cr_sem, ps_sem, pr_sem):
    step = pl.program_id(0)
    s_refs, kt_refs = (s_0, s_1, s_2, s_3), (kt_0, kt_1, kt_2)
    me = lax.axis_index('sp')
    core = lax.rem(me, 2)
    chip = me // 2
    other = 1 - chip
    peer_x = other * 2 + core
    peer_d = chip * 2 + 1 - core
    peer_xd = other * 2 + 1 - core

    def remote(src, dst, send_sem, recv_sem, peer):
        return pltpu.make_async_remote_copy(src, dst, send_sem, recv_sem, device_id={'sp': peer}, device_id_type=MESH)

    def send_x(r):
        return remote(own.at[r], xbuf.at[r], xs_sem.at[r], xr_sem.at[r], peer_x)

    def send_d(r):
        return remote(own.at[r], dbuf.at[lax.rem(r, 2)], ds_sem.at[r], dr_sem.at[r], peer_d)

    def relay(r):
        return remote(xbuf.at[r], rbuf.at[lax.rem(r, 2)], rs_sem.at[r], rr_sem.at[r], peer_d)

    def swap_ctx(r):
        return remote(ctx_buf.at[lax.rem(r, 2), 1 - core], ctx_recv.at[lax.rem(r, 2)], cs_sem.at[r], cr_sem.at[r], peer_d)

    def swap_pos(n, peer):
        return remote(pos_ref.at[:, pl.ds(128, 128)], posr.at[me], ps_sem.at[n], pr_sem.at[n], peer)

    def recv_pos(n, peer):
        return remote(pos_ref.at[:, pl.ds(128, 128)], posr.at[peer], ps_sem.at[n], pr_sem.at[n], peer)

    def load_hidden(r):
        return pltpu.make_async_copy(hid_hbm.at[r], own.at[r], hid_sem.at[r])

    def small_copies():
        pairs = ((gamma_hbm, gamma_ref), (beta_hbm, beta_ref), (pos_hbm, pos_ref), (bd_hbm, bd_ref), (bias_hbm, bias_ref), (tcos_hbm, tcos_ref), (tsin_hbm, tsin_ref))
        return [pltpu.make_async_copy(src, dst, t_sem.at[i]) for i, (src, dst) in enumerate(pairs)]

    def weight_copies():
        copies = []
        for group, owner in enumerate((me, peer_x, peer_d, peer_xd)):
            for slot, kind in ((0, 1), (6, 2), (12, 0)):
                copies.append((w_hbm.at[pl.ds(owner * 3, 3), kind], w_sc.at[pl.ds(18 * (group // 2) + slot + 3 * (group % 2), 3)]))
        for slot, owner in enumerate((me, peer_x, peer_d, peer_xd)):
            copies.append((wd_hbm.at[pl.ds(pl.multiple_of(owner * 192, 64), 192)], wd_sc.at[pl.ds(slot * 192, 192)]))
        return [pltpu.make_async_copy(src, dst, w_sem.at[i]) for i, (src, dst) in enumerate(copies)]

    def norm_row(r):
        gamma = gamma_ref[...].astype(F32).reshape(1, HID)
        beta = beta_ref[...].astype(F32).reshape(1, HID)
        for t in range(0, PART, 32):
            rows = pl.ds(t, 32)
            wide = own[r, rows, :].astype(F32)
            mean = jnp.sum(wide, axis=-1, keepdims=True) * (1.0 / HID)
            cent = wide - mean
            var = jnp.sum(cent * cent, axis=-1, keepdims=True) * (1.0 / HID)
            own[r, rows, :] = (cent * lax.rsqrt(var + LN_EPS) * gamma + beta).astype(BF16)

    def spread_bias():
        for group, owner in enumerate((me, peer_x, peer_d, peer_xd)):
            for slot, kind in ((0, 1), (6, 2), (12, 0)):
                for h in range(3):
                    row = bias_ref[owner * 3 + h, kind:kind + 1, :].astype(F32)
                    b_sc[18 * (group // 2) + slot + 3 * (group % 2) + h] = jnp.broadcast_to(row, (128, HEAD)).T

    @pl.when(step == 0)
    def _():
        small = small_copies()
        for c in small[:2]:
            c.start()

        def fetch(r, c):
            load_hidden(r).start()
            return c

        lax.fori_loop(0, ROWS, fetch, 0)
        barrier = pltpu.get_barrier_semaphore()
        for peer in (peer_x, peer_d, peer_xd):
            pl.semaphore_signal(barrier, inc=1, device_id={'sp': peer}, device_id_type=MESH)
        for c in small[2:] + weight_copies():
            c.start()
        for c in small[:2]:
            c.wait()
        load_hidden(0).wait()
        norm_row(0)
        pl.semaphore_wait(barrier, 3)
        load_hidden(1).wait()
        norm_row(1)
        send_x(0).start()

        def norm_and_send(r, c):
            load_hidden(r).wait()
            norm_row(r)

            @pl.when(r <= AHEAD)
            def _():
                send_x(r - 1).start()

            return c

        lax.fori_loop(2, ROWS, norm_and_send, 0)
        for c in small[2:]:
            c.wait()
        for n, peer in enumerate((peer_x, peer_d, peer_xd)):
            swap_pos(n, peer).start()
        send_d(0).start()
        posr[me] = pos_ref[:, 128:256]
        qbd[...] = jnp.zeros_like(qbd)
        spread_bias()
        for c in weight_copies():
            c.wait()
        for n, peer in enumerate((peer_x, peer_d, peer_xd)):
            recv_pos(n, peer).wait()

    def build_tables(r):
        tcos = tcos_ref[...]
        tsin = tsin_ref[...]
        lane = lax.broadcasted_iota(jnp.int32, (16, SEQ), 1)
        ctx = ctx_ref[r]
        last = posr[3, pl.ds(r, 1), :]
        last_lane = lax.broadcasted_iota(jnp.int32, (1, 128), 1)
        m_pos = jnp.sum(jnp.where(last_lane == 127, last, 0), axis=1, keepdims=True)

        def pick(table, hit):
            return jnp.sum(jnp.where(hit, table, 0.0), axis=1, keepdims=True)

        at_m = lane == m_pos
        at_c = lane == ctx - 1
        in_ctx = lane < ctx
        cos_c, sin_c = pick(tcos, at_c), pick(tsin, at_c)
        ctab[0:16] = jnp.where(in_ctx, tcos, pick(tcos, at_m))
        stab[0:16] = jnp.where(in_ctx, tsin, pick(tsin, at_m))
        ctab[16:32] = jnp.where(in_ctx, 1.0, tcos * cos_c + tsin * sin_c)
        stab[16:32] = jnp.where(in_ctx, 0.0, tsin * cos_c - tcos * sin_c)

    def dense(r):
        mixed = jnp.concatenate([ctx_buf[lax.rem(r, 2), core], ctx_recv[lax.rem(r, 2)]], axis=0)
        out_ref[r] = project_out(mixed, wd_sc[...], own[r], bd_ref)

    @pl.when(step > 0)
    def _():
        swap_ctx(step - 1).start()

    @pl.when(step == LAST)
    def _():
        build_tables(step)
        send_d(step).wait_recv()
        q_last[...] = jnp.zeros_like(q_last)
        for group in range(2):
            base = 3 * LOCAL * group
            multiply(y_0, w_sc, base, 3 * WIDE, own[LAST])
            multiply(y_1, w_sc, base, 2 * WIDE, dbuf[LAST % 2])
            last_refs = [k_last.at[group, pair] for pair in range(LOCAL // 2)]
            finish(y_0, b_sc, base, me, 0, ctab, stab, last_refs, v_last.at[group], q_last.at[group])
            finish(y_1, b_sc, base, peer_d, None, ctab, stab, last_refs, v_last.at[group], None)

    send_x(step).wait_recv()
    relay(step).start()

    @pl.when(step < ROWS - AHEAD)
    def _():
        send_x(step + AHEAD).start()

    @pl.when(step < LAST)
    def _():
        build_tables(step)
        send_d(step).wait_recv()
        multiply(y_0, w_sc, 0, 3 * WIDE, own[step])
        multiply(y_1, w_sc, 0, 3 * WIDE, dbuf[lax.rem(step, 2)])
        finish(y_0, b_sc, 0, me, core * PART, ctab, stab, kt_refs, vt, qbd)
        finish(y_1, b_sc, 0, peer_d, (1 - core) * PART, ctab, stab, kt_refs, vt, qbd)

    @pl.when(step == LAST)
    def _():
        a_last[0] = own[LAST]
        multiply(y_0, w_sc, 0, 2 * WIDE, xbuf[LAST])
        multiply(y_1, w_sc, 3 * LOCAL, 2 * WIDE, xbuf[LAST])
        for group in range(2):
            last_refs = [k_last.at[group, pair] for pair in range(LOCAL // 2)]
            finish((y_0, y_1)[group], b_sc, 3 * LOCAL * group, peer_x, None, ctab, stab, last_refs, v_last.at[group], None)

    @pl.when(step > 0)
    def _():
        swap_ctx(step - 1).wait()
        dense(step - 1)

    @pl.when(step < ROWS)
    def _():
        relay(step).wait_recv()

    @pl.when(step < ROWS - 1)
    def _():
        send_d(step + 1).start()

    @pl.when(step < LAST)
    def _():
        multiply(y_0, w_sc, 0, 2 * WIDE, xbuf[step])
        multiply(y_1, w_sc, 0, 2 * WIDE, rbuf[lax.rem(step, 2)])

    def rest(r, this_chip):
        finish(y_0, b_sc, 0, peer_x, None, ctab, stab, kt_refs, vt, qbd)
        finish(y_1, b_sc, 0, peer_xd, None, ctab, stab, kt_refs, vt, qbd)
        ko_ref[r, 0:2] = kt_0[...].reshape(2, HEAD, SEQ)
        ko_ref[r, 2] = kt_1[0:HEAD]
        vo_ref[r] = vt[0:192].reshape(3, HEAD, SEQ)
        for pair in range(LOCAL // 2):
            kk[pair] = kt_refs[pair][...].T

        def store(qb, v_rows, value):
            ctx_buf[lax.rem(r, 2), qb, v_rows, :] = value

        spec = ((768, 256), (768, 256)) if this_chip == 0 else ((768, 512), (1024, 768))
        attend(spec, this_chip * CHIP, ctx_ref[r], kk, qbd, vt, s_refs, top_sc, store)

    for this_chip in range(2):
        @pl.when(jnp.logical_and(step < LAST, chip == this_chip))
        def _():
            rest(step, this_chip)

    @pl.when(step == LAST)
    def _():
        a_last[1] = rbuf[LAST % 2]

        def drain(r, c):
            send_x(r).wait_send()
            relay(r).wait_send()
            send_d(r).wait_send()
            return c

        lax.fori_loop(0, ROWS, drain, 0)


def last_row(ctx_ref, bd_hbm, out_vm, keys_vm, values_vm, a_last, w_sc, b_sc, wd_sc, ctab, stab, k_last, v_last, q_last,
             out_hbm, keys_hbm, values_hbm,
             bd_ref, y_0, y_1, kt_0, kt_1, kt_2, vt, kk, s_0, s_2, top_sc, ctx_buf, out_row, key_row, value_row, sem, row_sem):
    me = lax.axis_index('sp')
    bulk = []
    for i, (src, dst) in enumerate(((keys_vm, keys_hbm), (values_vm, values_hbm), (out_vm, out_hbm))):
        for n in range(3):
            bulk.append(pltpu.make_async_copy(src.at[pl.ds(5 * n, 5)], dst.at[pl.ds(5 * n, 5)], sem.at[3 * i + n]))
    bd_copy = pltpu.make_async_copy(bd_hbm, bd_ref, row_sem.at[3])
    bd_copy.start()
    for c in bulk:
        c.start()
    kt_refs = (kt_0, kt_1, kt_2)
    s_refs = (s_0, None, s_2, None)
    row_copies = [pltpu.make_async_copy(src, dst.at[LAST], row_sem.at[i]) for i, (src, dst) in enumerate(((out_row, out_hbm), (key_row, keys_hbm), (value_row, values_hbm)))]
    far = 3 - me
    for group in range(2):
        multiply((y_0, y_1)[group], w_sc, 3 * LOCAL * group, 2 * WIDE, a_last[1])
    for group in range(2):
        for pair in range(LOCAL // 2):
            kt_refs[pair][...] = k_last[group, pair]
        vt[...] = v_last[group]
        finish((y_0, y_1)[group], b_sc, 3 * LOCAL * group, far, None, ctab, stab, kt_refs, vt, None)
        if group == 0:
            key_row[0:2] = kt_0[...].reshape(2, HEAD, SEQ)
            key_row[2] = kt_1[0:HEAD]
            value_row[...] = vt[0:192].reshape(3, HEAD, SEQ)
        for pair in range(LOCAL // 2):
            kk[pair] = kt_refs[pair][...].T

        def store(qb, v_rows, value):
            ctx_buf[group, v_rows, :] = value

        for live, spec in ((me < 2, (768, 256)), (me == 2, (768, 512)), (me == 3, (1024, 768))):
            @pl.when(live)
            def _():
                attend((spec,), me * PART, ctx_ref[LAST], kk, q_last.at[group], vt, s_refs, top_sc, store)

        if group == 0:
            row_copies[1].start()
            row_copies[2].start()
    bd_copy.wait()
    out_row[...] = project_out(ctx_buf[...].reshape(HID, PART), wd_sc[...], a_last[0], bd_ref)
    row_copies[0].start()
    for c in bulk + row_copies:
        c.wait()


def solution(mesh):
    seq_spec = P('dp', 'sp', None)
    row_spec = P('dp', 'sp')
    head_spec = P('dp', None, 'sp', None)
    replicated = P()
    tcos, tsin = rope_tables()

    def local_block(hidden, pos_ids, block_ids, ctx_len, ln_gamma, ln_beta, w_qkv, b_qkv, w_dense, b_dense):
        w_t = jnp.transpose(w_qkv, (1, 2, 3, 0))
        anywhere = pl.BlockSpec(memory_space=pltpu.HBM)

        held = pl.pallas_call(
            kernel,
            grid=(ROWS,),
            out_shape=(
                pltpu.VMEM((ROWS, PART, HID), BF16),
                pltpu.VMEM((ROWS, 3, HEAD, SEQ), BF16),
                pltpu.VMEM((ROWS, 3, HEAD, SEQ), BF16),
                pltpu.VMEM((2, PART, HID), BF16),
                pltpu.VMEM((36, HEAD, HID), BF16),
                pltpu.VMEM((36, HEAD, 128), F32),
                pltpu.VMEM((HID, HID), BF16),
                pltpu.VMEM((32, SEQ), F32),
                pltpu.VMEM((32, SEQ), F32),
                pltpu.VMEM((2, LOCAL // 2, 2 * HEAD, SEQ), BF16),
                pltpu.VMEM((2, WIDE, SEQ), BF16),
                pltpu.VMEM((2, LOCAL // 2, 2 * HEAD, 2 * PART), BF16),
            ),
            in_specs=[anywhere, anywhere, pl.BlockSpec(memory_space=pltpu.SMEM)] + [anywhere] * 8,
            out_specs=(pl.BlockSpec(memory_space=pltpu.VMEM),) * 12,
            scratch_shapes=[
                pltpu.VMEM((ROWS, PART), jnp.int32),
                pltpu.VMEM((HID,), BF16),
                pltpu.VMEM((HID,), BF16),
                pltpu.VMEM((HID,), BF16),
                pltpu.VMEM((12, 3, HEAD), BF16),
                pltpu.VMEM((16, SEQ), F32),
                pltpu.VMEM((16, SEQ), F32),
                pltpu.VMEM((ROWS, PART, HID), BF16),
                pltpu.VMEM((ROWS, PART, HID), BF16),
                pltpu.VMEM((2, PART, HID), BF16),
                pltpu.VMEM((2, PART, HID), BF16),
                pltpu.VMEM((4, ROWS, 128), jnp.int32),
                pltpu.VMEM((3 * WIDE, PART), F32),
                pltpu.VMEM((3 * WIDE, PART), F32),
                *[pltpu.VMEM((2 * HEAD, SEQ), BF16)] * 3,
                pltpu.VMEM((WIDE, SEQ), BF16),
                pltpu.VMEM((3, SEQ, 128), BF16),
                pltpu.VMEM((3, 128, 2 * CHIP), BF16),
                *[pltpu.VMEM((SEQ, PART), F32)] * 4,
                pltpu.VMEM((4, 8, PART), F32),
                pltpu.VMEM((2, 2, WIDE, PART), BF16),
                pltpu.VMEM((2, WIDE, PART), BF16),
                pltpu.SemaphoreType.DMA((7,)),
                pltpu.SemaphoreType.DMA((ROWS,)),
                pltpu.SemaphoreType.DMA((16,)),
            ] + [pltpu.SemaphoreType.DMA((ROWS,))] * 8 + [pltpu.SemaphoreType.DMA((3,))] * 2,
            compiler_params=pltpu.CompilerParams(
                collective_id=0, has_side_effects=True, vmem_limit_bytes=32 * 1024 * 1024, dimension_semantics=('arbitrary',)),
            name='glm_block',
        )(hidden, pos_ids, ctx_len, ln_gamma, ln_beta, b_dense,
          w_t, b_qkv, w_dense, jnp.asarray(tcos), jnp.asarray(tsin))
        held = [pltpu.with_memory_space_constraint(x, pltpu.VMEM) for x in held]
        out, keys_t, values_t = pl.pallas_call(
            last_row,
            out_shape=[jax.ShapeDtypeStruct(x.shape, BF16) for x in held[:3]],
            in_specs=[pl.BlockSpec(memory_space=pltpu.SMEM), anywhere] + [pl.BlockSpec(memory_space=pl.ANY)] * 3 + [pl.BlockSpec(memory_space=pltpu.VMEM)] * 9,
            out_specs=[anywhere] * 3,
            scratch_shapes=[
                pltpu.VMEM((HID,), BF16),
                *[pltpu.VMEM((2 * WIDE, PART), F32)] * 2,
                *[pltpu.VMEM((2 * HEAD, SEQ), BF16)] * 3,
                pltpu.VMEM((WIDE, SEQ), BF16),
                pltpu.VMEM((3, SEQ, 128), BF16),
                *[pltpu.VMEM((SEQ, PART), F32)] * 2,
                pltpu.VMEM((4, 8, PART), F32),
                pltpu.VMEM((2, WIDE, PART), BF16),
                pltpu.VMEM((PART, HID), BF16),
                pltpu.VMEM((3, HEAD, SEQ), BF16),
                pltpu.VMEM((3, HEAD, SEQ), BF16),
                pltpu.SemaphoreType.DMA((9,)),
                pltpu.SemaphoreType.DMA((4,)),
            ],
            compiler_params=pltpu.CompilerParams(vmem_limit_bytes=32 * 1024 * 1024),
            name='last_row',
        )(ctx_len, b_dense, *held)
        return out, jnp.transpose(keys_t, (0, 3, 1, 2)), jnp.transpose(values_t, (0, 3, 1, 2))

    return jax.shard_map(local_block, mesh=mesh, in_specs=(seq_spec, row_spec, row_spec, P('dp'), replicated, replicated, replicated, replicated, replicated, replicated), out_specs=(seq_spec, head_spec, head_spec), check_vma=False)
```

```python
import functools
import math

import jax
import jax.numpy as jnp
import numpy as np
from jax import lax
from jax.experimental import pallas as pl
from jax.experimental.pallas import tpu as pltpu
from jax.sharding import PartitionSpec as P

ALPHA = math.sqrt(56.0)
ROPE_BASE = 10000.0
LN_EPS = 1e-5
MESH = pl.DeviceIdType.MESH
F32 = jnp.float32
BF16 = jnp.bfloat16

ROWS = 16
PART = 256
AHEAD = 2
SEQ = 1024
LAST = ROWS - 1
HID = 768
HEAD = 64
CHIP = 512
LOCAL = 6
WIDE = LOCAL * HEAD
EXP_SCALE = math.log2(math.e) / math.sqrt(HEAD)
CHUNK = 64
MIX = 256


def rope_tables():
    freq = ROPE_BASE ** (-np.arange(0, 32, 2).astype(np.float64) / 32.0)
    angle = freq.astype(np.float32)[:, None] * np.arange(SEQ, dtype=np.float32)[None, :]
    return np.cos(angle.astype(np.float64)).astype(np.float32), np.sin(angle.astype(np.float64)).astype(np.float32)


def nt_dot(a, b):
    return lax.dot_general(a, b, (((1,), (1,)), ((), ())), preferred_element_type=F32)


def multiply(y_ref, w_ref, base, rows, tokens):
    y_ref[0:rows] = nt_dot(w_ref[base:base + rows // HEAD].reshape(rows, HID), tokens)


def finish(y_ref, b_ref, base, part, q_col, ctab, stab, kt_refs, vt, qbd):
    for h in range(LOCAL):
        for lt in range(PART // 128):
            cols = pl.ds(pl.multiple_of(part * PART + lt * 128, 128), 128)
            ycols = slice(lt * 128, lt * 128 + 128)
            for half in range(2):
                cos = ctab[16 * half:16 * half + 16, cols]
                sin = stab[16 * half:16 * half + 16, cols]

                def rotated(kind):
                    u0 = kind * WIDE + h * HEAD + half * 32
                    b0 = half * 32
                    bias = b_ref.at[base + kind * LOCAL + h]
                    u = (y_ref[u0:u0 + 16, ycols] + bias[b0:b0 + 16]).astype(BF16).astype(F32)
                    w = (y_ref[u0 + 16:u0 + 32, ycols] + bias[b0 + 16:b0 + 32]).astype(BF16).astype(F32)
                    return (u * cos - w * sin).astype(BF16), (w * cos + u * sin).astype(BF16)

                k0 = (h % 2) * HEAD + half * 32
                ku, kw = rotated(0)
                kt_refs[h // 2][k0:k0 + 16, cols] = ku
                kt_refs[h // 2][k0 + 16:k0 + 32, cols] = kw
                if q_col is not None:
                    qu, qw = rotated(2)
                    q_width = qbd.shape[2] // 2
                    qc = pl.ds(pl.multiple_of((h % 2) * q_width + q_col + lt * 128, 128), 128)
                    qbd[h // 2, k0:k0 + 16, qc] = qu
                    qbd[h // 2, k0 + 16:k0 + 32, qc] = qw
            v0 = WIDE + h * HEAD
            vt[h * HEAD:(h + 1) * HEAD, cols] = (y_ref[v0:v0 + HEAD, ycols] + b_ref[base + LOCAL + h]).astype(BF16)


def attend(spec, q_first, ctx, kk, qbd, vt, s_refs, top_sc, store):
    def score(pair, j):
        for qb, (key_len, mask_from) in enumerate(spec):
            q0 = (j * len(spec) + qb) * PART
            scores = jnp.dot(kk[pair, 0:key_len, :], qbd[pair, :, q0:q0 + PART], preferred_element_type=F32)
            q_pos = q_first + qb * PART + lax.broadcasted_iota(jnp.int32, (1, PART), 1)
            limit = jnp.maximum(q_pos, ctx - 1)
            top = None
            for k0 in range(0, key_len, CHUNK):
                part = scores[k0:k0 + CHUNK]
                if k0 >= mask_from:
                    k_pos = k0 + lax.broadcasted_iota(jnp.int32, (CHUNK, PART), 0)
                    part = jnp.where(k_pos <= limit, part, -jnp.inf)
                s_refs[2 * j + qb][k0:k0 + CHUNK] = part
                peak = jnp.max(part.reshape(CHUNK // 8, 8, PART), axis=0)
                top = peak if top is None else jnp.maximum(top, peak)
            top_sc[2 * j + qb] = jnp.broadcast_to(jnp.max(top, axis=0, keepdims=True) * EXP_SCALE, (8, PART))

    def mix(pair, j):
        v_rows = pl.ds(pl.multiple_of((2 * pair + j) * HEAD, HEAD), HEAD)
        for qb, (key_len, _) in enumerate(spec):
            top = top_sc[2 * j + qb, 0:1]
            total = jnp.zeros((8, PART), F32)
            mixed = None
            for k0 in range(0, key_len, MIX):
                probs = []
                for k1 in range(k0, k0 + MIX, CHUNK):
                    prob = jnp.exp2(s_refs[2 * j + qb][k1:k1 + CHUNK] * EXP_SCALE - top)
                    total = total + jnp.sum(prob.reshape(CHUNK // 8, 8, PART), axis=0)
                    probs.append(prob.astype(BF16))
                some = jnp.dot(vt[v_rows, k0:k0 + MIX], jnp.concatenate(probs, axis=0), preferred_element_type=F32)
                mixed = some if mixed is None else mixed + some
            store(qb, v_rows, (mixed * (1.0 / jnp.sum(total, axis=0, keepdims=True))).astype(BF16))

    score(0, 0)

    def one_pair(pair, c):
        score(pair, 1)
        mix(pair, 0)
        score(pair + 1, 0)
        mix(pair, 1)
        return c

    lax.fori_loop(0, LOCAL // 2 - 1, one_pair, 0)
    score(LOCAL // 2 - 1, 1)
    mix(LOCAL // 2 - 1, 0)
    mix(LOCAL // 2 - 1, 1)


def project_out(mixed, wd, normed, bd_ref):
    dense_out = lax.dot_general(mixed, wd, (((0,), (0,)), ((), ())), preferred_element_type=F32)
    return (normed.astype(F32) * ALPHA + dense_out + bd_ref[...].astype(F32).reshape(1, HID)).astype(BF16)


def kernel(hid_hbm, pos_hbm, ctx_ref, gamma_hbm, beta_hbm, bd_hbm, w_hbm, bias_hbm, wd_hbm, tcos_hbm, tsin_hbm,
           out_ref, ko_ref, vo_ref, a_last, w_sc, b_sc, wd_sc, ctab, stab, k_last, v_last, q_last,
           pos_ref, gamma_ref, beta_ref, bd_ref, bias_ref, tcos_ref, tsin_ref, own, xbuf, dbuf, rbuf, posr, y_0, y_1, kt_0, kt_1, kt_2, vt, kk, qbd, s_0, s_1, s_2, s_3, top_sc, ctx_buf, ctx_recv,
           t_sem, hid_sem, w_sem, xs_sem, xr_sem, ds_sem, dr_sem, rs_sem, rr_sem, cs_sem, cr_sem, ps_sem, pr_sem):
    step = pl.program_id(0)
    s_refs, kt_refs = (s_0, s_1, s_2, s_3), (kt_0, kt_1, kt_2)
    me = lax.axis_index('sp')
    core = lax.rem(me, 2)
    chip = me // 2
    other = 1 - chip
    peer_x = other * 2 + core
    peer_d = chip * 2 + 1 - core
    peer_xd = other * 2 + 1 - core

    def remote(src, dst, send_sem, recv_sem, peer):
        return pltpu.make_async_remote_copy(src, dst, send_sem, recv_sem, device_id={'sp': peer}, device_id_type=MESH)

    def send_x(r):
        return remote(own.at[r], xbuf.at[r], xs_sem.at[r], xr_sem.at[r], peer_x)

    def send_d(r):
        return remote(own.at[r], dbuf.at[lax.rem(r, 2)], ds_sem.at[r], dr_sem.at[r], peer_d)

    def relay(r):
        return remote(xbuf.at[r], rbuf.at[lax.rem(r, 2)], rs_sem.at[r], rr_sem.at[r], peer_d)

    def swap_ctx(r):
        return remote(ctx_buf.at[lax.rem(r, 2), 1 - core], ctx_recv.at[lax.rem(r, 2)], cs_sem.at[r], cr_sem.at[r], peer_d)

    def swap_pos(n, peer):
        return remote(pos_ref.at[:, pl.ds(128, 128)], posr.at[me], ps_sem.at[n], pr_sem.at[n], peer)

    def recv_pos(n, peer):
        return remote(pos_ref.at[:, pl.ds(128, 128)], posr.at[peer], ps_sem.at[n], pr_sem.at[n], peer)

    def load_hidden(r):
        return pltpu.make_async_copy(hid_hbm.at[r], own.at[r], hid_sem.at[r])

    def small_copies():
        pairs = ((gamma_hbm, gamma_ref), (beta_hbm, beta_ref), (pos_hbm, pos_ref), (bd_hbm, bd_ref), (bias_hbm, bias_ref), (tcos_hbm, tcos_ref), (tsin_hbm, tsin_ref))
        return [pltpu.make_async_copy(src, dst, t_sem.at[i]) for i, (src, dst) in enumerate(pairs)]

    def weight_copies():
        copies = []
        for group, owner in enumerate((me, peer_x, peer_d, peer_xd)):
            for slot, kind in ((0, 1), (6, 2), (12, 0)):
                copies.append((w_hbm.at[pl.ds(owner * 3, 3), kind], w_sc.at[pl.ds(18 * (group // 2) + slot + 3 * (group % 2), 3)]))
        for slot, owner in enumerate((me, peer_x, peer_d, peer_xd)):
            copies.append((wd_hbm.at[pl.ds(pl.multiple_of(owner * 192, 64), 192)], wd_sc.at[pl.ds(slot * 192, 192)]))
        return [pltpu.make_async_copy(src, dst, w_sem.at[i]) for i, (src, dst) in enumerate(copies)]

    def norm_row(r):
        gamma = gamma_ref[...].astype(F32).reshape(1, HID)
        beta = beta_ref[...].astype(F32).reshape(1, HID)
        for t in range(0, PART, 32):
            rows = pl.ds(t, 32)
            wide = own[r, rows, :].astype(F32)
            mean = jnp.sum(wide, axis=-1, keepdims=True) * (1.0 / HID)
            cent = wide - mean
            var = jnp.sum(cent * cent, axis=-1, keepdims=True) * (1.0 / HID)
            own[r, rows, :] = (cent * lax.rsqrt(var + LN_EPS) * gamma + beta).astype(BF16)

    def spread_bias():
        for group, owner in enumerate((me, peer_x, peer_d, peer_xd)):
            for slot, kind in ((0, 1), (6, 2), (12, 0)):
                for h in range(3):
                    row = bias_ref[owner * 3 + h, kind:kind + 1, :].astype(F32)
                    b_sc[18 * (group // 2) + slot + 3 * (group % 2) + h] = jnp.broadcast_to(row, (128, HEAD)).T

    @pl.when(step == 0)
    def _():
        small = small_copies()
        for c in small[:2]:
            c.start()

        def fetch(r, c):
            load_hidden(r).start()
            return c

        lax.fori_loop(0, ROWS, fetch, 0)
        barrier = pltpu.get_barrier_semaphore()
        for peer in (peer_x, peer_d, peer_xd):
            pl.semaphore_signal(barrier, inc=1, device_id={'sp': peer}, device_id_type=MESH)
        for c in small[2:] + weight_copies():
            c.start()
        for c in small[:2]:
            c.wait()
        load_hidden(0).wait()
        norm_row(0)
        pl.semaphore_wait(barrier, 3)
        load_hidden(1).wait()
        norm_row(1)
        send_x(0).start()

        def norm_and_send(r, c):
            load_hidden(r).wait()
            norm_row(r)

            @pl.when(r <= AHEAD)
            def _():
                send_x(r - 1).start()

            return c

        lax.fori_loop(2, ROWS, norm_and_send, 0)
        for c in small[2:]:
            c.wait()
        for n, peer in enumerate((peer_x, peer_d, peer_xd)):
            swap_pos(n, peer).start()
        send_d(0).start()
        posr[me] = pos_ref[:, 128:256]
        qbd[...] = jnp.zeros_like(qbd)
        spread_bias()
        for c in weight_copies():
            c.wait()
        for n, peer in enumerate((peer_x, peer_d, peer_xd)):
            recv_pos(n, peer).wait()

    def build_tables(r):
        tcos = tcos_ref[...]
        tsin = tsin_ref[...]
        lane = lax.broadcasted_iota(jnp.int32, (16, SEQ), 1)
        ctx = ctx_ref[r]
        last = posr[3, pl.ds(r, 1), :]
        last_lane = lax.broadcasted_iota(jnp.int32, (1, 128), 1)
        m_pos = jnp.sum(jnp.where(last_lane == 127, last, 0), axis=1, keepdims=True)

        def pick(table, hit):
            return jnp.sum(jnp.where(hit, table, 0.0), axis=1, keepdims=True)

        at_m = lane == m_pos
        at_c = lane == ctx - 1
        in_ctx = lane < ctx
        cos_c, sin_c = pick(tcos, at_c), pick(tsin, at_c)
        ctab[0:16] = jnp.where(in_ctx, tcos, pick(tcos, at_m))
        stab[0:16] = jnp.where(in_ctx, tsin, pick(tsin, at_m))
        ctab[16:32] = jnp.where(in_ctx, 1.0, tcos * cos_c + tsin * sin_c)
        stab[16:32] = jnp.where(in_ctx, 0.0, tsin * cos_c - tcos * sin_c)

    def dense(r):
        mixed = jnp.concatenate([ctx_buf[lax.rem(r, 2), core], ctx_recv[lax.rem(r, 2)]], axis=0)
        out_ref[r] = project_out(mixed, wd_sc[...], own[r], bd_ref)

    @pl.when(step > 0)
    def _():
        swap_ctx(step - 1).start()

    @pl.when(step == LAST)
    def _():
        build_tables(step)
        send_d(step).wait_recv()
        q_last[...] = jnp.zeros_like(q_last)
        for group in range(2):
            base = 3 * LOCAL * group
            multiply(y_0, w_sc, base, 3 * WIDE, own[LAST])
            multiply(y_1, w_sc, base, 2 * WIDE, dbuf[LAST % 2])
            last_refs = [k_last.at[group, pair] for pair in range(LOCAL // 2)]
            finish(y_0, b_sc, base, me, 0, ctab, stab, last_refs, v_last.at[group], q_last.at[group])
            finish(y_1, b_sc, base, peer_d, None, ctab, stab, last_refs, v_last.at[group], None)

    send_x(step).wait_recv()
    relay(step).start()

    @pl.when(step < ROWS - AHEAD)
    def _():
        send_x(step + AHEAD).start()

    @pl.when(step < LAST)
    def _():
        build_tables(step)
        send_d(step).wait_recv()
        multiply(y_0, w_sc, 0, 3 * WIDE, own[step])
        multiply(y_1, w_sc, 0, 3 * WIDE, dbuf[lax.rem(step, 2)])
        finish(y_0, b_sc, 0, me, core * PART, ctab, stab, kt_refs, vt, qbd)
        finish(y_1, b_sc, 0, peer_d, (1 - core) * PART, ctab, stab, kt_refs, vt, qbd)

    @pl.when(step == LAST)
    def _():
        a_last[0] = own[LAST]
        multiply(y_0, w_sc, 0, 2 * WIDE, xbuf[LAST])
        multiply(y_1, w_sc, 3 * LOCAL, 2 * WIDE, xbuf[LAST])
        for group in range(2):
            last_refs = [k_last.at[group, pair] for pair in range(LOCAL // 2)]
            finish((y_0, y_1)[group], b_sc, 3 * LOCAL * group, peer_x, None, ctab, stab, last_refs, v_last.at[group], None)

    @pl.when(step > 0)
    def _():
        swap_ctx(step - 1).wait()
        dense(step - 1)

    @pl.when(step < ROWS)
    def _():
        relay(step).wait_recv()

    @pl.when(step < ROWS - 1)
    def _():
        send_d(step + 1).start()

    @pl.when(step < LAST)
    def _():
        multiply(y_0, w_sc, 0, 2 * WIDE, xbuf[step])
        multiply(y_1, w_sc, 0, 2 * WIDE, rbuf[lax.rem(step, 2)])

    def rest(r, this_chip):
        finish(y_0, b_sc, 0, peer_x, None, ctab, stab, kt_refs, vt, qbd)
        finish(y_1, b_sc, 0, peer_xd, None, ctab, stab, kt_refs, vt, qbd)
        ko_ref[r, 0:2] = kt_0[...].reshape(2, HEAD, SEQ)
        ko_ref[r, 2] = kt_1[0:HEAD]
        vo_ref[r] = vt[0:192].reshape(3, HEAD, SEQ)
        for pair in range(LOCAL // 2):
            kk[pair] = kt_refs[pair][...].T

        def store(qb, v_rows, value):
            ctx_buf[lax.rem(r, 2), qb, v_rows, :] = value

        spec = ((768, 256), (768, 256)) if this_chip == 0 else ((768, 512), (1024, 768))
        attend(spec, this_chip * CHIP, ctx_ref[r], kk, qbd, vt, s_refs, top_sc, store)

    for this_chip in range(2):
        @pl.when(jnp.logical_and(step < LAST, chip == this_chip))
        def _():
            rest(step, this_chip)

    @pl.when(step == LAST)
    def _():
        a_last[1] = rbuf[LAST % 2]

        def drain(r, c):
            send_x(r).wait_send()
            relay(r).wait_send()
            send_d(r).wait_send()
            return c

        lax.fori_loop(0, ROWS, drain, 0)


def last_row(ctx_ref, bd_hbm, out_vm, keys_vm, values_vm, a_last, w_sc, b_sc, wd_sc, ctab, stab, k_last, v_last, q_last,
             out_hbm, keys_hbm, values_hbm,
             bd_ref, y_0, y_1, kt_0, kt_1, kt_2, vt, kk, s_0, s_2, top_sc, ctx_buf, out_row, key_row, value_row, sem, row_sem):
    me = lax.axis_index('sp')
    bulk = []
    for i, (src, dst) in enumerate(((keys_vm, keys_hbm), (values_vm, values_hbm), (out_vm, out_hbm))):
        for n in range(3):
            bulk.append(pltpu.make_async_copy(src.at[pl.ds(5 * n, 5)], dst.at[pl.ds(5 * n, 5)], sem.at[3 * i + n]))
    bd_copy = pltpu.make_async_copy(bd_hbm, bd_ref, row_sem.at[3])
    bd_copy.start()
    for c in bulk:
        c.start()
    kt_refs = (kt_0, kt_1, kt_2)
    s_refs = (s_0, None, s_2, None)
    row_copies = [pltpu.make_async_copy(src, dst.at[LAST], row_sem.at[i]) for i, (src, dst) in enumerate(((out_row, out_hbm), (key_row, keys_hbm), (value_row, values_hbm)))]
    far = 3 - me
    for group in range(2):
        multiply((y_0, y_1)[group], w_sc, 3 * LOCAL * group, 2 * WIDE, a_last[1])
    for group in range(2):
        for pair in range(LOCAL // 2):
            kt_refs[pair][...] = k_last[group, pair]
        vt[...] = v_last[group]
        finish((y_0, y_1)[group], b_sc, 3 * LOCAL * group, far, None, ctab, stab, kt_refs, vt, None)
        if group == 0:
            key_row[0:2] = kt_0[...].reshape(2, HEAD, SEQ)
            key_row[2] = kt_1[0:HEAD]
            value_row[...] = vt[0:192].reshape(3, HEAD, SEQ)
        for pair in range(LOCAL // 2):
            kk[pair] = kt_refs[pair][...].T

        def store(qb, v_rows, value):
            ctx_buf[group, v_rows, :] = value

        for live, spec in ((me < 2, (768, 256)), (me == 2, (768, 512)), (me == 3, (1024, 768))):
            @pl.when(live)
            def _():
                attend((spec,), me * PART, ctx_ref[LAST], kk, q_last.at[group], vt, s_refs, top_sc, store)

        if group == 0:
            row_copies[1].start()
            row_copies[2].start()
    bd_copy.wait()
    out_row[...] = project_out(ctx_buf[...].reshape(HID, PART), wd_sc[...], a_last[0], bd_ref)
    row_copies[0].start()
    for c in bulk + row_copies:
        c.wait()


def solution(mesh):
    seq_spec = P('dp', 'sp', None)
    row_spec = P('dp', 'sp')
    head_spec = P('dp', None, 'sp', None)
    replicated = P()
    tcos, tsin = rope_tables()

    def local_block(hidden, pos_ids, block_ids, ctx_len, ln_gamma, ln_beta, w_qkv, b_qkv, w_dense, b_dense):
        w_t = jnp.transpose(w_qkv, (1, 2, 3, 0))
        anywhere = pl.BlockSpec(memory_space=pltpu.HBM)

        held = pl.pallas_call(
            kernel,
            grid=(ROWS,),
            out_shape=(
                pltpu.VMEM((ROWS, PART, HID), BF16),
                pltpu.VMEM((ROWS, 3, HEAD, SEQ), BF16),
                pltpu.VMEM((ROWS, 3, HEAD, SEQ), BF16),
                pltpu.VMEM((2, PART, HID), BF16),
                pltpu.VMEM((36, HEAD, HID), BF16),
                pltpu.VMEM((36, HEAD, 128), F32),
                pltpu.VMEM((HID, HID), BF16),
                pltpu.VMEM((32, SEQ), F32),
                pltpu.VMEM((32, SEQ), F32),
                pltpu.VMEM((2, LOCAL // 2, 2 * HEAD, SEQ), BF16),
                pltpu.VMEM((2, WIDE, SEQ), BF16),
                pltpu.VMEM((2, LOCAL // 2, 2 * HEAD, 2 * PART), BF16),
            ),
            in_specs=[anywhere, anywhere, pl.BlockSpec(memory_space=pltpu.SMEM)] + [anywhere] * 8,
            out_specs=(pl.BlockSpec(memory_space=pltpu.VMEM),) * 12,
            scratch_shapes=[
                pltpu.VMEM((ROWS, PART), jnp.int32),
                pltpu.VMEM((HID,), BF16),
                pltpu.VMEM((HID,), BF16),
                pltpu.VMEM((HID,), BF16),
                pltpu.VMEM((12, 3, HEAD), BF16),
                pltpu.VMEM((16, SEQ), F32),
                pltpu.VMEM((16, SEQ), F32),
                pltpu.VMEM((ROWS, PART, HID), BF16),
                pltpu.VMEM((ROWS, PART, HID), BF16),
                pltpu.VMEM((2, PART, HID), BF16),
                pltpu.VMEM((2, PART, HID), BF16),
                pltpu.VMEM((4, ROWS, 128), jnp.int32),
                pltpu.VMEM((3 * WIDE, PART), F32),
                pltpu.VMEM((3 * WIDE, PART), F32),
                *[pltpu.VMEM((2 * HEAD, SEQ), BF16)] * 3,
                pltpu.VMEM((WIDE, SEQ), BF16),
                pltpu.VMEM((3, SEQ, 128), BF16),
                pltpu.VMEM((3, 128, 2 * CHIP), BF16),
                *[pltpu.VMEM((SEQ, PART), F32)] * 4,
                pltpu.VMEM((4, 8, PART), F32),
                pltpu.VMEM((2, 2, WIDE, PART), BF16),
                pltpu.VMEM((2, WIDE, PART), BF16),
                pltpu.SemaphoreType.DMA((7,)),
                pltpu.SemaphoreType.DMA((ROWS,)),
                pltpu.SemaphoreType.DMA((16,)),
            ] + [pltpu.SemaphoreType.DMA((ROWS,))] * 8 + [pltpu.SemaphoreType.DMA((3,))] * 2,
            compiler_params=pltpu.CompilerParams(
                collective_id=0, has_side_effects=True, vmem_limit_bytes=32 * 1024 * 1024, dimension_semantics=('arbitrary',)),
            name='glm_block',
        )(hidden, pos_ids, ctx_len, ln_gamma, ln_beta, b_dense,
          w_t, b_qkv, w_dense, jnp.asarray(tcos), jnp.asarray(tsin))
        held = [pltpu.with_memory_space_constraint(x, pltpu.VMEM) for x in held]
        out, keys_t, values_t = pl.pallas_call(
            last_row,
            out_shape=[jax.ShapeDtypeStruct(x.shape, BF16) for x in held[:3]],
            in_specs=[pl.BlockSpec(memory_space=pltpu.SMEM), anywhere] + [pl.BlockSpec(memory_space=pl.ANY)] * 3 + [pl.BlockSpec(memory_space=pltpu.VMEM)] * 9,
            out_specs=[anywhere] * 3,
            scratch_shapes=[
                pltpu.VMEM((HID,), BF16),
                *[pltpu.VMEM((2 * WIDE, PART), F32)] * 2,
                *[pltpu.VMEM((2 * HEAD, SEQ), BF16)] * 3,
                pltpu.VMEM((WIDE, SEQ), BF16),
                pltpu.VMEM((3, SEQ, 128), BF16),
                *[pltpu.VMEM((SEQ, PART), F32)] * 2,
                pltpu.VMEM((4, 8, PART), F32),
                pltpu.VMEM((2, WIDE, PART), BF16),
                pltpu.VMEM((PART, HID), BF16),
                pltpu.VMEM((3, HEAD, SEQ), BF16),
                pltpu.VMEM((3, HEAD, SEQ), BF16),
                pltpu.SemaphoreType.DMA((9,)),
                pltpu.SemaphoreType.DMA((4,)),
            ],
            compiler_params=pltpu.CompilerParams(vmem_limit_bytes=32 * 1024 * 1024),
            name='last_row',
        )(ctx_len, b_dense, *held)
        return out, jnp.transpose(keys_t, (0, 3, 1, 2)), jnp.transpose(values_t, (0, 3, 1, 2))

    return jax.shard_map(local_block, mesh=mesh, in_specs=(seq_spec, row_spec, row_spec, P('dp'), replicated, replicated, replicated, replicated, replicated, replicated), out_specs=(seq_spec, head_spec, head_spec), check_vma=False)
```
